16 devices in a mesh: data: 16 (over z, y, x, core).
Axes of the slice: x: 2, y: 2, z: 2, core: 2. Of those that a mesh axis runs over, the one named last changes fastest.
Arguments:
- x_init: bfloat16 [128, 128, 1280], P('data')
- cot_out: bfloat16 [128, 128, 1280], P('data')
- w_query: bfloat16 [2, 1280, 1280], replicated
- w_key: bfloat16 [2, 1280, 1280], replicated
- w_value: bfloat16 [2, 1280, 1280], replicated
- w_proj: bfloat16 [2, 1280, 1280], replicated
- w_up: bfloat16 [1280, 5120], replicated
- w_down: bfloat16 [5120, 1280], replicated
Outputs:
- output 1: float32 [2, 1280, 1280], replicated
- output 2: float32 [2, 1280, 1280], replicated
- output 3: float32 [2, 1280, 1280], replicated
- output 4: float32 [2, 1280, 1280], replicated
- output 5: float32 [1280, 5120], replicated
- output 6: float32 [5120, 1280], replicated
- output 7: bfloat16 [128, 128, 1280], P('data')
All inputs are finite; a program needn't handle non-finite values.
Results may differ from the reference program's by a relative error of at most 0.02.
Values are sent between devices in bfloat16 or wider.
A program may use at most 1 GiB of HBM per device.

```python
import jax
import jax.numpy as jnp
from jax import lax

D = 1280
HEADS = 20
LAYERS = 2
BATCH = 128
SEQ = 128
FF = 4 * D
HEAD_DIM = D // HEADS
EPS = 1e-6


def setup_inputs(seed: int = 0) -> dict:
    keys = jax.random.split(jax.random.key(seed), 8)
    res_scale = (2.0 * LAYERS) ** -0.5
    x_init = jax.random.normal(keys[0], (BATCH, SEQ, D), jnp.float32)
    cot_out = jax.random.normal(keys[1], (BATCH, SEQ, D), jnp.float32)
    w_query = jax.random.normal(keys[2], (LAYERS, D, D), jnp.float32) * D ** -0.5
    w_key = jax.random.normal(keys[3], (LAYERS, D, D), jnp.float32) * D ** -0.5
    w_value = jax.random.normal(keys[4], (LAYERS, D, D), jnp.float32) * D ** -0.5
    w_proj = jax.random.normal(keys[5], (LAYERS, D, D), jnp.float32) * (D ** -0.5 * res_scale)
    w_up = jax.random.normal(keys[6], (D, FF), jnp.float32) * D ** -0.5
    w_down = jax.random.normal(keys[7], (FF, D), jnp.float32) * (FF ** -0.5 * res_scale)
    return {
        "x_init": x_init.astype(jnp.bfloat16),
        "cot_out": cot_out.astype(jnp.bfloat16),
        "w_query": w_query.astype(jnp.bfloat16),
        "w_key": w_key.astype(jnp.bfloat16),
        "w_value": w_value.astype(jnp.bfloat16),
        "w_proj": w_proj.astype(jnp.bfloat16),
        "w_up": w_up.astype(jnp.bfloat16),
        "w_down": w_down.astype(jnp.bfloat16),
    }


def rms_norm(x_f32):
    return x_f32 * lax.rsqrt(jnp.mean(x_f32 * x_f32, axis=-1, keepdims=True) + EPS)


def as_bf16(val_f32):
    return val_f32.astype(jnp.bfloat16).astype(jnp.float32)


def layer_fwd(x_seq, w_query, w_key, w_value, w_proj, w_up, w_down):
    x_f32 = x_seq.astype(jnp.float32)
    normed = as_bf16(rms_norm(x_f32))
    query = as_bf16(jnp.dot(normed, w_query, preferred_element_type=jnp.float32)).reshape(SEQ, HEADS, HEAD_DIM)
    key_act = as_bf16(jnp.dot(normed, w_key, preferred_element_type=jnp.float32)).reshape(SEQ, HEADS, HEAD_DIM)
    value = as_bf16(jnp.dot(normed, w_value, preferred_element_type=jnp.float32)).reshape(SEQ, HEADS, HEAD_DIM)
    scores = jnp.einsum("qhd,khd->hqk", query, key_act) * HEAD_DIM ** -0.5
    probs = as_bf16(jax.nn.softmax(scores, axis=-1))
    mixed = as_bf16(jnp.einsum("hqk,khd->qhd", probs, value)).reshape(SEQ, D)
    hidden = as_bf16(x_f32 + as_bf16(jnp.dot(mixed, w_proj, preferred_element_type=jnp.float32)))
    normed2 = as_bf16(rms_norm(hidden))
    pre_act = as_bf16(jnp.dot(normed2, w_up, preferred_element_type=jnp.float32))
    activated = as_bf16(jax.nn.gelu(pre_act, approximate=True))
    mlp_out = as_bf16(jnp.dot(activated, w_down, preferred_element_type=jnp.float32))
    return (hidden + mlp_out).astype(jnp.bfloat16)


layer_ckpt = jax.checkpoint(layer_fwd)


def stack_fwd(x_seq, w_query, w_key, w_value, w_proj, w_up, w_down):
    def layer_step(x_carry, layer_w):
        x_new = layer_ckpt(x_carry, layer_w[0], layer_w[1], layer_w[2], layer_w[3], w_up, w_down)
        return x_new, None

    return lax.scan(layer_step, x_seq, (w_query, w_key, w_value, w_proj))[0]


def reference(x_init, cot_out, w_query, w_key, w_value, w_proj, w_up, w_down):
    weights = (
        w_query.astype(jnp.float32),
        w_key.astype(jnp.float32),
        w_value.astype(jnp.float32),
        w_proj.astype(jnp.float32),
        w_up.astype(jnp.float32),
        w_down.astype(jnp.float32),
    )
    zero_sums = tuple(jnp.zeros_like(weight) for weight in weights)

    def per_sequence(grad_sums, seq_pair):
        pull_back = jax.vjp(stack_fwd, seq_pair[0], *weights)[1]
        seq_grads = pull_back(seq_pair[1])
        new_sums = tuple(total + part for total, part in zip(grad_sums, seq_grads[1:]))
        return new_sums, seq_grads[0]

    grad_sums, dx_init = lax.scan(per_sequence, zero_sums, (x_init, cot_out))
    return (grad_sums[0], grad_sums[1], grad_sums[2], grad_sums[3], grad_sums[4], grad_sums[5], dx_init)
```

```python
import functools

import jax
import jax.numpy as jnp
from jax import lax
from jax.experimental import pallas as pl
from jax.experimental.pallas import tpu as pltpu
from jax.sharding import PartitionSpec as P

EPS = 1e-6
HEAD_DIM = 64
MESH = pl.DeviceIdType.MESH
ROWS, LANES = 40, 128
LAG = 2
ORDERS = ("xyz", "yzx", "zxy")


def rms_norm(x_f32):
    return x_f32 * lax.rsqrt(jnp.mean(x_f32 * x_f32, axis=-1, keepdims=True) + EPS)


def gelu_tanh(pre_f32):
    return jax.nn.gelu(pre_f32, approximate=True)


def product(subscripts, lhs, rhs):
    return jnp.einsum(subscripts, lhs, rhs, preferred_element_type=jnp.float32)


def scatter_kernel(segments, n_chunks, *refs):
    n_in_refs = len(segments)
    g_refs, out_refs = refs[:n_in_refs], refs[n_in_refs:2 * n_in_refs]
    own, rc, r1, r2, r3, load_sem, out_sem, send_sem, recv_sem = refs[2 * n_in_refs:]
    me = lax.axis_index("data")
    bit = {"c": lax.rem(me, 2), "x": lax.rem(me // 2, 2), "y": lax.rem(me // 4, 2), "z": me // 8}
    step = {"c": 1, "x": 2, "y": 4, "z": 8}
    peer = {d: me + step[d] * (1 - 2 * bit[d]) for d in step}
    barrier = pltpu.get_barrier_semaphore()
    for d in "cxyz":
        pl.semaphore_signal(barrier, inc=1, device_id=(peer[d],), device_id_type=MESH)
    pl.semaphore_wait(barrier, 4)
    n_own, n_in = own.shape[1], rc.shape[1]
    bufs = (rc, r1, r2, r3)

    def pick(color, stage, other):
        idx = {"z": slice(None), "y": slice(None), "x": slice(None)}
        for s in range(stage):
            d = ORDERS[color][s]
            idx[d] = 1 - bit[d] if (other and s == stage - 1) else bit[d]
        return tuple(idx[d] for d in "zyx")

    def place(seg, k):
        per, first = segments[seg]
        blocks = per // ROWS
        k = k - first
        return pl.multiple_of(lax.rem(k, blocks) * ROWS, 8), pl.multiple_of((k // blocks) * LANES, LANES)

    def each(k, fn):
        for seg in range(n_in_refs):
            first = segments[seg][1]
            last = segments[seg + 1][1] if seg + 1 < n_in_refs else n_chunks
            if n_in_refs == 1:
                fn(seg, k)
            else:
                @pl.when(jnp.logical_and(k >= first, k < last))
                def _():
                    fn(seg, k)

    def first_send(color, j, seg, k):
        row, col = place(seg, k)
        slot = lax.rem(j, n_in)
        return pltpu.make_async_remote_copy(
            g_refs[seg].at[:, :, :, 1 - bit["c"], pl.ds(row, ROWS), pl.ds(col, LANES)], rc.at[color, slot],
            send_sem.at[color, 0, slot], recv_sem.at[color, 0, slot], device_id=(peer["c"],), device_id_type=MESH)

    def next_send(color, stage, j):
        slot, so = lax.rem(j, n_in), lax.rem(j, n_own)
        return pltpu.make_async_remote_copy(
            own.at[(color, so) + pick(color, stage, True)], bufs[stage].at[color, slot],
            send_sem.at[color, stage, slot], recv_sem.at[color, stage, slot],
            device_id=(peer[ORDERS[color][stage - 1]],), device_id_type=MESH)

    def load(color, j, seg, k):
        so = lax.rem(j, n_own)
        row, col = place(seg, k)
        return pltpu.make_async_copy(g_refs[seg].at[:, :, :, bit["c"], pl.ds(row, ROWS), pl.ds(col, LANES)],
                                     own.at[color, so], load_sem.at[color, so])

    def store(color, j, seg, k):
        so = lax.rem(j, n_own)
        row, col = place(seg, k)
        return pltpu.make_async_copy(own.at[(color, so) + pick(color, 3, False)],
                                     out_refs[seg].at[pl.ds(row, ROWS), pl.ds(col, LANES)], out_sem.at[color, so])

    def live(j, color):
        return jnp.logical_and(j >= 0, 3 * j + color < n_chunks)

    def tick(t, carry):
        for color in range(3):
            j = t - 4 * LAG - 1

            @pl.when(live(j, color))
            def _():
                store(color, j, 0, segments[0][1]).wait()
        for stage in (3, 2, 1, 0):
            j = t - (stage + 1) * LAG
            for color in range(3):
                @pl.when(live(j, color))
                def _():
                    slot, so = lax.rem(j, n_in), lax.rem(j, n_own)
                    if stage == 0:
                        load(color, j, 0, segments[0][1]).wait()
                        copy = first_send(color, j, 0, segments[0][1])
                    else:
                        copy = next_send(color, stage, j)
                    copy.wait_send()
                    copy.wait_recv()
                    keep = (color, so) + pick(color, stage, False)
                    own[keep] = own[keep] + bufs[stage][color, slot]
                    if stage < 3:
                        next_send(color, stage + 1, j).start()
                    else:
                        each(3 * j + color, lambda seg, k: store(color, j, seg, k).start())
        for color in range(3):
            @pl.when(live(t, color))
            def _():
                def go(seg, k):
                    first_send(color, t, seg, k).start()
                    load(color, t, seg, k).start()
                each(3 * t + color, go)
        return carry

    lax.fori_loop(0, pl.cdiv(n_chunks, 3) + 4 * LAG + 1, tick, 0)


def scatter_sum(grads, collective_id):
    segments, first, views, outs = [], 0, [], []
    for grad in grads:
        rows, cols = grad.shape
        per = rows // 16
        segments.append((per, first))
        first += (per // ROWS) * (cols // LANES)
        views.append(grad.reshape(2, 2, 2, 2, per, cols))
        outs.append(jax.ShapeDtypeStruct((per, cols), jnp.float32))
    n_own, n_in, blk = 4 * LAG + 2, 2 * LAG, (ROWS, LANES)
    size = sum(g.size for g in grads) * 4
    return pl.pallas_call(
        functools.partial(scatter_kernel, tuple(segments), first),
        out_shape=outs,
        in_specs=[pl.BlockSpec(memory_space=pl.ANY)] * len(grads),
        out_specs=[pl.BlockSpec(memory_space=pl.ANY)] * len(grads),
        scratch_shapes=[
            pltpu.VMEM((3, n_own, 2, 2, 2) + blk, jnp.float32), pltpu.VMEM((3, n_in, 2, 2, 2) + blk, jnp.float32),
            pltpu.VMEM((3, n_in, 2, 2) + blk, jnp.float32), pltpu.VMEM((3, n_in, 2) + blk, jnp.float32),
            pltpu.VMEM((3, n_in) + blk, jnp.float32),
            pltpu.SemaphoreType.DMA((3, n_own)), pltpu.SemaphoreType.DMA((3, n_own)),
            pltpu.SemaphoreType.DMA((3, 4, n_in)), pltpu.SemaphoreType.DMA((3, 4, n_in))],
        compiler_params=pltpu.CompilerParams(collective_id=collective_id, has_side_effects=True),
        cost_estimate=pl.CostEstimate(flops=size * 8000, bytes_accessed=2 * size, transcendentals=0),
        name=f"scatter_sum_{collective_id}",
    )(*views)


def gather(shard):
    return lax.all_gather(shard, "data", axis=0, tiled=True)


def layer_forward(x_act, w_query, w_key, w_value, w_proj, w_up, w_down, heads):
    batch, seq_len, width = x_act.shape
    head_dim = width // heads
    x_f32 = x_act.astype(jnp.float32)
    normed = rms_norm(x_f32).astype(jnp.bfloat16)
    query = product("bsd,de->bse", normed, w_query).astype(jnp.bfloat16).reshape(batch, seq_len, heads, head_dim)
    key_act = product("bsd,de->bse", normed, w_key).astype(jnp.bfloat16).reshape(batch, seq_len, heads, head_dim)
    value = product("bsd,de->bse", normed, w_value).astype(jnp.bfloat16).reshape(batch, seq_len, heads, head_dim)
    scores = product("bqhd,bkhd->bhqk", query, key_act) * head_dim ** -0.5
    probs = jax.nn.softmax(scores, axis=-1).astype(jnp.bfloat16)
    mixed = product("bhqk,bkhd->bqhd", probs, value).astype(jnp.bfloat16).reshape(batch, seq_len, width)
    attn_out = product("bsd,de->bse", mixed, w_proj).astype(jnp.bfloat16)
    hidden = (x_f32 + attn_out.astype(jnp.float32)).astype(jnp.bfloat16)
    normed2 = rms_norm(hidden.astype(jnp.float32)).astype(jnp.bfloat16)
    pre_act = product("bsd,df->bsf", normed2, w_up).astype(jnp.bfloat16)
    activated = gelu_tanh(pre_act.astype(jnp.float32)).astype(jnp.bfloat16)
    mlp_out = product("bsf,fd->bsd", activated, w_down).astype(jnp.bfloat16)
    x_next = (hidden.astype(jnp.float32) + mlp_out.astype(jnp.float32)).astype(jnp.bfloat16)
    kept = (x_act, normed, query, key_act, value, probs, mixed, hidden, normed2, pre_act, activated)
    return x_next, kept


def mlp_backward(d_next, kept, w_up, w_down):
    hidden, normed2, pre_act = kept[7], kept[8], kept[9]
    d_activated = product("bsd,fd->bsf", d_next, w_down).astype(jnp.bfloat16)
    gelu_pull = jax.vjp(gelu_tanh, pre_act.astype(jnp.float32))[1]
    d_pre = gelu_pull(d_activated.astype(jnp.float32))[0].astype(jnp.bfloat16)
    d_normed2 = product("bsf,df->bsd", d_pre, w_up).astype(jnp.bfloat16)
    hidden_pull = jax.vjp(rms_norm, hidden.astype(jnp.float32))[1]
    d_hidden = (d_next.astype(jnp.float32) + hidden_pull(d_normed2.astype(jnp.float32))[0]).astype(jnp.bfloat16)
    return d_pre, d_hidden


def attention_backward(d_hidden, kept, w_query, w_key, w_value, w_proj):
    x_act, normed, query, key_act, value, probs, mixed = kept[:7]
    batch, seq_len, heads, head_dim = query.shape
    width = heads * head_dim
    g_proj = product("bsd,bse->de", mixed, d_hidden)
    d_mixed = product("bse,de->bsd", d_hidden, w_proj).astype(jnp.bfloat16).reshape(batch, seq_len, heads, head_dim)
    d_probs = product("bqhd,bkhd->bhqk", d_mixed, value).astype(jnp.bfloat16).astype(jnp.float32)
    d_value = product("bhqk,bqhd->bkhd", probs, d_mixed).astype(jnp.bfloat16).reshape(batch, seq_len, width)
    probs_f32 = probs.astype(jnp.float32)
    row_dot = jnp.sum(d_probs * probs_f32, axis=-1, keepdims=True)
    d_scores = (probs_f32 * (d_probs - row_dot) * head_dim ** -0.5).astype(jnp.bfloat16)
    d_query = product("bhqk,bkhd->bqhd", d_scores, key_act).astype(jnp.bfloat16).reshape(batch, seq_len, width)
    d_key = product("bhqk,bqhd->bkhd", d_scores, query).astype(jnp.bfloat16).reshape(batch, seq_len, width)
    g_query = product("bsd,bse->de", normed, d_query)
    g_key = product("bsd,bse->de", normed, d_key)
    g_value = product("bsd,bse->de", normed, d_value)
    d_normed = (product("bse,de->bsd", d_query, w_query) + product("bse,de->bsd", d_key, w_key)
                + product("bse,de->bsd", d_value, w_value)).astype(jnp.bfloat16)
    input_pull = jax.vjp(rms_norm, x_act.astype(jnp.float32))[1]
    d_input = (d_hidden.astype(jnp.float32) + input_pull(d_normed.astype(jnp.float32))[0]).astype(jnp.bfloat16)
    return d_input, (g_query, g_key, g_value, g_proj)


def place_rows(dst, shard_sum, layer):
    rows, cols = shard_sum.shape
    blk = 256

    def kernel(*refs):
        refs[-1][0] = refs[0][...]

    args = (shard_sum,) if dst is None else (shard_sum, dst)
    return pl.pallas_call(
        kernel,
        grid=(rows // blk,),
        out_shape=jax.ShapeDtypeStruct((2, rows, cols), jnp.float32),
        in_specs=[pl.BlockSpec((blk, cols), lambda i: (i, 0))] + [pl.BlockSpec(memory_space=pl.ANY)] * (len(args) - 1),
        out_specs=pl.BlockSpec((1, blk, cols), lambda i: (layer, i, 0)),
        input_output_aliases={} if dst is None else {1: 0},
        cost_estimate=pl.CostEstimate(flops=rows * cols, bytes_accessed=8 * rows * cols, transcendentals=0),
        name=f"place_rows_{layer}",
    )(*args)


def solution(mesh):
    def local_step(x_init, cot_out, w_query, w_key, w_value, w_proj, w_up, w_down):
        heads = x_init.shape[-1] // HEAD_DIM
        weights = [(w_query[i], w_key[i], w_value[i], w_proj[i]) for i in range(2)]
        x_mid, kept0 = layer_forward(x_init, *weights[0], w_up, w_down, heads)
        _, kept1 = layer_forward(x_mid, *weights[1], w_up, w_down, heads)
        d_pre1, d_hidden1 = mlp_backward(cot_out, kept1, w_up, w_down)
        d_mid, attn1 = attention_backward(d_hidden1, kept1, *weights[1])
        shards1 = scatter_sum(list(attn1), 1)
        full1 = [gather(s) for s in shards1]
        d_pre0, d_hidden0 = mlp_backward(d_mid, kept0, w_up, w_down)
        g_up = product("bsd,bsf->df", kept1[8], d_pre1) + product("bsd,bsf->df", kept0[8], d_pre0)
        g_down = product("bsf,bsd->fd", kept1[10], cot_out) + product("bsf,bsd->fd", kept0[10], d_mid)
        s_up, s_down = scatter_sum([g_up, g_down], 2)
        f_up, f_down = gather(s_up), gather(s_down)
        dx, attn0 = attention_backward(d_hidden0, kept0, *weights[0])
        shards0 = scatter_sum(list(attn0), 3)
        full0 = [gather(s) for s in shards0]
        attn = [place_rows(place_rows(None, a, 1), b, 0) for a, b in zip(full1, full0)]
        return (*attn, f_up, f_down, dx)

    data_spec = P("data")
    full_spec = P()
    in_specs = (data_spec, data_spec, full_spec, full_spec, full_spec, full_spec, full_spec, full_spec)
    out_specs = (full_spec, full_spec, full_spec, full_spec, full_spec, full_spec, data_spec)
    return jax.shard_map(local_step, mesh=mesh, in_specs=in_specs, out_specs=out_specs, check_vma=False)
```

```python
import functools
import jax, jax.numpy as jnp
from jax import lax
from jax.experimental import pallas as pl
from jax.experimental.pallas import tpu as pltpu
from jax.sharding import PartitionSpec as P

EPS = 1e-6
F32, BF16 = jnp.float32, jnp.bfloat16
TOK, D, FF, SEQ = 1024, 1280, 5120, 128
WB = 1280
NB = 256
PAIRS = 10
SLOTS = 2
MC, MCG, MCQ_, MCD_ = 128, 256, 256, 512
AHEAD = 1


def nn(a, b):
    return lax.dot_general(a, b, (((1,), (0,)), ((), ())), preferred_element_type=F32)


def nt(a, b):
    return lax.dot_general(a, b, (((1,), (1,)), ((), ())), preferred_element_type=F32)


def tn(a, b):
    return lax.dot_general(a, b, (((0,), (0,)), ((), ())), preferred_element_type=F32)


class Stage:
    def __init__(self, count, sub, start, step):
        self.count, self.sub, self.start, self.step = count, sub, start, step


def block_of(ref, row, col):
    return ref.at[pl.ds(row, D), pl.ds(col, WB)]


def run_stages(items, ring, sem):
    stages = [it for it in items if isinstance(it, Stage)]
    base, total = {}, 0
    for st in stages:
        base[id(st)] = total
        total += st.count * st.sub
    nxt = {id(a): b for a, b in zip(stages, stages[1:])}

    def begin(st, i, part, slot):
        for cond, src in st.start(i, part):
            if cond is None:
                pltpu.make_async_copy(src, ring.at[slot], sem.at[slot]).start()
            else:
                @pl.when(cond)
                def _():
                    pltpu.make_async_copy(src, ring.at[slot], sem.at[slot]).start()

    def wait(st, slot):
        pltpu.make_async_copy(st.start(0, 0)[0][1], ring.at[slot], sem.at[slot]).wait()

    flat = [(st, i, p) for st in stages for i in range(st.count) for p in range(st.sub)]
    for g in range(min(AHEAD, total)):
        st, i, p = flat[g]
        begin(st, i, p, g % SLOTS)
    for it in items:
        if not isinstance(it, Stage):
            it()
            continue
        st, n = it, it.count * it.sub

        def take(i, part, st=st, n=n):
            local = i * st.sub + part
            slot = lax.rem(base[id(st)] + local, SLOTS)
            wait(st, slot)
            ahead = local + AHEAD
            to = lax.rem(base[id(st)] + ahead, SLOTS)
            follow = nxt.get(id(st))
            inside = [None]

            @pl.when(ahead < n)
            def _():
                begin(st, ahead // st.sub, (part + AHEAD) % st.sub, to)
            if follow is not None:
                over = ahead - n

                @pl.when(over >= 0)
                def _():
                    if follow.sub == 1:
                        begin(follow, over, 0, to)
                    else:
                        for p in range(AHEAD):
                            @pl.when(over == p)
                            def _():
                                begin(follow, p // follow.sub, p % follow.sub, to)
            return slot

        if st.count == 1:
            st.step(0, functools.partial(take, 0))
        else:
            @pl.loop(0, st.count)
            def _(i):
                st.step(i, functools.partial(take, i))


C0 = 0.7978845608028654
C1 = C0 * 0.044715


def gelu(x):
    half = 0.5 * x
    return half * jnp.tanh(x * (C0 + C1 * (x * x))) + half


def gelu_grad(x, d):
    x2 = x * x
    t = jnp.tanh(x * (C0 + C1 * x2))
    return d * ((0.5 + 0.5 * t) + (x * (0.5 * C0 + 1.5 * C1 * x2)) * (1.0 - t * t))


def rms_rows(src, dst, rows=128):
    @pl.loop(0, TOK // rows)
    def _(i):
        r = pl.ds(pl.multiple_of(i * rows, rows), rows)
        x = src[r, :].astype(F32)
        dst[r, :] = (x * lax.rsqrt(jnp.mean(x * x, axis=-1, keepdims=True) + EPS)).astype(BF16)


def add_rms_rows(res, acc, out, dst, rows=128):
    @pl.loop(0, TOK // rows)
    def _(i):
        r = pl.ds(pl.multiple_of(i * rows, rows), rows)
        y = (res[r, :].astype(F32) + acc[r, :].astype(BF16).astype(F32)).astype(BF16)
        out[r, :] = y
        x = y.astype(F32)
        dst[r, :] = (x * lax.rsqrt(jnp.mean(x * x, axis=-1, keepdims=True) + EPS)).astype(BF16)


def rms_back_rows(x_ref, dy_acc, dres_ref, dst, rows=128):
    @pl.loop(0, TOK // rows)
    def _(i):
        r = pl.ds(pl.multiple_of(i * rows, rows), rows)
        x = x_ref[r, :].astype(F32)
        dy = dy_acc[r, :].astype(BF16).astype(F32)
        inv = lax.rsqrt(jnp.mean(x * x, axis=-1, keepdims=True) + EPS)
        dot = jnp.mean(dy * x, axis=-1, keepdims=True)
        dst[r, :] = (dres_ref[r, :].astype(F32) + (dy * inv - x * (inv * inv * inv * dot))).astype(BF16)


def lane_mask():
    return lax.broadcasted_iota(jnp.int32, (SEQ, 2 * 64), 1) < 64


def split_heads(x, mask):
    zero = jnp.zeros_like(x)
    return jnp.concatenate([jnp.where(mask, x, zero), jnp.where(mask, zero, x)], axis=0)


def attention_fwd(qkv, pt, mixed):
    mask = lane_mask()

    @pl.loop(0, TOK // SEQ)
    def _(s):
        rows = pl.ds(pl.multiple_of(s * SEQ, SEQ), SEQ)
        for h in range(PAIRS):
            lanes = lambda part: pl.ds(part * D + h * 128, 128)
            q, k, v = qkv[rows, lanes(0)], qkv[rows, lanes(1)], qkv[rows, lanes(2)]
            st = nt(k, split_heads(q, mask)) * 0.125
            e = jnp.exp(st - jnp.max(st, axis=0, keepdims=True))
            p = (e / jnp.sum(e, axis=0, keepdims=True)).astype(BF16)
            pt[s * PAIRS + h] = p
            o = tn(p, v)
            mixed[rows, pl.ds(h * 128, 128)] = jnp.where(mask, o[:SEQ], o[SEQ:]).astype(BF16)


def attention_bwd(qkv, pt, dmixed):
    mask = lane_mask()

    @pl.loop(0, TOK // SEQ)
    def _(s):
        rows = pl.ds(pl.multiple_of(s * SEQ, SEQ), SEQ)
        for h in range(PAIRS):
            lanes = lambda part: pl.ds(part * D + h * 128, 128)
            q, k, v = qkv[rows, lanes(0)], qkv[rows, lanes(1)], qkv[rows, lanes(2)]
            do = split_heads(dmixed[rows, pl.ds(h * 128, 128)], mask)
            p = pt[s * PAIRS + h]
            dp = nt(v, do).astype(BF16).astype(F32)
            pf = p.astype(F32)
            dot = jnp.sum(dp * pf, axis=0, keepdims=True)
            ds = (pf * (dp - dot) * 0.125).astype(BF16)
            dq = tn(ds, k)
            qkv[rows, lanes(0)] = jnp.where(mask, dq[:SEQ], dq[SEQ:]).astype(BF16)
            qkv[rows, lanes(1)] = nn(ds, split_heads(q, mask)).astype(BF16)
            qkv[rows, lanes(2)] = nn(p, do).astype(BF16)


def lane(i, width):
    return pl.ds(pl.multiple_of(i * width, 128), width)


class Saver:
    def __init__(self, sems):
        self.sems, self.n, self.open = sems, 0, {}

    def put(self, key, src, dst):
        cp = pltpu.make_async_copy(src, dst, self.sems.at[self.n])
        self.n += 1
        cp.start()
        self.open[key] = cp

    def done(self, *keys):
        for key in keys:
            if key in self.open:
                self.open.pop(key).wait()

    def finish(self):
        self.done(*list(self.open))


N_SAVE = 20


def front_kernel(x0, cot, wq, wk, wv, wo, w1, w2,
                 n0, qkv0, pt0, mx0, h0, nn0, pre0, act0, xmid, n1, dqkv1, mx1, nn1, act1, dpre1, dh1,
                 x, nrm, qkv, pt, mx, h, n2, big, g, acc, stg, ring, wsem, sems, stg_sem, in_sem):
    save = Saver(sems)
    cx = pltpu.make_async_copy(x0, x, in_sem.at[0])
    cg = pltpu.make_async_copy(cot, g, in_sem.at[1])
    cx.start()
    cg.start()

    def stage_wait(i, dst):
        @pl.when(i >= 2)
        def _():
            slot = lax.rem(i, 2)
            pltpu.make_async_copy(stg.at[slot], dst.at[:, pl.ds(0, D)], stg_sem.at[slot]).wait()

    def stage_put(i, dst):
        slot = lax.rem(i, 2)
        pltpu.make_async_copy(stg.at[slot], dst.at[:, lane(i, D)], stg_sem.at[slot]).start()

    def drain(dst):
        for slot in range(2):
            pltpu.make_async_copy(stg.at[slot], dst.at[:, pl.ds(0, D)], stg_sem.at[slot]).wait()

    MCQ, MCD = [[pl.ds(k * z, z) for k in range(TOK // z)] for z in (MCQ_, MCD_)]
    MGH = [pl.ds(k * MCG, MCG) for k in range(TOK // MCG)]
    MCH = [pl.ds(k * MC, MC) for k in range(TOK // MC)]
    subs = [pl.ds(j * NB, NB) for j in range(D // NB)]

    def sub(i, j):
        return pl.ds(pl.multiple_of(i * D + j * NB, NB), NB)

    def qkv_stage(layer):
        def start(i, part):
            return [(i == m, w.at[layer]) for m, w in enumerate((wq, wk, wv))]

        def step(i, take):
            slot = take(0)
            for j, c in enumerate(subs):
                for r in MCQ:
                    qkv[r, sub(i, j)] = nn(nrm[r, :], ring[slot, :, c]).astype(BF16)
        return Stage(3, 1, start, step)

    def proj_stage(layer):
        def step(i, take):
            slot = take(0)
            for c in subs:
                y = nn(mx[...], ring[slot, :, c]).astype(BF16).astype(F32)
                h[:, c] = (x[:, c].astype(F32) + y).astype(BF16)
        return Stage(1, 1, lambda i, part: [(None, wo.at[layer])], step)

    def up_stage(layer):
        to = pre0 if layer == 0 else act1

        def step(i, take):
            slot, half = take(0), lax.rem(i, 2)
            stage_wait(i, to)
            for j, c in enumerate(subs):
                for r in MCH:
                    pre = nn(n2[r, :], ring[slot, :, c]).astype(BF16)
                    act = gelu(pre.astype(F32)).astype(BF16)
                    big[r, sub(i, j)] = act if layer == 0 else pre
                    stg[half, r, c] = pre if layer == 0 else act
            stage_put(i, to)
        return Stage(4, 1, lambda i, part: [(None, w1.at[:, lane(i, D)])], step)

    def down_stage():
        def step(i, take):
            slot = take(0)

            @pl.when(i == 0)
            def _():
                for c in subs:
                    for r in MCD:
                        acc[r, c] = nn(big[r, lane(i, D)], ring[slot, :, c])

            @pl.when(i > 0)
            def _():
                for c in subs:
                    for r in MCD:
                        acc[r, c] += nn(big[r, lane(i, D)], ring[slot, :, c])
        return Stage(4, 1, lambda i, part: [(None, w2.at[lane(i, D)])], step)

    def dact_stage():
        def step(i, take):
            slot = take(0)
            for j, c in enumerate(subs):
                for r in MGH:
                    d = nt(g[r, :], ring[slot, c]).astype(BF16).astype(F32)
                    big[r, sub(i, j)] = gelu_grad(big[r, sub(i, j)].astype(F32), d).astype(BF16)
        return Stage(4, 1, lambda i, part: [(None, w2.at[lane(i, D)])], step)

    def dn2_stage():
        def step(i, take):
            slot = take(0)

            @pl.when(i == 0)
            def _():
                for c in subs:
                    for r in MCD:
                        acc[r, c] = nt(big[r, lane(i, D)], ring[slot, c])

            @pl.when(i > 0)
            def _():
                for c in subs:
                    for r in MCD:
                        acc[r, c] += nt(big[r, lane(i, D)], ring[slot, c])
        return Stage(4, 1, lambda i, part: [(None, w1.at[:, lane(i, D)])], step)

    def dmix_stage(layer, src, dst):
        def step(i, take):
            slot = take(0)
            for c in subs:
                dst[:, c] = nt(src[...], ring[slot, c]).astype(BF16)
        return Stage(1, 1, lambda i, part: [(None, wo.at[layer])], step)

    def first():
        cx.wait()
        rms_rows(x, nrm)
        save.put("nrm", nrm, n0)

    def attend0():
        save.put("qkv", qkv, qkv0)
        attention_fwd(qkv, pt, mx)
        save.put("pt", pt, pt0)
        save.put("mx", mx, mx0)

    def mid0():
        rms_rows(h, n2)
        save.put("h", h, h0)
        save.put("n2", n2, nn0)

    def after_up0():
        save.put("big", big, act0)
        drain(pre0)

    def second():
        save.done("nrm")
        add_rms_rows(h, acc, x, nrm)
        save.put("x", x, xmid)
        save.put("nrm", nrm, n1)
        save.done("qkv", "pt", "mx")

    def attend1():
        attention_fwd(qkv, pt, mx)
        save.put("mx", mx, mx1)
        save.done("h", "n2")

    def mid1():
        rms_rows(h, n2)
        save.put("n2", n2, nn1)
        save.done("big")

    def after_up1():
        drain(act1)
        cg.wait()

    def after_dact():
        save.put("big", big, dpre1)

    def after_dn2():
        save.done("x")
        rms_back_rows(h, acc, g, x)
        save.put("x", x, dh1)
        save.done("nrm")

    def last():
        attention_bwd(qkv, pt, nrm)
        save.put("qkv", qkv, dqkv1)
        save.finish()

    run_stages([first, qkv_stage(0), attend0, proj_stage(0), mid0, up_stage(0), after_up0, down_stage(), second,
                qkv_stage(1), attend1, proj_stage(1), mid1, up_stage(1), after_up1, dact_stage(), after_dact, dn2_stage(),
                after_dn2, dmix_stage(1, x, nrm), last], ring, wsem)


def front(x0, cot, wq, wk, wv, wo, w1, w2):
    td, t3, tf, tp = (TOK, D), (TOK, 3 * D), (TOK, FF), (TOK // SEQ * PAIRS, SEQ, 2 * SEQ)
    outs = [td, t3, tp, td, td, td, tf, tf, td, td, t3, td, td, tf, tf, td]
    return pl.pallas_call(
        front_kernel,
        out_shape=[jax.ShapeDtypeStruct(s, BF16) for s in outs],
        in_specs=[pl.BlockSpec(memory_space=pl.ANY)] * 8,
        out_specs=[pl.BlockSpec(memory_space=pl.ANY)] * len(outs),
        scratch_shapes=[pltpu.VMEM(td, BF16), pltpu.VMEM(td, BF16), pltpu.VMEM(t3, BF16), pltpu.VMEM(tp, BF16), pltpu.VMEM(td, BF16),
                        pltpu.VMEM(td, BF16), pltpu.VMEM(td, BF16), pltpu.VMEM(tf, BF16), pltpu.VMEM(td, BF16), pltpu.VMEM(td, F32),
                        pltpu.VMEM((2, TOK, D), BF16), pltpu.VMEM((SLOTS, D, D), BF16),
                        pltpu.SemaphoreType.DMA((SLOTS,)), pltpu.SemaphoreType.DMA((N_SAVE,)), pltpu.SemaphoreType.DMA((2,)),
                        pltpu.SemaphoreType.DMA((2,))],
        compiler_params=pltpu.CompilerParams(vmem_limit_bytes=67043328),
        name="front",
    )(x0.reshape(td), cot.reshape(td), wq, wk, wv, wo, w1, w2)


def mid_kernel(x0, xmid, h0, dh1, dqkv1, qkv0, pt0, pre0, wq, wk, wv, wo, w1, w2, _,
               dmid, dpre0, dh0, dqkv0, dx,
               x, h, g, t, dqkv, qkv, pt, big, acc, ring, wsem, sems, in_sem):
    save = Saver(sems)
    loads = {}
    for n, (key, src, dst) in enumerate([("dqkv", dqkv1, dqkv), ("x", xmid, x), ("t", dh1, t), ("big", pre0, big), ("h", h0, h),
                                         ("qkv", qkv0, qkv), ("pt", pt0, pt)]):
        loads[key] = pltpu.make_async_copy(src, dst, in_sem.at[n])
        loads[key].start()
    subs = [pl.ds(j * NB, NB) for j in range(D // NB)]
    MGH, MCD = [[pl.ds(k * z, z) for k in range(TOK // z)] for z in (MCG, MCD_)]

    def sub(i, j):
        return pl.ds(pl.multiple_of(i * D + j * NB, NB), NB)

    def sum_stage(count, start, src):
        def step(i, take):
            slot = take(0)

            @pl.when(i == 0)
            def _():
                for c in subs:
                    for r in MCD:
                        acc[r, c] = nt(src[r, lane(i, D)], ring[slot, c])

            @pl.when(i > 0)
            def _():
                for c in subs:
                    for r in MCD:
                        acc[r, c] += nt(src[r, lane(i, D)], ring[slot, c])
        return Stage(count, 1, start, step)

    def dn_stage(layer, src):
        return sum_stage(3, lambda i, part: [(i == m, w.at[layer]) for m, w in enumerate((wq, wk, wv))], src)

    def dact_stage():
        def step(i, take):
            slot = take(0)
            for j, c in enumerate(subs):
                for r in MGH:
                    d = nt(g[r, :], ring[slot, c]).astype(BF16).astype(F32)
                    big[r, sub(i, j)] = gelu_grad(big[r, sub(i, j)].astype(F32), d).astype(BF16)
        return Stage(4, 1, lambda i, part: [(None, w2.at[lane(i, D)])], step)

    def dmix_stage():
        def step(i, take):
            slot = take(0)
            for c in subs:
                x[:, c] = nt(t[...], ring[slot, c]).astype(BF16)
        return Stage(1, 1, lambda i, part: [(None, wo.at[0])], step)

    def first():
        loads["dqkv"].wait()

    def after_dn1():
        loads["x"].wait()
        loads["t"].wait()
        rms_back_rows(x, acc, t, g)
        save.put("g", g, dmid)
        loads["big"].wait()

    def after_dact():
        save.put("big", big, dpre0)
        loads["h"].wait()

    def after_dn2():
        rms_back_rows(h, acc, g, t)
        save.put("t", t, dh0)

    def attend():
        loads["qkv"].wait()
        loads["pt"].wait()
        attention_bwd(qkv, pt, x)
        save.put("qkv", qkv, dqkv0)
        again = pltpu.make_async_copy(x0, h, in_sem.at[0])
        again.start()
        again.wait()

    def last():
        save.done("g")
        rms_back_rows(h, acc, t, g)
        save.put("dx", g, dx)
        save.finish()

    run_stages([first, dn_stage(1, dqkv), after_dn1, dact_stage(), after_dact,
                sum_stage(4, lambda i, part: [(None, w1.at[:, lane(i, D)])], big), after_dn2, dmix_stage(), attend,
                dn_stage(0, qkv), last], ring, wsem)


def mid(x0, kept, wq, wk, wv, wo, w1, w2, after):
    td, t3, tf, tp = (TOK, D), (TOK, 3 * D), (TOK, FF), (TOK // SEQ * PAIRS, SEQ, 2 * SEQ)
    outs = [td, tf, td, t3, td]
    args = (x0.reshape(td), *kept, wq, wk, wv, wo, w1, w2, after)
    return pl.pallas_call(
        mid_kernel,
        out_shape=[jax.ShapeDtypeStruct(s, BF16) for s in outs],
        in_specs=[pl.BlockSpec(memory_space=pl.ANY)] * len(args),
        out_specs=[pl.BlockSpec(memory_space=pl.ANY)] * len(outs),
        scratch_shapes=[pltpu.VMEM(td, BF16)] * 4 + [pltpu.VMEM(t3, BF16), pltpu.VMEM(t3, BF16), pltpu.VMEM(tp, BF16),
                        pltpu.VMEM(tf, BF16), pltpu.VMEM(td, F32), pltpu.VMEM((SLOTS, D, D), BF16),
                        pltpu.SemaphoreType.DMA((SLOTS,)), pltpu.SemaphoreType.DMA((N_SAVE,)), pltpu.SemaphoreType.DMA((7,))],
        compiler_params=pltpu.CompilerParams(vmem_limit_bytes=67043328),
        cost_estimate=pl.CostEstimate(flops=100 * 10 ** 9, bytes_accessed=10 ** 8, transcendentals=0),
        name="mid",
    )(*args)


MESH = pl.DeviceIdType.MESH
ROWS, LANES = 40, 128
LAG = 2
TILES = 4
ORDERS = ("xyz", "yzx", "zxy")


def scatter_kernel(groups, n_tiles, depth, n_src, n_after, *refs):
    srcs, out_ref = refs[:n_src], refs[n_src + n_after]
    a_buf, b_buf, tiles, own, rc, r1, r2, r3, a_sem, b_sem, out_sem, send_sem, recv_sem = refs[n_src + n_after + 1:]
    me = lax.axis_index("data")
    bit = {"c": lax.rem(me, 2), "x": lax.rem(me // 2, 2), "y": lax.rem(me // 4, 2), "z": me // 8}
    step = {"c": 1, "x": 2, "y": 4, "z": 8}
    peer = {d: me + step[d] * (1 - 2 * bit[d]) for d in step}
    n_own, n_in = own.shape[1], rc.shape[1]
    n_chunks = 4 * n_tiles
    bufs = (rc, r1, r2, r3)

    def group_of(m):
        a = 0
        for first in groups[1:]:
            a = a + (m >= first[0]).astype(jnp.int32)
        return a

    def a_load(a, layer):
        return pltpu.make_async_copy(srcs[groups[a][1][layer]].at[:, pl.ds(groups[a][2], D)], a_buf.at[a % 2, layer], a_sem.at[a % 2, layer])

    def b_load(a, m, layer, first=None):
        col = pl.multiple_of(groups[a][4] + (m - groups[a][0]) * NB, NB) if first is None else first
        slot = lax.rem(m, 2)
        return pltpu.make_async_copy(srcs[groups[a][3][layer]].at[:, pl.ds(col, NB)], b_buf.at[slot, layer], b_sem.at[slot, layer])

    def in_group(a, m, fn):
        last = groups[a + 1][0] if a + 1 < len(groups) else n_tiles

        @pl.when(jnp.logical_and(m >= groups[a][0], m < last))
        def _():
            fn()

    def b_start(m):
        for a in range(len(groups)):
            def go(a=a):
                for layer in range(depth):
                    b_load(a, m, layer).start()
            in_group(a, m, go)

    def produce(m):
        for layer in range(depth):
            b_load(0, m, layer, 0).wait()
        for a in range(len(groups)):
            @pl.when(m == groups[a][0])
            def _():
                for layer in range(depth):
                    a_load(a, layer).wait()
                if a + 1 < len(groups):
                    for layer in range(depth):
                        a_load(a + 1, layer).start()
        b_start(m + 1)
        half, slot, to = lax.rem(group_of(m), 2), lax.rem(m, 2), lax.rem(m, TILES)
        for z in range(2):
            tot = None
            for layer in range(depth):
                y = tn(a_buf[half, layer, :, pl.ds(z * 640, 640)], b_buf[slot, layer])
                tot = y if tot is None else tot + y
            tiles[to, z] = tot.reshape(2, 2, 2, 2 * ROWS, NB)

    def pick(color, stage, other):
        idx = {"z": slice(None), "y": slice(None), "x": slice(None)}
        for s in range(stage):
            d = ORDERS[color][s]
            idx[d] = 1 - bit[d] if (other and s == stage - 1) else bit[d]
        return tuple(idx[d] for d in "zyx")

    def piece(k):
        sub = lax.rem(k, 4)
        return (lax.rem(k // 4, TILES), pl.multiple_of(lax.rem(sub, 2) * ROWS, 8), pl.multiple_of((sub // 2) * LANES, LANES))

    def send(color, stage, j):
        slot, so = lax.rem(j, n_in), lax.rem(j, n_own)
        if stage == 0:
            tile, row, col = piece(3 * j + color)
            src, to = tiles.at[tile, :, :, :, 1 - bit["c"], pl.ds(row, ROWS), pl.ds(col, LANES)], peer["c"]
        else:
            src, to = own.at[(color, so) + pick(color, stage, True)], peer[ORDERS[color][stage - 1]]
        return pltpu.make_async_remote_copy(src, bufs[stage].at[color, slot], send_sem.at[color, stage, slot],
                                            recv_sem.at[color, stage, slot], device_id=(to,), device_id_type=MESH)

    def store(color, j):
        so, k = lax.rem(j, n_own), 3 * j + color
        _, row, col = piece(k)
        col = pl.multiple_of((k // 4) * NB + col, LANES)
        return pltpu.make_async_copy(own.at[(color, so) + pick(color, 3, False)],
                                     out_ref.at[pl.ds(row, ROWS), pl.ds(col, LANES)], out_sem.at[color, so])

    def live(j, color):
        return jnp.logical_and(j >= 0, 3 * j + color < n_chunks)

    def tick(t, carry):
        for color in range(3):
            j = t - 4 * LAG - 1

            @pl.when(live(j, color))
            def _():
                store(color, j).wait()
        for stage in (3, 2, 1, 0):
            j = t - (stage + 1) * LAG
            for color in range(3):
                @pl.when(live(j, color))
                def _():
                    slot, so = lax.rem(j, n_in), lax.rem(j, n_own)
                    copy = send(color, stage, j)
                    copy.wait_send()
                    copy.wait_recv()
                    keep = (color, so) + pick(color, stage, False)
                    if stage == 0:
                        tile, row, col = piece(3 * j + color)
                        mine = tiles[tile, :, :, :, bit["c"], pl.ds(row, ROWS), pl.ds(col, LANES)]
                    else:
                        mine = own[keep]
                    own[keep] = mine + bufs[stage][color, slot]
                    if stage < 3:
                        send(color, stage + 1, j).start()
                    else:
                        store(color, j).start()
        for color in range(3):
            @pl.when(live(t, color))
            def _():
                send(color, 0, t).start()
        m = (3 * t + 5) // 4

        @pl.when(jnp.logical_and(m != (3 * t + 2) // 4, m < n_tiles))
        def _():
            produce(m)
        return carry

    for layer in range(depth):
        a_load(0, layer).start()
    b_start(jnp.int32(0))
    barrier = pltpu.get_barrier_semaphore()
    for d in "cxyz":
        pl.semaphore_signal(barrier, inc=1, device_id=(peer[d],), device_id_type=MESH)
    pl.semaphore_wait(barrier, 4)
    produce(jnp.int32(0))
    lax.fori_loop(0, pl.cdiv(n_chunks, 3) + 4 * LAG + 1, tick, 0)


def scatter_sum(srcs, groups, n_tiles, collective_id, after=()):
    depth = len(groups[0][1])
    n_own, n_in, blk = 4 * LAG + 2, 2 * LAG, (ROWS, LANES)
    size = D * NB * n_tiles * 4
    return pl.pallas_call(
        functools.partial(scatter_kernel, groups, n_tiles, depth, len(srcs), len(after)),
        out_shape=jax.ShapeDtypeStruct((2 * ROWS, NB * n_tiles), F32),
        in_specs=[pl.BlockSpec(memory_space=pl.ANY)] * (len(srcs) + len(after)),
        out_specs=pl.BlockSpec(memory_space=pl.ANY),
        scratch_shapes=[
            pltpu.VMEM((2, depth, TOK, D), BF16), pltpu.VMEM((2, depth, TOK, NB), BF16),
            pltpu.VMEM((TILES, 2, 2, 2, 2, 2 * ROWS, NB), F32),
            pltpu.VMEM((3, n_own, 2, 2, 2) + blk, F32), pltpu.VMEM((3, n_in, 2, 2, 2) + blk, F32),
            pltpu.VMEM((3, n_in, 2, 2) + blk, F32), pltpu.VMEM((3, n_in, 2) + blk, F32), pltpu.VMEM((3, n_in) + blk, F32),
            pltpu.SemaphoreType.DMA((2, depth)), pltpu.SemaphoreType.DMA((2, depth)), pltpu.SemaphoreType.DMA((3, n_own)),
            pltpu.SemaphoreType.DMA((3, 4, n_in)), pltpu.SemaphoreType.DMA((3, 4, n_in))],
        compiler_params=pltpu.CompilerParams(collective_id=collective_id, has_side_effects=True, vmem_limit_bytes=67043328),
        cost_estimate=pl.CostEstimate(flops=size * 4000, bytes_accessed=2 * size, transcendentals=0),
        name=f"scatter_sum_{collective_id}",
    )(*srcs, *after)


def gather(shard):
    return lax.all_gather(shard, "data", axis=0, tiled=True)


def place_attention(full, layer, dst):
    rows = 160

    def kernel(src, *refs):
        for n, out in enumerate(refs[-4:]):
            out[0] = src[:, n * D:(n + 1) * D]

    dst = dst or ()
    return pl.pallas_call(
        kernel,
        grid=(D // rows,),
        out_shape=[jax.ShapeDtypeStruct((2, D, D), F32)] * 4,
        in_specs=[pl.BlockSpec((rows, 4 * D), lambda i: (i, 0))] + [pl.BlockSpec(memory_space=pl.ANY)] * len(dst),
        out_specs=[pl.BlockSpec((1, rows, D), lambda i: (layer, i, 0))] * 4,
        input_output_aliases={n + 1: n for n in range(len(dst))},
        compiler_params=pltpu.CompilerParams(vmem_limit_bytes=60 << 20),
        cost_estimate=pl.CostEstimate(flops=D * D, bytes_accessed=32 * D * D, transcendentals=0),
        name=f"place_attention_{layer}",
    )(full, *dst)


def place_up(full, after):
    rows = 160
    return pl.pallas_call(
        lambda src, _, out: out.__setitem__(Ellipsis, src[...]),
        grid=(D // rows,),
        out_shape=jax.ShapeDtypeStruct((D, FF), F32),
        in_specs=[pl.BlockSpec((rows, FF), lambda i: (i, 0)), pl.BlockSpec(memory_space=pl.ANY)],
        out_specs=pl.BlockSpec((rows, FF), lambda i: (i, 0)),
        compiler_params=pltpu.CompilerParams(vmem_limit_bytes=60 << 20),
        cost_estimate=pl.CostEstimate(flops=D * D, bytes_accessed=32 * D * D, transcendentals=0),
        name="place_up",
    )(full, after)


def place_down(full, first, dst, after):
    rows = 640
    per, quarters = D // rows, full.shape[1] // D
    behind = (after,) if dst is None else (dst,)
    return pl.pallas_call(
        lambda src, _, out: out.__setitem__(Ellipsis, src[...]),
        grid=(quarters, per),
        out_shape=jax.ShapeDtypeStruct((FF, D), F32),
        in_specs=[pl.BlockSpec((rows, D), lambda q, i: (i, q)), pl.BlockSpec(memory_space=pl.ANY)],
        out_specs=pl.BlockSpec((rows, D), lambda q, i: ((first + q) * per + i, 0)),
        input_output_aliases={} if dst is None else {1: 0},
        compiler_params=pltpu.CompilerParams(vmem_limit_bytes=60 << 20),
        cost_estimate=pl.CostEstimate(flops=D * D, bytes_accessed=8 * quarters * D * D, transcendentals=0),
        name=f"place_down_{first}",
    )(full, *behind)


def solution(mesh):
    def local_step(x_init, cot_out, w_query, w_key, w_value, w_proj, w_up, w_down):
        weights = (w_query, w_key, w_value, w_proj, w_up, w_down)
        (n0, qkv0, pt0, mx0, h0, nn0, pre0, act0, xmid, n1, dqkv1, mx1, nn1, act1, dpre1, dh1) = front(x_init, cot_out, *weights)
        attention = ((0, (0,), 0, (1,), 0), (15, (2,), 0, (3,), 0))
        shard1 = scatter_sum((n1, dqkv1, mx1, dh1), attention, 20, 1)
        full1 = gather(shard1)
        dmid, dpre0, dh0, dqkv0, dx = mid(x_init, (xmid, h0, dh1, dqkv1, qkv0, pt0, pre0), *weights, shard1)
        shard0 = scatter_sum((n0, dqkv0, mx0, dh0), attention, 20, 2)
        full0 = gather(shard0)
        cot = cot_out.reshape(TOK, D)
        up = ((0, (0, 1), 0, (2, 3), 0),)
        shard_up = scatter_sum((nn0, nn1, dpre0, dpre1), up, 20, 3, (shard0,))
        full_up = gather(shard_up)
        down = [tuple((5 * n, (0, 1), q * D, (2, 3), 0) for n, q in enumerate(qs)) for qs in ((0, 1, 2), (3,))]
        shard_a = scatter_sum((act0, act1, dmid, cot), down[0], 15, 4, (shard_up,))
        full_a = gather(shard_a)
        shard_b = scatter_sum((act0, act1, dmid, cot), down[1], 5, 5, (shard_a,))
        full_b = gather(shard_b)
        attn = place_attention(full0, 0, place_attention(full1, 1, None))
        g_up = place_up(full_up, attn[0])
        g_down = place_down(full_b, 3, place_down(full_a, 0, None, g_up), None)
        return (*attn, g_up, g_down, dx.reshape(x_init.shape))

    data_spec = P("data")
    full_spec = P()
    in_specs = (data_spec, data_spec, full_spec, full_spec, full_spec, full_spec, full_spec, full_spec)
    out_specs = (full_spec, full_spec, full_spec, full_spec, full_spec, full_spec, data_spec)
    return jax.shard_map(local_step, mesh=mesh, in_specs=in_specs, out_specs=out_specs, check_vma=False)
```

```python
import functools
import jax, jax.numpy as jnp
from jax import lax
from jax.experimental import pallas as pl
from jax.experimental.pallas import tpu as pltpu
from jax.sharding import PartitionSpec as P

EPS = 1e-6
F32, BF16 = jnp.float32, jnp.bfloat16
TOK, D, FF, SEQ = 1024, 1280, 5120, 128
WB = 1280
NB = 256
PAIRS = 10
SLOTS = 2
MC, MCG, MCQ_, MCD_ = 128, 256, 256, 512
AHEAD = 1


def nn(a, b):
    return lax.dot_general(a, b, (((1,), (0,)), ((), ())), preferred_element_type=F32)


def nt(a, b):
    return lax.dot_general(a, b, (((1,), (1,)), ((), ())), preferred_element_type=F32)


def tn(a, b):
    return lax.dot_general(a, b, (((0,), (0,)), ((), ())), preferred_element_type=F32)


class Stage:
    def __init__(self, count, sub, start, step):
        self.count, self.sub, self.start, self.step = count, sub, start, step


def block_of(ref, row, col):
    return ref.at[pl.ds(row, D), pl.ds(col, WB)]


def run_stages(items, ring, sem):
    stages = [it for it in items if isinstance(it, Stage)]
    base, total = {}, 0
    for st in stages:
        base[id(st)] = total
        total += st.count * st.sub
    nxt = {id(a): b for a, b in zip(stages, stages[1:])}

    def begin(st, i, part, slot):
        for cond, src in st.start(i, part):
            if cond is None:
                pltpu.make_async_copy(src, ring.at[slot], sem.at[slot]).start()
            else:
                @pl.when(cond)
                def _():
                    pltpu.make_async_copy(src, ring.at[slot], sem.at[slot]).start()

    def wait(st, slot):
        pltpu.make_async_copy(st.start(0, 0)[0][1], ring.at[slot], sem.at[slot]).wait()

    flat = [(st, i, p) for st in stages for i in range(st.count) for p in range(st.sub)]
    for g in range(min(AHEAD, total)):
        st, i, p = flat[g]
        begin(st, i, p, g % SLOTS)
    for it in items:
        if not isinstance(it, Stage):
            it()
            continue
        st, n = it, it.count * it.sub

        def take(i, part, st=st, n=n):
            local = i * st.sub + part
            slot = lax.rem(base[id(st)] + local, SLOTS)
            wait(st, slot)
            ahead = local + AHEAD
            to = lax.rem(base[id(st)] + ahead, SLOTS)
            follow = nxt.get(id(st))
            inside = [None]

            @pl.when(ahead < n)
            def _():
                begin(st, ahead // st.sub, (part + AHEAD) % st.sub, to)
            if follow is not None:
                over = ahead - n

                @pl.when(over >= 0)
                def _():
                    if follow.sub == 1:
                        begin(follow, over, 0, to)
                    else:
                        for p in range(AHEAD):
                            @pl.when(over == p)
                            def _():
                                begin(follow, p // follow.sub, p % follow.sub, to)
            return slot

        if st.count == 1:
            st.step(0, functools.partial(take, 0))
        else:
            @pl.loop(0, st.count)
            def _(i):
                st.step(i, functools.partial(take, i))


C0 = 0.7978845608028654
C1 = C0 * 0.044715


def gelu(x):
    half = 0.5 * x
    return half * jnp.tanh(x * (C0 + C1 * (x * x))) + half


def gelu_grad(x, d):
    x2 = x * x
    t = jnp.tanh(x * (C0 + C1 * x2))
    return d * ((0.5 + 0.5 * t) + (x * (0.5 * C0 + 1.5 * C1 * x2)) * (1.0 - t * t))


def rms_rows(src, dst, rows=128):
    @pl.loop(0, TOK // rows)
    def _(i):
        r = pl.ds(pl.multiple_of(i * rows, rows), rows)
        x = src[r, :].astype(F32)
        dst[r, :] = (x * lax.rsqrt(jnp.mean(x * x, axis=-1, keepdims=True) + EPS)).astype(BF16)


def add_rms_rows(res, acc, out, dst, rows=128):
    @pl.loop(0, TOK // rows)
    def _(i):
        r = pl.ds(pl.multiple_of(i * rows, rows), rows)
        y = (res[r, :].astype(F32) + acc[r, :].astype(BF16).astype(F32)).astype(BF16)
        out[r, :] = y
        x = y.astype(F32)
        dst[r, :] = (x * lax.rsqrt(jnp.mean(x * x, axis=-1, keepdims=True) + EPS)).astype(BF16)


def rms_back_rows(x_ref, dy_acc, dres_ref, dst, rows=128):
    @pl.loop(0, TOK // rows)
    def _(i):
        r = pl.ds(pl.multiple_of(i * rows, rows), rows)
        x = x_ref[r, :].astype(F32)
        dy = dy_acc[r, :].astype(BF16).astype(F32)
        inv = lax.rsqrt(jnp.mean(x * x, axis=-1, keepdims=True) + EPS)
        dot = jnp.mean(dy * x, axis=-1, keepdims=True)
        dst[r, :] = (dres_ref[r, :].astype(F32) + (dy * inv - x * (inv * inv * inv * dot))).astype(BF16)


def lane_mask():
    return lax.broadcasted_iota(jnp.int32, (SEQ, 2 * 64), 1) < 64


def split_heads(x, mask):
    zero = jnp.zeros_like(x)
    return jnp.concatenate([jnp.where(mask, x, zero), jnp.where(mask, zero, x)], axis=0)


def split_heads_t(x):
    y = x.T
    top = lax.broadcasted_iota(jnp.int32, y.shape, 0) < 64
    zero = jnp.zeros_like(y)
    return jnp.concatenate([jnp.where(top, y, zero), jnp.where(top, zero, y)], axis=1)


def attention_fwd(qkv, pt, mixed):
    mask = lane_mask()

    @pl.loop(0, TOK // SEQ)
    def _(s):
        rows = pl.ds(pl.multiple_of(s * SEQ, SEQ), SEQ)
        for h in range(PAIRS):
            lanes = lambda part: pl.ds(part * D + h * 128, 128)
            q, k, v = qkv[rows, lanes(0)], qkv[rows, lanes(1)], qkv[rows, lanes(2)]
            st = nn(k, split_heads_t(q)) * 0.125
            e = jnp.exp(st - jnp.max(st, axis=0, keepdims=True))
            p = (e / jnp.sum(e, axis=0, keepdims=True)).astype(BF16)
            pt[rows, pl.ds(h * 256, 256)] = p
            o = tn(p, v)
            mixed[rows, pl.ds(h * 128, 128)] = jnp.where(mask, o[:SEQ], o[SEQ:]).astype(BF16)


def attention_bwd(s, qkv, pt, dmixed):
    mask = lane_mask()
    rows = pl.ds(pl.multiple_of(s * SEQ, SEQ), SEQ)
    for h in range(PAIRS):
        lanes = lambda part: pl.ds(part * D + h * 128, 128)
        q, k, v = qkv[rows, lanes(0)], qkv[rows, lanes(1)], qkv[rows, lanes(2)]
        do = split_heads(dmixed[rows, pl.ds(h * 128, 128)], mask)
        p = pt[rows, pl.ds(h * 256, 256)]
        dp = nt(v, do).astype(BF16).astype(F32)
        pf = p.astype(F32)
        dot = jnp.sum(dp * pf, axis=0, keepdims=True)
        ds = (pf * (dp - dot) * 0.125).astype(BF16)
        dq = tn(ds, k)
        qkv[rows, lanes(0)] = jnp.where(mask, dq[:SEQ], dq[SEQ:]).astype(BF16)
        qkv[rows, lanes(1)] = nn(ds, split_heads(q, mask)).astype(BF16)
        qkv[rows, lanes(2)] = nn(p, do).astype(BF16)


def lane(i, width):
    return pl.ds(pl.multiple_of(i * width, 128), width)


class Saver:
    def __init__(self, sems):
        self.sems, self.n, self.open = sems, 0, {}

    def put(self, key, src, dst):
        cp = pltpu.make_async_copy(src, dst, self.sems.at[self.n])
        self.n += 1
        cp.start()
        self.open[key] = cp

    def done(self, *keys):
        for key in keys:
            if key in self.open:
                self.open.pop(key).wait()

    def finish(self):
        self.done(*list(self.open))


N_SAVE = 20
SUBS = [pl.ds(j * NB, NB) for j in range(D // NB)]
MGH, MCD = [[pl.ds(k * z, z) for k in range(TOK // z)] for z in (MCG, MCD_)]


def front_kernel(x0, cot, wq, wk, wv, wo, w1, w2,
                 n0, qkv0, pt0, mx0, h0, nn0, pre0, act0, xmid, n1, qkv1, pt1, dmix1, mx1, nn1, act1, dpre1, dh1,
                 x, nrm, qkv, pt, mx, h, n2, big, g, acc, stg, ring, wsem, sems, stg_sem, in_sem):
    save = Saver(sems)
    cx = pltpu.make_async_copy(x0, x, in_sem.at[0])
    cg = pltpu.make_async_copy(cot, g, in_sem.at[1])
    cx.start()
    cg.start()

    def stage_wait(i, dst):
        @pl.when(i >= 2)
        def _():
            slot = lax.rem(i, 2)
            pltpu.make_async_copy(stg.at[slot], dst.at[:, pl.ds(0, D)], stg_sem.at[slot]).wait()

    def stage_put(i, dst):
        slot = lax.rem(i, 2)
        pltpu.make_async_copy(stg.at[slot], dst.at[:, lane(i, D)], stg_sem.at[slot]).start()

    def drain(dst):
        for slot in range(2):
            pltpu.make_async_copy(stg.at[slot], dst.at[:, pl.ds(0, D)], stg_sem.at[slot]).wait()

    MCQ, MCD = [[pl.ds(k * z, z) for k in range(TOK // z)] for z in (MCQ_, MCD_)]
    MGH = [pl.ds(k * MCG, MCG) for k in range(TOK // MCG)]
    MCH = [pl.ds(k * MC, MC) for k in range(TOK // MC)]
    subs = [pl.ds(j * NB, NB) for j in range(D // NB)]

    def sub(i, j):
        return pl.ds(pl.multiple_of(i * D + j * NB, NB), NB)

    def qkv_stage(layer):
        def start(i, part):
            return [(i == m, w.at[layer]) for m, w in enumerate((wq, wk, wv))]

        def step(i, take):
            slot = take(0)
            for j, c in enumerate(subs):
                for r in MCQ:
                    qkv[r, sub(i, j)] = nn(nrm[r, :], ring[slot, :, c]).astype(BF16)
        return Stage(3, 1, start, step)

    def proj_stage(layer):
        def step(i, take):
            slot = take(0)
            for c in subs:
                y = nn(mx[...], ring[slot, :, c]).astype(BF16).astype(F32)
                h[:, c] = (x[:, c].astype(F32) + y).astype(BF16)
        return Stage(1, 1, lambda i, part: [(None, wo.at[layer])], step)

    def up_stage(layer):
        to = pre0 if layer == 0 else act1

        def step(i, take):
            slot, half = take(0), lax.rem(i, 2)
            stage_wait(i, to)
            for j, c in enumerate(subs):
                for r in MCH:
                    pre = nn(n2[r, :], ring[slot, :, c]).astype(BF16)
                    act = gelu(pre.astype(F32)).astype(BF16)
                    big[r, sub(i, j)] = act if layer == 0 else pre
                    stg[half, r, c] = pre if layer == 0 else act
            stage_put(i, to)
        return Stage(4, 1, lambda i, part: [(None, w1.at[:, lane(i, D)])], step)

    def down_stage():
        def step(i, take):
            slot = take(0)

            for c in subs:
                for r in MCD:
                    acc[r, c] = jnp.where(i == 0, 0.0, acc[r, c]) + nn(big[r, lane(i, D)], ring[slot, :, c])
        return Stage(4, 1, lambda i, part: [(None, w2.at[lane(i, D)])], step)

    def dact_stage():
        def step(i, take):
            slot = take(0)
            for j, c in enumerate(subs):
                for r in MGH:
                    d = nt(g[r, :], ring[slot, c]).astype(BF16).astype(F32)
                    big[r, sub(i, j)] = gelu_grad(big[r, sub(i, j)].astype(F32), d).astype(BF16)
        return Stage(4, 1, lambda i, part: [(None, w2.at[lane(i, D)])], step)

    def dn2_stage():
        def step(i, take):
            slot = take(0)

            for c in subs:
                for r in MCD:
                    acc[r, c] = jnp.where(i == 0, 0.0, acc[r, c]) + nt(big[r, lane(i, D)], ring[slot, c])
        return Stage(4, 1, lambda i, part: [(None, w1.at[:, lane(i, D)])], step)

    def dmix_stage(layer, src, dst):
        def step(i, take):
            slot = take(0)
            for c in subs:
                dst[:, c] = nt(src[...], ring[slot, c]).astype(BF16)
        return Stage(1, 1, lambda i, part: [(None, wo.at[layer])], step)

    def first():
        cx.wait()
        rms_rows(x, nrm)
        save.put("nrm", nrm, n0)

    def attend0():
        save.put("qkv", qkv, qkv0)
        attention_fwd(qkv, pt, mx)
        save.put("pt", pt, pt0)
        save.put("mx", mx, mx0)

    def mid0():
        rms_rows(h, n2)
        save.put("h", h, h0)
        save.put("n2", n2, nn0)

    def after_up0():
        save.put("big", big, act0)
        drain(pre0)

    def second():
        save.done("nrm")
        add_rms_rows(h, acc, x, nrm)
        save.put("x", x, xmid)
        save.put("nrm", nrm, n1)
        save.done("qkv", "pt", "mx")

    def attend1():
        save.put("qkv", qkv, qkv1)
        attention_fwd(qkv, pt, mx)
        save.put("pt", pt, pt1)
        save.put("mx", mx, mx1)
        save.done("h", "n2")

    def mid1():
        rms_rows(h, n2)
        save.put("n2", n2, nn1)
        save.done("big")

    def after_up1():
        drain(act1)
        cg.wait()

    def after_dact():
        save.put("big", big, dpre1)

    def after_dn2():
        save.done("x")
        rms_back_rows(h, acc, g, x)
        save.put("x", x, dh1)
        save.done("nrm")

    def last():
        save.put("dmix", nrm, dmix1)
        save.finish()

    run_stages([first, qkv_stage(0), attend0, proj_stage(0), mid0, up_stage(0), after_up0, down_stage(), second,
                qkv_stage(1), attend1, proj_stage(1), mid1, up_stage(1), after_up1, dact_stage(), after_dact, dn2_stage(),
                after_dn2, dmix_stage(1, x, nrm), last], ring, wsem)


def front(x0, cot, wq, wk, wv, wo, w1, w2):
    td, t3, tf, tp = (TOK, D), (TOK, 3 * D), (TOK, FF), (TOK, PAIRS * 2 * SEQ)
    outs = [td, t3, tp, td, td, td, tf, tf, td, td, t3, tp, td, td, td, tf, tf, td]
    return pl.pallas_call(
        front_kernel,
        out_shape=[jax.ShapeDtypeStruct(s, BF16) for s in outs],
        in_specs=[pl.BlockSpec(memory_space=pl.ANY)] * 8,
        out_specs=[pl.BlockSpec(memory_space=pl.ANY)] * len(outs),
        scratch_shapes=[pltpu.VMEM(td, BF16), pltpu.VMEM(td, BF16), pltpu.VMEM(t3, BF16), pltpu.VMEM(tp, BF16), pltpu.VMEM(td, BF16),
                        pltpu.VMEM(td, BF16), pltpu.VMEM(td, BF16), pltpu.VMEM(tf, BF16), pltpu.VMEM(td, BF16), pltpu.VMEM(td, F32),
                        pltpu.VMEM((2, TOK, D), BF16), pltpu.VMEM((SLOTS, D, D), BF16),
                        pltpu.SemaphoreType.DMA((SLOTS,)), pltpu.SemaphoreType.DMA((N_SAVE,)), pltpu.SemaphoreType.DMA((2,)),
                        pltpu.SemaphoreType.DMA((2,))],
        compiler_params=pltpu.CompilerParams(vmem_limit_bytes=67043328),
        name="front",
    )(x0.reshape(td), cot.reshape(td), wq, wk, wv, wo, w1, w2)


MESH = pl.DeviceIdType.MESH
ROWS, LANES = 40, 128
GAP = 2
EARLY = TOK // SEQ
ORDERS = ("xyz", "yzx", "zxy")


def scatter_kernel(groups, n_tiles, depth, n_src, n_after, chain, layer_in, lag, *refs):
    srcs, refs = refs[:n_src], refs[n_src + n_after:]
    n_out = (1, 2, 4)[chain]
    out_ref, more, refs = refs[0], refs[1:n_out], refs[n_out:]
    a_buf, b_buf, tiles, own, rc, r1, r2, r3, a_sem, b_sem, out_sem, send_sem, recv_sem = refs[:13]
    if chain:
        xb, gb, tb, acc, wring, w_sem, at_sem, big = refs[13:21]
    if chain == 1:
        qkv = refs[21]
        dmixed_in, qkv_in, pt_in, x_in, d_in, wq, wk, wv = srcs[3:]
        pt = big
    if chain == 2:
        h_in, pre_in, d_in, wo, w1, w2 = srcs[4:]
    me = lax.axis_index("data")
    bit = {"c": lax.rem(me, 2), "x": lax.rem(me // 2, 2), "y": lax.rem(me // 4, 2), "z": me // 8}
    step = {"c": 1, "x": 2, "y": 4, "z": 8}
    peer = {d: me + step[d] * (1 - 2 * bit[d]) for d in step}
    n_own, n_in, ring = own.shape[1], rc.shape[1], tiles.shape[0]
    gap = GAP if chain == 1 else 0
    n_chunks = 4 * (n_tiles + gap)
    bufs = (rc, r1, r2, r3)

    def group_of(m):
        a = 0
        for first in groups[1:]:
            a = a + (m >= first[0]).astype(jnp.int32)
        return a

    def a_load(a, layer):
        return pltpu.make_async_copy(srcs[groups[a][1][layer]].at[:, pl.ds(groups[a][2], D)], a_buf.at[a % 2, layer], a_sem.at[a % 2, layer])

    def b_load(a, m, layer, first=None):
        col = pl.multiple_of(groups[a][4] + (m - groups[a][0]) * NB, NB) if first is None else first
        slot = lax.rem(m, 2)
        return pltpu.make_async_copy(srcs[groups[a][3][layer]].at[:, pl.ds(col, NB)], b_buf.at[slot, layer], b_sem.at[slot, layer])

    def in_group(a, m, fn):
        last = groups[a + 1][0] - gap if a + 1 < len(groups) else n_tiles + gap

        @pl.when(jnp.logical_and(m >= groups[a][0], m < last))
        def _():
            fn()

    def b_start(m):
        for a in range(len(groups)):
            if groups[a][3] is None:
                continue

            def go(a=a):
                for layer in range(depth):
                    b_load(a, m, layer).start()
            in_group(a, m, go)

    def produce(m):
        loaded = m < groups[-1][0] if gap else m >= 0

        @pl.when(loaded)
        def _():
            for layer in range(depth):
                b_load(0, m, layer, 0).wait()
        for a in range(len(groups)):
            @pl.when(m == groups[a][0])
            def _():
                for layer in range(depth):
                    a_load(a, layer).wait()
                if a + 1 < len(groups):
                    for layer in range(depth):
                        a_load(a + 1, layer).start()
        b_start(m + 1)
        half, slot, to = lax.rem(group_of(m), 2), lax.rem(m, 2), lax.rem(m, ring)

        def fill(b_of):
            for z in range(2):
                tot = None
                for layer in range(depth):
                    y = tn(a_buf[half, layer, :, pl.ds(z * 640, 640)], b_of(layer))
                    tot = y if tot is None else tot + y
                tiles[to, z] = tot.reshape(2, 2, 2, 2 * ROWS, NB)

        if gap:
            @pl.when(loaded)
            def _():
                fill(lambda layer: b_buf[slot, layer])

            @pl.when(jnp.logical_not(loaded))
            def _():
                fill(lambda layer: qkv[:, pl.ds(pl.multiple_of((m - groups[-1][0]) * NB, NB), NB)])
        else:
            fill(lambda layer: b_buf[slot, layer])

    def pick(color, stage, other):
        idx = {"z": slice(None), "y": slice(None), "x": slice(None)}
        for s in range(stage):
            d = ORDERS[color][s]
            idx[d] = 1 - bit[d] if (other and s == stage - 1) else bit[d]
        return tuple(idx[d] for d in "zyx")

    def piece(k):
        sub = lax.rem(k, 4)
        return (lax.rem(k // 4, ring), pl.multiple_of(lax.rem(sub, 2) * ROWS, 8), pl.multiple_of((sub // 2) * LANES, LANES))

    def send(color, stage, j):
        slot, so = lax.rem(j, n_in), lax.rem(j, n_own)
        if stage == 0:
            tile, row, col = piece(3 * j + color)
            src, to = tiles.at[tile, :, :, :, 1 - bit["c"], pl.ds(row, ROWS), pl.ds(col, LANES)], peer["c"]
        else:
            src, to = own.at[(color, so) + pick(color, stage, True)], peer[ORDERS[color][stage - 1]]
        return pltpu.make_async_remote_copy(src, bufs[stage].at[color, slot], send_sem.at[color, stage, slot],
                                            recv_sem.at[color, stage, slot], device_id=(to,), device_id_type=MESH)

    def store(color, j):
        so, k = lax.rem(j, n_own), 3 * j + color
        _, row, col = piece(k)
        tile = k // 4
        if gap:
            tile = tile - gap * (tile >= groups[1][0]).astype(jnp.int32)
        col = pl.multiple_of(tile * NB + col, LANES)
        return pltpu.make_async_copy(own.at[(color, so) + pick(color, 3, False)],
                                     out_ref.at[pl.ds(row, ROWS), pl.ds(col, LANES)], out_sem.at[color, so])

    def live(j, color):
        k = 3 * j + color
        ok = jnp.logical_and(j >= 0, k < n_chunks)
        if gap:
            ok = jnp.logical_and(ok, jnp.logical_or(k < 4 * (groups[1][0] - gap), k >= 4 * groups[1][0]))
        return ok

    n_steps = (0, 16, 46)[chain]

    def w_begin(w):
        def go(cond, src):
            @pl.when(cond)
            def _():
                slot = lax.rem(w, 3)
                pltpu.make_async_copy(src, wring.at[slot], w_sem.at[slot]).start()
        j = pl.multiple_of(lax.rem(w, 5) * NB, NB)
        if chain == 1:
            for m, ref in enumerate((wq, wk, wv)):
                go(jnp.logical_and(w >= 5 * m, w < 5 * m + 5), ref.at[layer_in, pl.ds(j, NB)])
        else:
            go(w < 20, w2.at[pl.ds(pl.multiple_of(w * NB, NB), NB)])
            go(jnp.logical_and(w >= 20, w < 40), w1.at[pl.ds(j, NB), pl.ds(pl.multiple_of(((w - 20) // 5) * D, 128), D)])
            go(jnp.logical_and(w >= 40, w < 45), wo.at[layer_in, pl.ds(j, NB)])

    def w_take(w):
        slot = lax.rem(w, 3)
        pltpu.make_async_copy((wq if chain == 1 else wo).at[0, pl.ds(0, NB)], wring.at[slot], w_sem.at[slot]).wait()
        w_begin(w + 2)
        return slot

    def start(*names):
        for name in names:
            copies[name].start()

    def wait(*names):
        for name in names:
            copies[name].wait()

    if chain:
        if chain == 1:
            table = dict(dmixed=(dmixed_in, xb), qkv=(qkv_in, qkv), pt=(pt_in, pt), x=(x_in, xb), d=(d_in, tb), first=(gb, more[0]))
        else:
            table = dict(d=(d_in, gb), h=(h_in, xb), pre=(pre_in, big), dpre=(big, more[0]), dh=(tb, more[1]), dmix=(xb, more[2]))
        copies = {name: pltpu.make_async_copy(src, dst, at_sem.at[n]) for n, (name, (src, dst)) in enumerate(table.items())}

    def sum_step(g, src, slot):
        c, m = pl.ds(pl.multiple_of(lax.rem(g, 5) * NB, NB), NB), g // 5
        for r in MCD:
            acc[r, c] = jnp.where(m == 0, 0.0, acc[r, c]) + nt(src[r, lane(m, D)], wring[slot])

    def input_step(g):
        @pl.when(g < 15)
        def _():
            sum_step(g, qkv, w_take(g))

        @pl.when(g == 15)
        def _():
            wait("x", "d")
            rms_back_rows(xb, acc, tb, gb)
            start("first")

    def mlp_step(g):
        @pl.when(g == 0)
        def _():
            wait("d", "pre")

        @pl.when(g < 20)
        def _():
            slot = w_take(g)
            c = pl.ds(pl.multiple_of(g * NB, NB), NB)
            for r in MGH:
                d = nt(gb[r, :], wring[slot]).astype(BF16).astype(F32)
                big[r, c] = gelu_grad(big[r, c].astype(F32), d).astype(BF16)

        @pl.when(g == 20)
        def _():
            start("dpre")

        @pl.when(jnp.logical_and(g >= 20, g < 40))
        def _():
            sum_step(g - 20, big, w_take(g))

        @pl.when(g == 40)
        def _():
            wait("h")
            rms_back_rows(xb, acc, gb, tb)
            start("dh")

        @pl.when(jnp.logical_and(g >= 41, g < 46))
        def _():
            slot = w_take(g - 1)
            c = pl.ds(pl.multiple_of((g - 41) * NB, NB), NB)
            for r in MCD:
                xb[r, c] = nt(tb[r, :], wring[slot]).astype(BF16)

        @pl.when(g == 45)
        def _():
            start("dmix")

    def tick(t, carry):
        for color in range(3):
            j = t - 4 * lag - 1

            @pl.when(live(j, color))
            def _():
                store(color, j).wait()
        for stage in (3, 2, 1, 0):
            j = t - (stage + 1) * lag
            for color in range(3):
                @pl.when(live(j, color))
                def _():
                    slot, so = lax.rem(j, n_in), lax.rem(j, n_own)
                    copy = send(color, stage, j)
                    copy.wait_send()
                    copy.wait_recv()
                    keep = (color, so) + pick(color, stage, False)
                    if stage == 0:
                        tile, row, col = piece(3 * j + color)
                        mine = tiles[tile, :, :, :, bit["c"], pl.ds(row, ROWS), pl.ds(col, LANES)]
                    else:
                        mine = own[keep]
                    own[keep] = mine + bufs[stage][color, slot]
                    if stage < 3:
                        send(color, stage + 1, j).start()
                    else:
                        store(color, j).start()
        for color in range(3):
            @pl.when(live(t, color))
            def _():
                send(color, 0, t).start()
        m = (3 * t + 5) // 4

        fresh = jnp.logical_and(m != (3 * t + 2) // 4, m < n_tiles + gap)
        if gap:
            fresh = jnp.logical_and(fresh, jnp.logical_or(m < groups[1][0] - gap, m >= groups[1][0]))

        @pl.when(fresh)
        def _():
            produce(m)
        if chain == 1:
            @pl.when(t == 0)
            def _():
                wait("dmixed", "qkv", "pt")

            @pl.when(t < EARLY)
            def _():
                attention_bwd(t, qkv, pt, xb)

            @pl.when(t == EARLY)
            def _():
                start("x")

            @pl.when(jnp.logical_and(t >= EARLY, t < EARLY + 16))
            def _():
                input_step(t - EARLY)
        if chain == 2:
            @pl.when(t < 23)
            def _():
                @pl.loop(0, 2)
                def _(u):
                    mlp_step(2 * t + u)
        return carry

    for layer in range(depth):
        a_load(0, layer).start()
    b_start(jnp.int32(0))
    if chain:
        start(*(("dmixed", "qkv", "pt", "d") if chain == 1 else ("d", "pre", "h")))
        w_begin(jnp.int32(0))
        w_begin(jnp.int32(1))
    barrier = pltpu.get_barrier_semaphore()
    for d in "cxyz":
        pl.semaphore_signal(barrier, inc=1, device_id=(peer[d],), device_id_type=MESH)
    pl.semaphore_wait(barrier, 4)
    produce(jnp.int32(0))
    ticks = pl.cdiv(n_chunks, 3) + 4 * lag + 1
    lax.fori_loop(0, ticks, tick, 0)
    if chain:
        wait(*(("first",) if chain == 1 else ("dpre", "dh", "dmix")))


def scatter_sum(srcs, groups, n_tiles, collective_id, after=(), chain=0, layer=0, lag=2):
    depth = len(groups[0][1])
    n_own, n_in, ring, blk = 4 * lag + 2, 2 * lag + (4 if chain == 1 else 0), lag + 2, (ROWS, LANES)
    size = D * NB * n_tiles * 4
    td, t3, tf = (TOK, D), (TOK, 3 * D), (TOK, FF)
    outs = [(), (td,), (tf, td, td)][chain]
    args = (*srcs, *after)
    scratch = [
        pltpu.VMEM((2, depth, TOK, D), BF16), pltpu.VMEM((2, depth, TOK, NB), BF16),
        pltpu.VMEM((ring, 2, 2, 2, 2, 2 * ROWS, NB), F32),
        pltpu.VMEM((3, n_own, 2, 2, 2) + blk, F32), pltpu.VMEM((3, n_in, 2, 2, 2) + blk, F32),
        pltpu.VMEM((3, n_in, 2, 2) + blk, F32), pltpu.VMEM((3, n_in, 2) + blk, F32), pltpu.VMEM((3, n_in) + blk, F32),
        pltpu.SemaphoreType.DMA((2, depth)), pltpu.SemaphoreType.DMA((2, depth)), pltpu.SemaphoreType.DMA((3, n_own)),
        pltpu.SemaphoreType.DMA((3, 4, n_in)), pltpu.SemaphoreType.DMA((3, 4, n_in))]
    if chain:
        scratch += [pltpu.VMEM(td, BF16), pltpu.VMEM(td, BF16), pltpu.VMEM(td, BF16), pltpu.VMEM(td, F32),
                    pltpu.VMEM((3, NB, D), BF16), pltpu.SemaphoreType.DMA((3,)), pltpu.SemaphoreType.DMA((6,))]
        scratch += [pltpu.VMEM((TOK, PAIRS * 2 * SEQ), BF16), pltpu.VMEM(t3, BF16)] if chain == 1 else [pltpu.VMEM(tf, BF16)]
    return pl.pallas_call(
        functools.partial(scatter_kernel, groups, n_tiles, depth, len(srcs), len(after), chain, layer, lag),
        out_shape=[jax.ShapeDtypeStruct((2 * ROWS, NB * n_tiles), F32)] + [jax.ShapeDtypeStruct(o, BF16) for o in outs],
        in_specs=[pl.BlockSpec(memory_space=pl.ANY)] * len(args),
        out_specs=[pl.BlockSpec(memory_space=pl.ANY)] * (1 + len(outs)),
        scratch_shapes=scratch,
        compiler_params=pltpu.CompilerParams(collective_id=collective_id, has_side_effects=True, vmem_limit_bytes=67043328),
        cost_estimate=pl.CostEstimate(flops=size * 4000, bytes_accessed=2 * size, transcendentals=0),
        name=f"scatter_sum_{collective_id}",
    )(*args)


def gather(shard):
    return lax.all_gather(shard, "data", axis=0, tiled=True)


ANY = pl.BlockSpec(memory_space=pl.ANY)


def place_attention(full, layer, dst, carry, after):
    rows, part = 160, TOK * 160 // D

    def kernel(src, *refs):
        outs = refs[-4 - len(carry):]
        for n, out in zip((1, 2, 3, 0), outs):
            out[0] = src[:, n * D:(n + 1) * D]
        for ref, out in zip(refs, outs[4:]):
            out[...] = ref[...]

    strip = pl.BlockSpec((part, D), lambda i: (i, 0))
    return pl.pallas_call(
        kernel,
        grid=(D // rows,),
        out_shape=[jax.ShapeDtypeStruct((2, D, D), F32)] * 4 + [jax.ShapeDtypeStruct((TOK, D), BF16)] * len(carry),
        in_specs=[pl.BlockSpec((rows, 4 * D), lambda i: (i, 0))] + [strip] * len(carry) + [ANY] * (len(dst) + len(after)),
        out_specs=[pl.BlockSpec((1, rows, D), lambda i: (layer, i, 0))] * 4 + [strip] * len(carry),
        input_output_aliases={n + 1 + len(carry): n for n in range(len(dst))},
        compiler_params=pltpu.CompilerParams(vmem_limit_bytes=60 << 20),
        cost_estimate=pl.CostEstimate(flops=D * D, bytes_accessed=32 * D * D, transcendentals=0),
        name=f"place_attention_{layer}",
    )(full, *carry, *dst, *after)


def place_blocks(full, shape, where, dst, after, name):
    rows = 640
    per, blocks = D // rows, full.shape[1] // D

    def to(n, i):
        row, col = where(n)
        return row * per + i, col

    def kernel(src, *refs):
        refs[-1][...] = src[...]

    return pl.pallas_call(
        kernel,
        grid=(blocks, per),
        out_shape=jax.ShapeDtypeStruct(shape, F32),
        in_specs=[pl.BlockSpec((rows, D), lambda n, i: (i, n))] + [ANY] * (len(dst) + len(after)),
        out_specs=pl.BlockSpec((rows, D), to),
        input_output_aliases={1: 0} if dst else {},
        compiler_params=pltpu.CompilerParams(vmem_limit_bytes=60 << 20),
        cost_estimate=pl.CostEstimate(flops=D * D, bytes_accessed=8 * blocks * D * D, transcendentals=0),
        name=name,
    )(full, *dst, *after)


def solution(mesh):
    def local_step(x_init, cot_out, w_query, w_key, w_value, w_proj, w_up, w_down):
        weights = (w_query, w_key, w_value, w_proj, w_up, w_down)
        (n0, qkv0, pt0, mx0, h0, nn0, pre0, act0, xmid, n1, qkv1, pt1, dmix1, mx1, nn1, act1, dpre1, dh1) = front(
            x_init, cot_out, *weights)
        cot, x0 = cot_out.reshape(TOK, D), x_init.reshape(TOK, D)
        w_in = (w_query, w_key, w_value)
        attention = ((0, (0,), 0, (1,), 0), (5 + GAP, (2,), 0, None, 0))
        down = [tuple((5 * n, (0, 1), q * D, (2, 3), 0) for n, q in enumerate(qs)) for qs in ((0, 1, 2), (3,))]
        up = ((0, (0, 1), 0, (2, 3), 0),)
        shard1, dmid = scatter_sum((mx1, dh1, n1, dmix1, qkv1, pt1, xmid, dh1, *w_in), attention, 20, 1, chain=1, layer=1)
        full1 = gather(shard1)
        shard_a, dpre0, dh0, dmix0 = scatter_sum(
            (act0, act1, dmid, cot, h0, pre0, dmid, w_proj, w_up, w_down), down[0], 15, 2, (shard1,), chain=2, layer=0)
        full_a = gather(shard_a)
        shard0, dx = scatter_sum((mx0, dh0, n0, dmix0, qkv0, pt0, x0, dh0, *w_in), attention, 20, 3, (shard_a,), chain=1, layer=0)
        full0 = gather(shard0)
        shard_up, = scatter_sum((nn0, nn1, dpre0, dpre1), up, 20, 4, (shard0,))
        full_up = gather(shard_up)
        shard_b, = scatter_sum((act0, act1, dmid, cot), down[1], 5, 5, (shard_up,))
        full_b = gather(shard_b)
        half = place_attention(full1, 1, (), (), (shard_b,))
        g_down = place_blocks(full_a, (FF, D), lambda n: (n, 0), (), (half[0],), "place_down_0")
        *attn, dx = place_attention(full0, 0, half, (dx,), (g_down,))
        g_up = place_blocks(full_up, (D, FF), lambda n: (0, n), (), (attn[0],), "place_up")
        g_down = place_blocks(full_b, (FF, D), lambda n: (3 + n, 0), (g_down,), (g_up,), "place_down_3")
        return (*attn, g_up, g_down, dx.reshape(x_init.shape))

    data_spec = P("data")
    full_spec = P()
    in_specs = (data_spec, data_spec, full_spec, full_spec, full_spec, full_spec, full_spec, full_spec)
    out_specs = (full_spec, full_spec, full_spec, full_spec, full_spec, full_spec, data_spec)
    return jax.shard_map(local_step, mesh=mesh, in_specs=in_specs, out_specs=out_specs, check_vma=False)
```

```python
import functools

import jax
import jax.numpy as jnp
from jax import lax
from jax.experimental import pallas as pl
from jax.experimental.pallas import tpu as pltpu
from jax.sharding import PartitionSpec as P

EPS = 1e-6
F32, BF16 = jnp.float32, jnp.bfloat16
TOK, D, FF, SEQ = 1024, 1280, 5120, 128
NB = 256
DB, FB = D // NB, FF // NB
PAIRS = 10
VMEM_MOST = 67043328
SUBS = [pl.ds(j * NB, NB) for j in range(DB)]
ANY = pl.BlockSpec(memory_space=pl.ANY)
C0 = 0.7978845608028654
C1 = C0 * 0.044715


def nn(a, b):
    return lax.dot_general(a, b, (((1,), (0,)), ((), ())), preferred_element_type=F32)


def nt(a, b):
    return lax.dot_general(a, b, (((1,), (1,)), ((), ())), preferred_element_type=F32)


def tn(a, b):
    return lax.dot_general(a, b, (((0,), (0,)), ((), ())), preferred_element_type=F32)


def part(i, width):
    return pl.ds(pl.multiple_of(i * width, 128), width)


def rows_of(size):
    return [pl.ds(k * size, size) for k in range(TOK // size)]


class Stage:
    def __init__(self, count, source, step):
        self.count, self.source, self.step = count, source, step


def begin(sources, ring, sem, slot):
    for cond, src in sources:
        copy = pltpu.make_async_copy(src, ring.at[slot], sem.at[slot])
        if cond is None:
            copy.start()
        else:
            pl.when(cond)(copy.start)


def run_stages(items, ring, sem, follow=()):
    stages = [it for it in items if isinstance(it, Stage)]
    base = 0
    for it in items:
        if not isinstance(it, Stage):
            it()
            continue
        after = stages[stages.index(it) + 1].source(0) if it is not stages[-1] else follow

        def one(i, it=it, base=base, after=after):
            slot = lax.rem(base + i, 2)
            pltpu.make_async_copy(it.source(0)[0][1], ring.at[slot], sem.at[slot]).wait()
            other = lax.rem(base + i + 1, 2)

            @pl.when(i + 1 < it.count)
            def _():
                begin(it.source(i + 1), ring, sem, other)

            @pl.when(i + 1 >= it.count)
            def _():
                begin(after, ring, sem, other)
            it.step(i, slot)

        pl.loop(0, it.count)(one)
        base += it.count


def gelu(x):
    half = 0.5 * x
    return half * jnp.tanh(x * (C0 + C1 * (x * x))) + half


def gelu_grad(x, d):
    x2 = x * x
    t = jnp.tanh(x * (C0 + C1 * x2))
    return d * ((0.5 + 0.5 * t) + (x * (0.5 * C0 + 1.5 * C1 * x2)) * (1.0 - t * t))


def by_rows(fn, rows=128):
    @pl.loop(0, TOK // rows)
    def _(i):
        fn(part(i, rows))


def inverse_rms(x):
    return lax.rsqrt(jnp.mean(x * x, axis=-1, keepdims=True) + EPS)


def rms_rows(src, dst):
    def one(r):
        x = src[r, :].astype(F32)
        dst[r, :] = (x * inverse_rms(x)).astype(BF16)
    by_rows(one)


def add_rms_rows(res, acc, out, dst):
    def one(r):
        y = (res[r, :].astype(F32) + acc[r, :].astype(BF16).astype(F32)).astype(BF16)
        out[r, :] = y
        x = y.astype(F32)
        dst[r, :] = (x * inverse_rms(x)).astype(BF16)
    by_rows(one)


def rms_back_rows(x_ref, dy_acc, dres_ref, dst):
    def one(r):
        x = x_ref[r, :].astype(F32)
        dy = dy_acc[r, :].astype(BF16).astype(F32)
        inv = inverse_rms(x)
        dot = jnp.mean(dy * x, axis=-1, keepdims=True)
        dst[r, :] = (dres_ref[r, :].astype(F32) + (dy * inv - x * (inv * inv * inv * dot))).astype(BF16)
    by_rows(one)


def lane_mask():
    return lax.broadcasted_iota(jnp.int32, (SEQ, 2 * 64), 1) < 64


def split_heads(x, mask):
    zero = jnp.zeros_like(x)
    return jnp.concatenate([jnp.where(mask, x, zero), jnp.where(mask, zero, x)], axis=0)


def split_heads_t(x):
    y = x.T
    top = lax.broadcasted_iota(jnp.int32, y.shape, 0) < 64
    zero = jnp.zeros_like(y)
    return jnp.concatenate([jnp.where(top, y, zero), jnp.where(top, zero, y)], axis=1)


def attention_fwd(qkv, pt, mixed):
    mask = lane_mask()

    def one(rows):
        for h in range(PAIRS):
            q, k, v = (qkv[rows, pl.ds(n * D + h * SEQ, SEQ)] for n in range(3))
            st = nn(k, split_heads_t(q)) * 0.125
            e = jnp.exp(st - jnp.max(st, axis=0, keepdims=True))
            p = (e / jnp.sum(e, axis=0, keepdims=True)).astype(BF16)
            pt[rows, pl.ds(h * NB, NB)] = p
            o = tn(p, v)
            mixed[rows, pl.ds(h * SEQ, SEQ)] = jnp.where(mask, o[:SEQ], o[SEQ:]).astype(BF16)
    by_rows(one, SEQ)


def attention_bwd(s, duo, qkv, pt, dmixed):
    mask = lane_mask()
    rows = part(s, SEQ)
    for h in range(2):
        lanes = [pl.ds(pl.multiple_of(n * D + duo * NB + h * SEQ, SEQ), SEQ) for n in range(3)]
        q, k, v = (qkv[rows, c] for c in lanes)
        do = split_heads(dmixed[rows, lanes[0]], mask)
        p = pt[rows, part(2 * duo + h, NB)]
        dp = nt(v, do).astype(BF16).astype(F32)
        pf = p.astype(F32)
        dot = jnp.sum(dp * pf, axis=0, keepdims=True)
        ds = (pf * (dp - dot) * 0.125).astype(BF16)
        dq = tn(ds, k)
        qkv[rows, lanes[0]] = jnp.where(mask, dq[:SEQ], dq[SEQ:]).astype(BF16)
        qkv[rows, lanes[1]] = nn(ds, split_heads(q, mask)).astype(BF16)
        qkv[rows, lanes[2]] = nn(p, do).astype(BF16)


def front_kernel(x0, cot, wq, wk, wv, wo, w1, w2,
                 n_out, qkv_out, pt_out, mx_out, nn_out, act_out, h0, pre0, xmid, dmix1, dpre1, dh1,
                 x, nrm, qkv, pt, mx, h, n2, big, g, acc, stg, ring, wsem, sems, stg_sem):
    def copy(n, src, dst):
        return pltpu.make_async_copy(src, dst, sems.at[n])

    cx, cg = copy(0, x0, x), copy(1, cot, g)
    cx.start()
    cg.start()
    begin([(None, wq.at[0])], ring, wsem, 0)
    cx.wait()
    rms_rows(x, nrm)

    def stage_copy(i, dst):
        slot = lax.rem(i, 2)
        return pltpu.make_async_copy(stg.at[slot], dst.at[:, part(i, D)], stg_sem.at[slot])

    def sums(stage_count, source, src, times, weight):
        def step(i, slot):
            for c in SUBS:
                for r in rows_of(512):
                    acc[r, c] = jnp.where(i == 0, 0.0, acc[r, c]) + times(src[r, part(i, D)], weight(slot, c))
        return Stage(stage_count, source, step)

    @pl.loop(0, 2)
    def _(l):
        first = l == 0
        outs = dict(n=copy(2, nrm, n_out.at[l]), qkv=copy(3, qkv, qkv_out.at[l]), pt=copy(4, pt, pt_out.at[l]),
                    mx=copy(5, mx, mx_out.at[l]), nn=copy(6, n2, nn_out.at[l]))
        only = dict(h=copy(7, h, h0), act=copy(8, big, act_out.at[0]))

        def qkv_step(i, slot):
            for j, c in enumerate(SUBS):
                for r in rows_of(256):
                    qkv[r, pl.ds(pl.multiple_of(i * D + j * NB, NB), NB)] = nn(nrm[r, :], ring[slot, :, c]).astype(BF16)

        def attend():
            outs["qkv"].start()
            attention_fwd(qkv, pt, mx)
            outs["pt"].start()
            outs["mx"].start()

        def proj_step(i, slot):
            for c in SUBS:
                y = nn(mx[...], ring[slot, :, c]).astype(BF16).astype(F32)
                h[:, c] = (x[:, c].astype(F32) + y).astype(BF16)

        def middle():
            rms_rows(h, n2)
            outs["nn"].start()
            pl.when(first)(only["h"].start)

        def up_step(i, slot):
            half = lax.rem(i, 2)
            pl.when(i >= 2)(stage_copy(i, pre0).wait)
            for j, c in enumerate(SUBS):
                for r in rows_of(128):
                    pre = nn(n2[r, :], ring[slot, :, c]).astype(BF16)
                    act = gelu(pre.astype(F32)).astype(BF16)
                    big[r, pl.ds(pl.multiple_of(i * D + j * NB, NB), NB)] = jnp.where(first, act, pre)
                    stg[half, r, c] = jnp.where(first, pre, act)
            pl.when(first)(stage_copy(i, pre0).start)
            pl.when(l == 1)(stage_copy(i, act_out.at[1]).start)

        outs["n"].start()
        run_stages([Stage(3, lambda i: [(i == m, w.at[l]) for m, w in enumerate((wq, wk, wv))], qkv_step), attend,
                    Stage(1, lambda i: [(None, wo.at[l])], proj_step), middle,
                    Stage(4, lambda i: [(None, w1.at[:, part(i, D)])], up_step)], ring, wsem, [(None, w2.at[pl.ds(0, D)])])
        for i in range(2):
            stage_copy(i, pre0).wait()

        @pl.when(first)
        def _():
            only["act"].start()
            run_stages([sums(4, lambda i: [(None, w2.at[part(i, D)])], big, nn, lambda slot, c: ring[slot, :, c])],
                       ring, wsem, [(None, wq.at[1])])
            for cp in (*outs.values(), *only.values()):
                cp.wait()
            add_rms_rows(h, acc, x, nrm)
            copy(9, x, xmid).start()

    def dact_step(i, slot):
        for j, c in enumerate(SUBS):
            to = pl.ds(pl.multiple_of(i * D + j * NB, NB), NB)
            for r in rows_of(256):
                d = nt(g[r, :], ring[slot, c]).astype(BF16).astype(F32)
                big[r, to] = gelu_grad(big[r, to].astype(F32), d).astype(BF16)

    def after_dact():
        copy(8, big, dpre1).start()

    def after_dn2():
        copy(9, x, xmid).wait()
        rms_back_rows(h, acc, g, x)
        copy(9, x, dh1).start()
        copy(2, nrm, n_out.at[1]).wait()

    def dmix_step(i, slot):
        for c in SUBS:
            nrm[:, c] = nt(x[...], ring[slot, c]).astype(BF16)

    cg.wait()
    run_stages([Stage(4, lambda i: [(None, w2.at[part(i, D)])], dact_step), after_dact,
                sums(4, lambda i: [(None, w1.at[:, part(i, D)])], big, nt, lambda slot, c: ring[slot, c]), after_dn2,
                Stage(1, lambda i: [(None, wo.at[1])], dmix_step)], ring, wsem)
    copy(2, nrm, dmix1).start()
    for n, src, dst in ((2, nrm, dmix1), (3, qkv, qkv_out.at[1]), (4, pt, pt_out.at[1]), (5, mx, mx_out.at[1]),
                        (6, n2, nn_out.at[1]), (8, big, dpre1), (9, x, dh1)):
        copy(n, src, dst).wait()


TD, T3, TF, TP = (TOK, D), (TOK, 3 * D), (TOK, FF), (TOK, PAIRS * NB)


def front(x0, cot, *weights):
    both = [(2,) + s for s in (TD, T3, TP, TD, TD, TF)]
    outs = both + [TD, TF, TD, TD, TF, TD]
    vmem = [pltpu.VMEM(s, BF16) for s in (TD, TD, T3, TP, TD, TD, TD, TF, TD)]
    return pl.pallas_call(
        front_kernel,
        out_shape=[jax.ShapeDtypeStruct(s, BF16) for s in outs],
        in_specs=[ANY] * (2 + len(weights)),
        out_specs=[ANY] * len(outs),
        scratch_shapes=vmem + [pltpu.VMEM(TD, F32), pltpu.VMEM((2, TOK, D), BF16), pltpu.VMEM((2, D, D), BF16),
                               pltpu.SemaphoreType.DMA((2,)), pltpu.SemaphoreType.DMA((10,)), pltpu.SemaphoreType.DMA((2,))],
        compiler_params=pltpu.CompilerParams(vmem_limit_bytes=VMEM_MOST),
        name="front",
    )(x0, cot, *weights)


MESH = pl.DeviceIdType.MESH
ROWS, LANES = 40, 128
OFFSETS = (1, 3, 5, 7)
LAST = OFFSETS[3] + 1
ORDERS = ("xyz", "yzx", "zxy")
CUBE = (2, 2, 2)
HEADS, MLP = 1, 2
N_OUT = (1, 2, 4)


def scatter_kernel(groups, n_tiles, n_src, n_after, chain, layer_in, spread, *refs):
    srcs, refs = refs[:n_src], refs[n_src + n_after:]
    out_ref, more, refs = refs[0], refs[1:N_OUT[chain]], refs[N_OUT[chain]:]
    a_buf, b_buf, tiles, own, rc, r1, r2, r3, a_sem, b_sem, out_sem, send_sem, recv_sem, *refs = refs
    heads, mlp, depth = chain == HEADS, chain == MLP, len(groups[0][1])
    if spread:
        all_send, all_recv = refs
    if chain:
        xb, gb, tb, acc, wring, w_sem, at_sem, big, *refs = refs
    if heads:
        (qkv, head_sem), pt = refs, big
        _, _, _, dmixed_in, qkv_in, pt_in, x_in, d_in, wq, wk, wv = srcs
        qkv_in, pt_in = qkv_in.at[layer_in], pt_in.at[layer_in]
    if mlp:
        _, _, _, h_in, pre_in, d_in, wo, w1, w2 = srcs
    me = lax.axis_index("data")
    bit, peer = {}, {}
    for n, d in enumerate("cxyz"):
        bit[d] = lax.rem(me // 2 ** n, 2)
        peer[d] = me + 2 ** n * (1 - 2 * bit[d])
    n_own, n_in, ring = own.shape[1], rc.shape[1], tiles.shape[0]
    n_chunks = 4 * n_tiles
    bufs = (rc, r1, r2, r3)

    def group_of(m):
        a = 0
        for first in groups[1:]:
            a = a + (m >= first[0]).astype(jnp.int32)
        return a

    def source(spec):
        n, layer = spec
        return srcs[n] if layer is None else srcs[n].at[layer]

    def a_load(a, layer):
        _, ins, col, _, _ = groups[a]
        return pltpu.make_async_copy(source(ins[layer]).at[:, pl.ds(col, D)], a_buf.at[a % 2, layer], a_sem.at[a % 2, layer])

    def b_load(a, m, layer, ahead=True):
        first, _, _, ins, col = groups[a]
        if ahead:
            col = pl.multiple_of(col + (m - first) * NB, NB)
        slot = lax.rem(m, 2)
        return pltpu.make_async_copy(source(ins[layer]).at[:, pl.ds(col, NB)], b_buf.at[slot, layer], b_sem.at[slot, layer])

    def in_group(a, m, fn):
        last = groups[a + 1][0] if a + 1 < len(groups) else n_tiles

        @pl.when(jnp.logical_and(m >= groups[a][0], m < last))
        def _():
            fn()

    def b_start(m):
        for a in range(len(groups)):
            if groups[a][3] is None:
                continue

            def go(a=a):
                for layer in range(depth):
                    b_load(a, m, layer).start()
            in_group(a, m, go)

    def produce(m):
        half, slot, to = lax.rem(group_of(m), 2), lax.rem(m, 2), lax.rem(m, ring)

        @pl.when(m < (DB if heads else n_tiles))
        def _():
            for layer in range(depth):
                b_load(0, m, layer, False).wait()
        if heads:
            @pl.when(m >= DB)
            def _():
                b_buf[slot, 0] = qkv[:, pl.ds(pl.multiple_of(lax.rem(m - DB, 3) * D + ((m - DB) // 3) * NB, NB), NB)]
        for a in range(len(groups)):
            @pl.when(m == groups[a][0])
            def _():
                for layer in range(depth):
                    a_load(a, layer).wait()
                if a + 1 < len(groups):
                    for layer in range(depth):
                        a_load(a + 1, layer).start()
        b_start(m + 1)

        for z in range(2):
            tot = None
            for layer in range(depth):
                y = tn(a_buf[half, layer, :, part(z, D // 2)], b_buf[slot, layer])
                tot = y if tot is None else tot + y
            tiles[to, z] = tot.reshape(CUBE + (2 * ROWS, NB))

    def pick(color, stage, other):
        idx = {d: slice(None) for d in "zyx"}
        for s in range(stage):
            d = ORDERS[color][s]
            idx[d] = 1 - bit[d] if (other and s == stage - 1) else bit[d]
        return tuple(idx[d] for d in "zyx")

    def piece(k):
        sub = lax.rem(k, 4)
        return (lax.rem(k // 4, ring), pl.multiple_of(lax.rem(sub, 2) * ROWS, 8), pl.multiple_of((sub // 2) * LANES, LANES))

    def send(color, stage, j):
        slot, so = lax.rem(j, n_in), lax.rem(j, n_own)
        if stage == 0:
            tile, row, col = piece(3 * j + color)
            src, to = tiles.at[tile, :, :, :, 1 - bit["c"], pl.ds(row, ROWS), pl.ds(col, LANES)], peer["c"]
        else:
            src, to = own.at[(color, so) + pick(color, stage, True)], peer[ORDERS[color][stage - 1]]
        return pltpu.make_async_remote_copy(src, bufs[stage].at[color, slot], send_sem.at[color, stage, slot],
                                            recv_sem.at[color, stage, slot], device_id=(to,), device_id_type=MESH)

    def place(color, j):
        k = 3 * j + color
        _, row, col = piece(k)
        tile = k // 4
        if heads:
            tile = jnp.where(tile < DB, tile, DB + DB * lax.rem(tile - DB, 3) + (tile - DB) // 3)
        return pl.ds(row, ROWS), pl.ds(pl.multiple_of(tile * NB + col, LANES), LANES)

    def store(color, j):
        so = lax.rem(j, n_own)
        where = place(color, j)
        if spread:
            where = (bit["z"], bit["y"], bit["x"], bit["c"]) + where
        return pltpu.make_async_copy(own.at[(color, so) + pick(color, 3, False)], out_ref.at[where], out_sem.at[color, so])

    def hand_on(color, stage, j):
        slot, so = lax.rem(j, n_in), lax.rem(j, n_own)
        idx = {d: bit[d] for d in "zyxc"}
        for d in ORDERS[color][3 - stage:]:
            idx[d] = slice(None)
        dst = out_ref.at[(idx["z"], idx["y"], idx["x"], idx["c"]) + place(color, j)]
        src = dst if stage else own.at[(color, so) + pick(color, 3, False)]
        to = peer[ORDERS[color][2 - stage] if stage < 3 else "c"]
        return pltpu.make_async_remote_copy(src, dst, all_send.at[color, stage, slot], all_recv.at[color, stage, slot],
                                            device_id=(to,), device_id_type=MESH)

    def live(j, color):
        return jnp.logical_and(j >= 0, 3 * j + color < n_chunks)

    up_from, norm_at, end = FB, 2 * FB, 2 * FB + 1 + DB

    def w_begin(w):
        slot = lax.rem(w, 3)
        begin([(w < up_from, w2.at[part(w, NB)]),
               (jnp.logical_and(w >= up_from, w < norm_at), w1.at[part(lax.rem(w, DB), NB), part((w - up_from) // DB, D)]),
               (jnp.logical_and(w >= norm_at, w < end - 1), wo.at[layer_in, part(lax.rem(w, DB), NB)])], wring, w_sem, slot)

    def w_take(w):
        slot = lax.rem(w, 3)
        pltpu.make_async_copy(wo.at[0, pl.ds(0, NB)], wring.at[slot], w_sem.at[slot]).wait()
        w_begin(w + 2)
        return slot

    def head_weights(duo):
        col = pl.multiple_of(duo * NB, NB)
        base = 3 * lax.rem(duo, 2)
        return [pltpu.make_async_copy(ref.at[layer_in, :, pl.ds(col, NB)], wring.at[base + m], w_sem.at[base + m])
                for m, ref in enumerate((wq, wk, wv))]

    def start(*names):
        for name in names:
            copies[name].start()

    def wait(*names):
        for name in names:
            copies[name].wait()

    if chain:
        if heads:
            table = dict(x=(x_in, xb), d=(d_in, tb), first=(gb, *more))
        else:
            table = dict(d=(d_in, gb), h=(h_in, xb), pre=(pre_in, big), dpre=(big, more[0]), dh=(tb, more[1]), dmix=(xb, more[2]))
        copies = {name: pltpu.make_async_copy(src, dst, at_sem.at[n]) for n, (name, (src, dst)) in enumerate(table.items())}

    def head_loads(duo):
        cols = [pl.ds(n * D + duo * NB, NB) for n in range(3)]
        pairs = [(dmixed_in, xb, cols[0]), (pt_in, pt, pl.ds(duo * 2 * NB, 2 * NB))] + [(qkv_in, qkv, c) for c in cols]
        return [pltpu.make_async_copy(src.at[:, c], dst.at[:, c], head_sem.at[duo, n]) for n, (src, dst, c) in enumerate(pairs)]

    def input_step(duo, turn):
        @pl.when(turn == 0)
        def _():
            for copy in head_weights(duo):
                copy.wait()

            @pl.when(duo < DB - 1)
            def _():
                for copy in head_weights(duo + 1):
                    copy.start()
        base = 3 * lax.rem(duo, 2)

        @pl.loop(jnp.where(turn == 0, 0, turn + 1), turn + 2)
        def _(n):
            c = part(n, NB)
            tot = jnp.where(duo == 0, 0.0, acc[:, c])
            for m in range(3):
                tot = tot + nt(qkv[:, pl.ds(pl.multiple_of(m * D + duo * NB, NB), NB)], wring[base + m, c])
            acc[:, c] = tot

    def sum_step(g, src, slot):
        c, m = part(lax.rem(g, DB), NB), g // DB

        for r in rows_of(512):
            acc[r, c] = jnp.where(m == 0, 0.0, acc[r, c]) + nt(src[r, part(m, D)], wring[slot])

    def mlp_step(g):
        @pl.when(g == 0)
        def _():
            wait("d", "pre")

        @pl.when(g < up_from)
        def _():
            slot, c = w_take(g), part(g, NB)

            for r in rows_of(256):
                d = nt(gb[r, :], wring[slot]).astype(BF16).astype(F32)
                big[r, c] = gelu_grad(big[r, c].astype(F32), d).astype(BF16)

        @pl.when(g == up_from)
        def _():
            start("dpre")

        @pl.when(jnp.logical_and(g >= up_from, g < norm_at))
        def _():
            sum_step(g - up_from, big, w_take(g))

        @pl.when(g == norm_at)
        def _():
            wait("h")
            rms_back_rows(xb, acc, gb, tb)
            start("dh")

        @pl.when(jnp.logical_and(g > norm_at, g < end))
        def _():
            slot, c = w_take(g - 1), part(g - norm_at - 1, NB)

            for r in rows_of(512):
                xb[r, c] = nt(tb[r, :], wring[slot]).astype(BF16)

        @pl.when(g == end - 1)
        def _():
            start("dmix")

    def tick(t, carry):
        for stage in (3, 2, 1, 0) if spread else ():
            j = t - OFFSETS[3] - 2 * (stage + 1)
            for color in range(3):
                @pl.when(live(j, color))
                def _():
                    copy = hand_on(color, stage, j)
                    copy.wait_send()
                    copy.wait_recv()
                    if stage == 0:
                        store(color, j).wait()
                    if stage < 3:
                        hand_on(color, stage + 1, j).start()
        for color in () if spread else range(3):
            j = t - LAST

            @pl.when(live(j, color))
            def _():
                store(color, j).wait()
        for stage in (3, 2, 1, 0):
            j = t - OFFSETS[stage]
            for color in range(3):
                @pl.when(live(j, color))
                def _():
                    slot, so = lax.rem(j, n_in), lax.rem(j, n_own)
                    copy = send(color, stage, j)
                    copy.wait_send()
                    copy.wait_recv()
                    keep = (color, so) + pick(color, stage, False)
                    if stage == 0:
                        tile, row, col = piece(3 * j + color)
                        mine = tiles[tile, :, :, :, bit["c"], pl.ds(row, ROWS), pl.ds(col, LANES)]
                    else:
                        mine = own[keep]
                    own[keep] = mine + bufs[stage][color, slot]
                    if stage < 3:
                        send(color, stage + 1, j).start()
                    else:
                        store(color, j).start()
                        if spread:
                            hand_on(color, 0, j).start()
        for color in range(3):
            @pl.when(live(t, color))
            def _():
                send(color, 0, t).start()
        if heads:
            for duo in range(DB):
                @pl.when(t == 1 + 4 * duo)
                def _():
                    for copy in head_loads(duo):
                        copy.wait()

            @pl.when(jnp.logical_and(t > 0, t <= 4 * DB))
            def _():
                for u in range(2):
                    attention_bwd(2 * lax.rem(t - 1, 4) + u, (t - 1) // 4, qkv, pt, xb)
        m = (3 * t + 5) // 4

        @pl.when(jnp.logical_and(m != (3 * t + 2) // 4, m < n_tiles))
        def _():
            produce(m)
        if heads:
            first_tick, last_attend = DB, 4 * DB
            since = t - first_tick
            quarter = jnp.where(t > last_attend, since - last_attend // 2 + 2, since // 2)
            norm_tick = first_tick + last_attend + last_attend // 2 - 2

            @pl.when(jnp.logical_and(jnp.logical_and(since >= 0, t < norm_tick), jnp.logical_or(t > last_attend, lax.rem(since, 2) == 0)))
            def _():
                input_step(quarter // 4, lax.rem(quarter, 4))

            @pl.when(t == last_attend + 1)
            def _():
                start("x")

            @pl.when(t == norm_tick)
            def _():
                wait("x", "d")
                rms_back_rows(xb, acc, tb, gb)
                start("first")
        if mlp:
            @pl.when(2 * t < end)
            def _():
                @pl.loop(0, 2)
                def _(u):
                    mlp_step(2 * t + u)
        return carry

    for layer in range(depth):
        a_load(0, layer).start()
    b_start(jnp.int32(0))
    if heads:
        for duo in range(DB):
            for copy in head_loads(duo):
                copy.start()
        for copy in head_weights(jnp.int32(0)):
            copy.start()
        start("d")
    if mlp:
        start("d", "pre", "h")
        for n in range(2):
            w_begin(jnp.int32(n))
    barrier = pltpu.get_barrier_semaphore()
    for d in "cxyz":
        pl.semaphore_signal(barrier, inc=1, device_id=(peer[d],), device_id_type=MESH)
    pl.semaphore_wait(barrier, 4)
    produce(jnp.int32(0))
    ticks = pl.cdiv(n_chunks, 3) + LAST + 8 * spread
    lax.fori_loop(0, ticks, tick, 0)
    if heads:
        wait("first")
    if mlp:
        wait("dpre", "dh", "dmix")


def scatter_sum(srcs, groups, n_tiles, collective_id, after=(), chain=0, layer=0, spread=False):
    depth = len(groups[0][1])
    n_own, n_in, blk = LAST + 1 + spread, 4, (ROWS, LANES)
    size = D * NB * n_tiles * 4
    outs = [(), (TD,), (TF, TD, TD)][chain]
    sums = (CUBE + (2,)) * spread + (2 * ROWS, NB * n_tiles)
    args = (*srcs, *after)
    dma = pltpu.SemaphoreType.DMA
    scratch = [
        pltpu.VMEM((2, depth, TOK, D), BF16), pltpu.VMEM((2, depth, TOK, NB), BF16), pltpu.VMEM((n_in, 2) + CUBE + (2 * ROWS, NB), F32),
        pltpu.VMEM((3, n_own) + CUBE + blk, F32)] + [pltpu.VMEM((3, n_in) + CUBE[n:] + blk, F32) for n in range(4)] + [
        dma((2, depth)), dma((2, depth)), dma((3, n_own)), dma((3, 4, n_in)), dma((3, 4, n_in))]
    if spread:
        scratch += [dma((3, 4, n_in))] * 2
    if chain:
        scratch += [pltpu.VMEM(TD, BF16)] * 3 + [
            pltpu.VMEM(TD, F32), pltpu.VMEM((6, D, NB) if chain == HEADS else (3, NB, D), BF16), dma((6,)), dma((6,))]
        scratch += [pltpu.VMEM(TP, BF16), pltpu.VMEM(T3, BF16), dma((DB, DB))] if chain == HEADS else [pltpu.VMEM(TF, BF16)]
    return pl.pallas_call(
        functools.partial(scatter_kernel, groups, n_tiles, len(srcs), len(after), chain, layer, spread),
        out_shape=[jax.ShapeDtypeStruct(sums, F32)] + [jax.ShapeDtypeStruct(o, BF16) for o in outs],
        in_specs=[ANY] * len(args),
        out_specs=[ANY] * (1 + len(outs)),
        scratch_shapes=scratch,
        compiler_params=pltpu.CompilerParams(collective_id=collective_id, has_side_effects=True, vmem_limit_bytes=VMEM_MOST),
        cost_estimate=pl.CostEstimate(flops=size * 4000, bytes_accessed=2 * size, transcendentals=0),
        name=f"scatter_sum_{collective_id}",
    )(*args)


def gather(shard):
    return lax.all_gather(shard, "data", axis=0, tiled=True)


def place_attention(full, layer, dst, carry, after):
    rows, part = 160, TOK * 160 // D

    def kernel(src, *refs):
        outs = refs[-4 - len(carry):]
        for n, out in zip((1, 2, 3, 0), outs):
            out[0] = src[:, n * D:(n + 1) * D]
        for ref, out in zip(refs, outs[4:]):
            out[...] = ref[...]

    strip = pl.BlockSpec((part, D), lambda i: (i, 0))
    return pl.pallas_call(
        kernel,
        grid=(D // rows,),
        out_shape=[jax.ShapeDtypeStruct((2, D, D), F32)] * 4 + [jax.ShapeDtypeStruct((TOK, D), BF16)] * len(carry),
        in_specs=[pl.BlockSpec((rows, 4 * D), lambda i: (i, 0))] + [strip] * len(carry) + [ANY] * (len(dst) + len(after)),
        out_specs=[pl.BlockSpec((1, rows, D), lambda i: (layer, i, 0))] * 4 + [strip] * len(carry),
        input_output_aliases={n + 1 + len(carry): n for n in range(len(dst))},
        compiler_params=pltpu.CompilerParams(vmem_limit_bytes=60 << 20),
        cost_estimate=pl.CostEstimate(flops=D * D, bytes_accessed=32 * D * D, transcendentals=0),
        name=f"place_attention_{layer}",
    )(full, *carry, *dst, *after)


def place_blocks(full, shape, where, dst, after, name):
    rows = 640
    per, blocks = D // rows, full.shape[1] // D

    def to(n, i):
        row, col = where(n)
        return row * per + i, col

    def kernel(src, *refs):
        refs[-1][...] = src[...]

    return pl.pallas_call(
        kernel,
        grid=(blocks, per),
        out_shape=jax.ShapeDtypeStruct(shape, F32),
        in_specs=[pl.BlockSpec((rows, D), lambda n, i: (i, n))] + [ANY] * (len(dst) + len(after)),
        out_specs=pl.BlockSpec((rows, D), to),
        input_output_aliases={1: 0} if dst else {},
        compiler_params=pltpu.CompilerParams(vmem_limit_bytes=60 << 20),
        cost_estimate=pl.CostEstimate(flops=D * D, bytes_accessed=8 * blocks * D * D, transcendentals=0),
        name=name,
    )(full, *dst, *after)


def solution(mesh):
    def local_step(x_init, cot_out, w_query, w_key, w_value, w_proj, w_up, w_down):
        cot, x0 = cot_out.reshape(TD), x_init.reshape(TD)
        (nrm, qkv, pt, mx, nn2, act, h0, pre0, xmid, dmix1, dpre1, dh1) = front(x0, cot, w_query, w_key, w_value, w_proj, w_up, w_down)
        w_in = (w_query, w_key, w_value)
        both, ends = ((0, 0), (0, 1)), ((1, None), (2, None))

        def attention(layer, d_hidden, d_mixed, x_in, number, after):
            groups = ((0, ((0, layer),), 0, ((1, None),), 0), (DB, ((2, layer),), 0, None, 0))
            srcs = (mx, d_hidden, nrm, d_mixed, qkv, pt, x_in, d_hidden, *w_in)
            return scatter_sum(srcs, groups, 4 * DB, number, after, chain=HEADS, layer=layer)

        down = [tuple((DB * n, both, q * D, ends, 0) for n, q in enumerate(qs)) for qs in ((0, 1, 2), (3,))]
        shard1, dmid = attention(1, dh1, dmix1, xmid, 1, ())
        full1 = gather(shard1)
        shard_a, dpre0, dh0, dmix0 = scatter_sum(
            (act, dmid, cot, h0, pre0, dmid, w_proj, w_up, w_down), down[0], 3 * DB, 2, (shard1,), chain=MLP)
        full_a = gather(shard_a)
        shard0, dx = attention(0, dh0, dmix0, x0, 3, (shard_a,))
        full0 = gather(shard0)
        shard_up, = scatter_sum((nn2, dpre0, dpre1), ((0, both, 0, ends, 0),), FB, 4, (shard0,))
        full_up = gather(shard_up)
        shard_b, = scatter_sum((act, dmid, cot), down[1], DB, 5, (shard_up,), spread=True)
        half = place_attention(full1, 1, (), (), (shard_b,))
        g_down = place_blocks(full_a, (FF, D), lambda n: (n, 0), (), (half[0],), "place_down_0")
        g_down = place_blocks(shard_b.reshape(D, D), (FF, D), lambda n: (3, 0), (g_down,), (), "place_down_3")
        *attn, dx = place_attention(full0, 0, half, (dx,), (g_down,))
        g_up = place_blocks(full_up, (D, FF), lambda n: (0, n), (), (attn[0],), "place_up")
        return (*attn, g_up, g_down, dx.reshape(x_init.shape))

    data_spec = P("data")
    full_spec = P()
    in_specs = (data_spec, data_spec) + (full_spec,) * 6
    out_specs = (full_spec,) * 6 + (data_spec,)
    return jax.shard_map(local_step, mesh=mesh, in_specs=in_specs, out_specs=out_specs, check_vma=False)
```

```python
import functools

import jax
import jax.numpy as jnp
from jax import lax
from jax.experimental import pallas as pl
from jax.experimental.pallas import tpu as pltpu
from jax.sharding import PartitionSpec as P

EPS = 1e-6
F32, BF16 = jnp.float32, jnp.bfloat16
TOK, D, FF, SEQ = 1024, 1280, 5120, 128
NB = 256
DB, FB = D // NB, FF // NB
PAIRS = 10
VMEM_MOST = 67043328
SUBS = [pl.ds(j * NB, NB) for j in range(DB)]
ANY = pl.BlockSpec(memory_space=pl.ANY)
C0 = 0.7978845608028654
C1 = C0 * 0.044715


def nn(a, b):
    return lax.dot_general(a, b, (((1,), (0,)), ((), ())), preferred_element_type=F32)


def nt(a, b):
    return lax.dot_general(a, b, (((1,), (1,)), ((), ())), preferred_element_type=F32)


def tn(a, b):
    return lax.dot_general(a, b, (((0,), (0,)), ((), ())), preferred_element_type=F32)


def part(i, width):
    return pl.ds(pl.multiple_of(i * width, 128), width)


def rows_of(size):
    return [pl.ds(k * size, size) for k in range(TOK // size)]


class Stage:
    def __init__(self, count, source, step):
        self.count, self.source, self.step = count, source, step


def begin(sources, ring, sem, slot):
    for cond, src in sources:
        copy = pltpu.make_async_copy(src, ring.at[slot], sem.at[slot])
        if cond is None:
            copy.start()
        else:
            pl.when(cond)(copy.start)


def run_stages(items, ring, sem, follow=()):
    stages = [it for it in items if isinstance(it, Stage)]
    base = 0
    for it in items:
        if not isinstance(it, Stage):
            it()
            continue
        after = stages[stages.index(it) + 1].source(0) if it is not stages[-1] else follow

        def one(i, it=it, base=base, after=after):
            slot = lax.rem(base + i, 2)
            pltpu.make_async_copy(it.source(0)[0][1], ring.at[slot], sem.at[slot]).wait()
            other = lax.rem(base + i + 1, 2)

            @pl.when(i + 1 < it.count)
            def _():
                begin(it.source(i + 1), ring, sem, other)

            @pl.when(i + 1 >= it.count)
            def _():
                begin(after, ring, sem, other)
            it.step(i, slot)

        pl.loop(0, it.count)(one)
        base += it.count


def gelu(x):
    half = 0.5 * x
    return half * jnp.tanh(x * (C0 + C1 * (x * x))) + half


def gelu_grad(x, d):
    x2 = x * x
    t = jnp.tanh(x * (C0 + C1 * x2))
    return d * ((0.5 + 0.5 * t) + ((1.0 - t * t) * x) * (0.5 * C0 + 1.5 * C1 * x2))


def by_rows(fn, rows=256):
    @pl.loop(0, TOK // rows)
    def _(i):
        fn(part(i, rows))


def inverse_rms(x):
    return lax.rsqrt(jnp.mean(x * x, axis=-1, keepdims=True) + EPS)


def rms_rows(src, dst):
    def one(r):
        x = src[r, :].astype(F32)
        dst[r, :] = (x * inverse_rms(x)).astype(BF16)
    by_rows(one)


def add_rms_rows(res, acc, out, dst):
    def one(r):
        y = (res[r, :].astype(F32) + acc[r, :].astype(BF16).astype(F32)).astype(BF16)
        out[r, :] = y
        x = y.astype(F32)
        dst[r, :] = (x * inverse_rms(x)).astype(BF16)
    by_rows(one)


def rms_back_rows(x_ref, dy_acc, dres_ref, dst):
    def one(r):
        x = x_ref[r, :].astype(F32)
        dy = dy_acc[r, :].astype(BF16).astype(F32)
        inv = inverse_rms(x)
        dot = jnp.mean(dy * x, axis=-1, keepdims=True)
        dst[r, :] = (dres_ref[r, :].astype(F32) + (dy * inv - x * (inv * inv * inv * dot))).astype(BF16)
    by_rows(one)


def lane_mask():
    return lax.broadcasted_iota(jnp.int32, (SEQ, 2 * 64), 1) < 64


def split_heads(x, mask):
    zero = jnp.zeros_like(x)
    return jnp.concatenate([jnp.where(mask, x, zero), jnp.where(mask, zero, x)], axis=0)


def split_heads_t(x):
    y = x.T
    top = lax.broadcasted_iota(jnp.int32, y.shape, 0) < 64
    zero = jnp.zeros_like(y)
    return jnp.concatenate([jnp.where(top, y, zero), jnp.where(top, zero, y)], axis=1)


def attention_fwd(qkv, pt, mixed):
    mask = lane_mask()

    def one(rows):
        for h in range(PAIRS):
            q, k, v = (qkv[rows, pl.ds(n * D + h * SEQ, SEQ)] for n in range(3))
            st = nn(k, split_heads_t(q)) * 0.125
            e = jnp.exp(st - jnp.max(st, axis=0, keepdims=True))
            p = (e / jnp.sum(e, axis=0, keepdims=True)).astype(BF16)
            pt[rows, pl.ds(h * NB, NB)] = p
            o = tn(p, v)
            mixed[rows, pl.ds(h * SEQ, SEQ)] = jnp.where(mask, o[:SEQ], o[SEQ:]).astype(BF16)
    by_rows(one, SEQ)


def attention_bwd(s, duo, qkv, pt, dmixed):
    mask = lane_mask()
    rows = part(s, SEQ)
    for h in range(2):
        lanes = [pl.ds(pl.multiple_of(n * D + duo * NB + h * SEQ, SEQ), SEQ) for n in range(3)]
        q, k, v = (qkv[rows, c] for c in lanes)
        do = split_heads(dmixed[rows, lanes[0]], mask)
        p = pt[rows, part(2 * duo + h, NB)]
        dp = nt(v, do).astype(BF16).astype(F32)
        pf = p.astype(F32)
        dot = jnp.sum(dp * pf, axis=0, keepdims=True)
        ds = (pf * (dp - dot) * 0.125).astype(BF16)
        dq = tn(ds, k)
        qkv[rows, lanes[0]] = jnp.where(mask, dq[:SEQ], dq[SEQ:]).astype(BF16)
        qkv[rows, lanes[1]] = nn(ds, split_heads(q, mask)).astype(BF16)
        qkv[rows, lanes[2]] = nn(p, do).astype(BF16)


def front_kernel(x0, cot, wq, wk, wv, wo, w1, w2,
                 n_out, qkv_out, pt_out, mx_out, nn_out, act_out, h0, pre0, xmid, dmix1, dpre1, dh1,
                 x, nrm, qkv, pt, mx, h, n2, big, g, acc, stg, ring, wsem, sems, stg_sem):
    def copy(n, src, dst):
        return pltpu.make_async_copy(src, dst, sems.at[n])

    cx, cg = copy(0, x0, x), copy(1, cot, g)
    cx.start()
    cg.start()
    begin([(None, wq.at[0])], ring, wsem, 0)
    cx.wait()
    rms_rows(x, nrm)

    def stage_copy(i, dst):
        slot = lax.rem(i, 2)
        return pltpu.make_async_copy(stg.at[slot], dst.at[:, part(i, D)], stg_sem.at[slot])

    def sums(stage_count, source, src, times, weight):
        def step(i, slot):
            for c in SUBS:
                for r in rows_of(512):
                    acc[r, c] = jnp.where(i == 0, 0.0, acc[r, c]) + times(src[r, part(i, D)], weight(slot, c))
        return Stage(stage_count, source, step)

    @pl.loop(0, 2)
    def _(l):
        first = l == 0
        outs = dict(n=copy(2, nrm, n_out.at[l]), qkv=copy(3, qkv, qkv_out.at[l]), pt=copy(4, pt, pt_out.at[l]),
                    mx=copy(5, mx, mx_out.at[l]), nn=copy(6, n2, nn_out.at[l]))
        only = dict(h=copy(7, h, h0), act=copy(8, big, act_out.at[0]))

        def qkv_step(i, slot):
            for j, c in enumerate(SUBS):
                for r in rows_of(256):
                    qkv[r, pl.ds(pl.multiple_of(i * D + j * NB, NB), NB)] = nn(nrm[r, :], ring[slot, :, c]).astype(BF16)

        def attend():
            outs["qkv"].start()
            attention_fwd(qkv, pt, mx)
            outs["pt"].start()
            outs["mx"].start()

        def proj_step(i, slot):
            for c in SUBS:
                y = nn(mx[...], ring[slot, :, c]).astype(BF16).astype(F32)
                h[:, c] = (x[:, c].astype(F32) + y).astype(BF16)

        def middle():
            rms_rows(h, n2)
            outs["nn"].start()
            pl.when(first)(only["h"].start)

        def up_step(i, slot):
            half = lax.rem(i, 2)
            pl.when(i >= 2)(stage_copy(i, pre0).wait)
            for j, c in enumerate(SUBS):
                for r in rows_of(128):
                    pre = nn(n2[r, :], ring[slot, :, c]).astype(BF16)
                    act = gelu(pre.astype(F32)).astype(BF16)
                    big[r, pl.ds(pl.multiple_of(i * D + j * NB, NB), NB)] = jnp.where(first, act, pre)
                    stg[half, r, c] = jnp.where(first, pre, act)
            pl.when(first)(stage_copy(i, pre0).start)
            pl.when(l == 1)(stage_copy(i, act_out.at[1]).start)

        outs["n"].start()
        run_stages([Stage(3, lambda i: [(i == m, w.at[l]) for m, w in enumerate((wq, wk, wv))], qkv_step), attend,
                    Stage(1, lambda i: [(None, wo.at[l])], proj_step), middle,
                    Stage(4, lambda i: [(None, w1.at[:, part(i, D)])], up_step)], ring, wsem, [(None, w2.at[pl.ds(0, D)])])
        for i in range(2):
            stage_copy(i, pre0).wait()

        @pl.when(first)
        def _():
            only["act"].start()
            run_stages([sums(4, lambda i: [(None, w2.at[part(i, D)])], big, nn, lambda slot, c: ring[slot, :, c])],
                       ring, wsem, [(None, wq.at[1])])
            for cp in (*outs.values(), *only.values()):
                cp.wait()
            add_rms_rows(h, acc, x, nrm)
            copy(9, x, xmid).start()

    def dact_step(i, slot):
        for j, c in enumerate(SUBS):
            to = pl.ds(pl.multiple_of(i * D + j * NB, NB), NB)
            for r in rows_of(256):
                d = nt(g[r, :], ring[slot, c]).astype(BF16).astype(F32)
                big[r, to] = gelu_grad(big[r, to].astype(F32), d).astype(BF16)

    def after_dact():
        copy(8, big, dpre1).start()

    def after_dn2():
        copy(9, x, xmid).wait()
        rms_back_rows(h, acc, g, x)
        copy(9, x, dh1).start()
        copy(2, nrm, n_out.at[1]).wait()

    def dmix_step(i, slot):
        for c in SUBS:
            nrm[:, c] = nt(x[...], ring[slot, c]).astype(BF16)

    cg.wait()
    run_stages([Stage(4, lambda i: [(None, w2.at[part(i, D)])], dact_step), after_dact,
                sums(4, lambda i: [(None, w1.at[:, part(i, D)])], big, nt, lambda slot, c: ring[slot, c]), after_dn2,
                Stage(1, lambda i: [(None, wo.at[1])], dmix_step)], ring, wsem)
    copy(2, nrm, dmix1).start()
    for n, src, dst in ((2, nrm, dmix1), (3, qkv, qkv_out.at[1]), (4, pt, pt_out.at[1]), (5, mx, mx_out.at[1]),
                        (6, n2, nn_out.at[1]), (8, big, dpre1), (9, x, dh1)):
        copy(n, src, dst).wait()


TD, T3, TF, TP = (TOK, D), (TOK, 3 * D), (TOK, FF), (TOK, PAIRS * NB)


def front(x0, cot, *weights):
    both = [(2,) + s for s in (TD, T3, TP, TD, TD, TF)]
    outs = both + [TD, TF, TD, TD, TF, TD]
    vmem = [pltpu.VMEM(s, BF16) for s in (TD, TD, T3, TP, TD, TD, TD, TF, TD)]
    return pl.pallas_call(
        front_kernel,
        out_shape=[jax.ShapeDtypeStruct(s, BF16) for s in outs],
        in_specs=[ANY] * (2 + len(weights)),
        out_specs=[ANY] * len(outs),
        scratch_shapes=vmem + [pltpu.VMEM(TD, F32), pltpu.VMEM((2, TOK, D), BF16), pltpu.VMEM((2, D, D), BF16),
                               pltpu.SemaphoreType.DMA((2,)), pltpu.SemaphoreType.DMA((10,)), pltpu.SemaphoreType.DMA((2,))],
        compiler_params=pltpu.CompilerParams(vmem_limit_bytes=VMEM_MOST),
        name="front",
    )(x0, cot, *weights)


MESH = pl.DeviceIdType.MESH
ROWS, LANES = 40, 128
OFFSETS = (1, 3, 5, 7)
LAST = OFFSETS[3] + 1
ORDERS = ("xyz", "yzx", "zxy")
CUBE = (2, 2, 2)
HEADS, MLP = 1, 2
N_OUT = (1, 2, 4)


def scatter_kernel(groups, n_tiles, n_src, n_after, chain, layer_in, spread, *refs):
    srcs, refs = refs[:n_src], refs[n_src + n_after:]
    out_ref, more, refs = refs[0], refs[1:N_OUT[chain]], refs[N_OUT[chain]:]
    a_buf, b_buf, tiles, own, rc, r1, r2, r3, a_sem, b_sem, out_sem, send_sem, recv_sem, *refs = refs
    heads, mlp, depth = chain == HEADS, chain == MLP, len(groups[0][1])
    if spread:
        all_send, all_recv = refs
    if chain:
        xb, gb, tb, acc, wring, w_sem, at_sem, big, *refs = refs
    if heads:
        (qkv, head_sem), pt = refs, big
        _, _, _, dmixed_in, qkv_in, pt_in, x_in, d_in, wq, wk, wv = srcs
        qkv_in, pt_in = qkv_in.at[layer_in], pt_in.at[layer_in]
    if mlp:
        _, _, _, h_in, pre_in, d_in, wo, w1, w2 = srcs
    me = lax.axis_index("data")
    bit, peer = {}, {}
    for n, d in enumerate("cxyz"):
        bit[d] = lax.rem(me // 2 ** n, 2)
        peer[d] = me + 2 ** n * (1 - 2 * bit[d])
    n_own, n_in, ring = own.shape[1], rc.shape[1], tiles.shape[0]
    n_chunks = 4 * n_tiles
    bufs = (rc, r1, r2, r3)

    def group_of(m):
        a = 0
        for first in groups[1:]:
            a = a + (m >= first[0]).astype(jnp.int32)
        return a

    def source(spec):
        n, layer = spec
        return srcs[n] if layer is None else srcs[n].at[layer]

    def a_load(a, layer):
        _, ins, col, _, _ = groups[a]
        return pltpu.make_async_copy(source(ins[layer]).at[:, pl.ds(col, D)], a_buf.at[a % 2, layer], a_sem.at[a % 2, layer])

    def b_load(a, m, layer, ahead=True):
        first, _, _, ins, col = groups[a]
        if ahead:
            col = pl.multiple_of(col + (m - first) * NB, NB)
        slot = lax.rem(m, 2)
        return pltpu.make_async_copy(source(ins[layer]).at[:, pl.ds(col, NB)], b_buf.at[slot, layer], b_sem.at[slot, layer])

    def in_group(a, m, fn):
        last = groups[a + 1][0] if a + 1 < len(groups) else n_tiles

        @pl.when(jnp.logical_and(m >= groups[a][0], m < last))
        def _():
            fn()

    def b_start(m):
        for a in range(len(groups)):
            if groups[a][3] is None:
                continue

            def go(a=a):
                for layer in range(depth):
                    b_load(a, m, layer).start()
            in_group(a, m, go)

    def produce(m):
        half, slot, to = lax.rem(group_of(m), 2), lax.rem(m, 2), lax.rem(m, ring)

        @pl.when(m < (DB if heads else n_tiles))
        def _():
            for layer in range(depth):
                b_load(0, m, layer, False).wait()
        if heads:
            @pl.when(m >= DB)
            def _():
                b_buf[slot, 0] = qkv[:, pl.ds(pl.multiple_of(lax.rem(m - DB, 3) * D + ((m - DB) // 3) * NB, NB), NB)]
        for a in range(len(groups)):
            @pl.when(m == groups[a][0])
            def _():
                for layer in range(depth):
                    a_load(a, layer).wait()
                if a + 1 < len(groups):
                    for layer in range(depth):
                        a_load(a + 1, layer).start()
        b_start(m + 1)

        for z in range(2):
            tot = None
            for layer in range(depth):
                y = tn(a_buf[half, layer, :, part(z, D // 2)], b_buf[slot, layer])
                tot = y if tot is None else tot + y
            tiles[to, z] = tot.reshape(CUBE + (2 * ROWS, NB))

    def pick(color, stage, other):
        idx = {d: slice(None) for d in "zyx"}
        for s in range(stage):
            d = ORDERS[color][s]
            idx[d] = 1 - bit[d] if (other and s == stage - 1) else bit[d]
        return tuple(idx[d] for d in "zyx")

    def piece(k):
        sub = lax.rem(k, 4)
        return (lax.rem(k // 4, ring), pl.multiple_of(lax.rem(sub, 2) * ROWS, 8), pl.multiple_of((sub // 2) * LANES, LANES))

    def send(color, stage, j):
        slot, so = lax.rem(j, n_in), lax.rem(j, n_own)
        if stage == 0:
            tile, row, col = piece(3 * j + color)
            src, to = tiles.at[tile, :, :, :, 1 - bit["c"], pl.ds(row, ROWS), pl.ds(col, LANES)], peer["c"]
        else:
            src, to = own.at[(color, so) + pick(color, stage, True)], peer[ORDERS[color][stage - 1]]
        return pltpu.make_async_remote_copy(src, bufs[stage].at[color, slot], send_sem.at[color, stage, slot],
                                            recv_sem.at[color, stage, slot], device_id=(to,), device_id_type=MESH)

    def place(color, j):
        k = 3 * j + color
        _, row, col = piece(k)
        tile = k // 4
        if heads:
            tile = jnp.where(tile < DB, tile, DB + DB * lax.rem(tile - DB, 3) + (tile - DB) // 3)
        return pl.ds(row, ROWS), pl.ds(pl.multiple_of(tile * NB + col, LANES), LANES)

    def store(color, j):
        so = lax.rem(j, n_own)
        where = place(color, j)
        if spread:
            where = (bit["z"], bit["y"], bit["x"], bit["c"]) + where
        return pltpu.make_async_copy(own.at[(color, so) + pick(color, 3, False)], out_ref.at[where], out_sem.at[color, so])

    def hand_on(color, stage, j):
        slot, so = lax.rem(j, n_in), lax.rem(j, n_own)
        idx = {d: bit[d] for d in "zyxc"}
        for d in ORDERS[color][3 - stage:]:
            idx[d] = slice(None)
        dst = out_ref.at[(idx["z"], idx["y"], idx["x"], idx["c"]) + place(color, j)]
        src = dst if stage else own.at[(color, so) + pick(color, 3, False)]
        to = peer[ORDERS[color][2 - stage] if stage < 3 else "c"]
        return pltpu.make_async_remote_copy(src, dst, all_send.at[color, stage, slot], all_recv.at[color, stage, slot],
                                            device_id=(to,), device_id_type=MESH)

    def live(j, color):
        return jnp.logical_and(j >= 0, 3 * j + color < n_chunks)

    up_from, norm_at, end = FB, 2 * FB, 2 * FB + 1 + DB

    def w_begin(w):
        slot = lax.rem(w, 3)
        begin([(w < up_from, w2.at[part(w, NB)]),
               (jnp.logical_and(w >= up_from, w < norm_at), w1.at[part(lax.rem(w, DB), NB), part((w - up_from) // DB, D)]),
               (jnp.logical_and(w >= norm_at, w < end - 1), wo.at[layer_in, part(lax.rem(w, DB), NB)])], wring, w_sem, slot)

    def w_take(w):
        slot = lax.rem(w, 3)
        pltpu.make_async_copy(wo.at[0, pl.ds(0, NB)], wring.at[slot], w_sem.at[slot]).wait()
        w_begin(w + 2)
        return slot

    def head_weights(duo):
        col = pl.multiple_of(duo * NB, NB)
        base = 3 * lax.rem(duo, 2)
        return [pltpu.make_async_copy(ref.at[layer_in, :, pl.ds(col, NB)], wring.at[base + m], w_sem.at[base + m])
                for m, ref in enumerate((wq, wk, wv))]

    def start(*names):
        for name in names:
            copies[name].start()

    def wait(*names):
        for name in names:
            copies[name].wait()

    if chain:
        if heads:
            table = dict(x=(x_in, xb), d=(d_in, tb), first=(gb, *more))
        else:
            table = dict(d=(d_in, gb), h=(h_in, xb), pre=(pre_in, big), dpre=(big, more[0]), dh=(tb, more[1]), dmix=(xb, more[2]))
        copies = {name: pltpu.make_async_copy(src, dst, at_sem.at[n]) for n, (name, (src, dst)) in enumerate(table.items())}

    def head_loads(duo):
        cols = [pl.ds(n * D + duo * NB, NB) for n in range(3)]
        pairs = [(dmixed_in, xb, cols[0]), (pt_in, pt, pl.ds(duo * 2 * NB, 2 * NB))] + [(qkv_in, qkv, c) for c in cols]
        return [pltpu.make_async_copy(src.at[:, c], dst.at[:, c], head_sem.at[duo, n]) for n, (src, dst, c) in enumerate(pairs)]

    def input_step(duo, turn):
        @pl.when(turn == 0)
        def _():
            for copy in head_weights(duo):
                copy.wait()

            @pl.when(duo < DB - 1)
            def _():
                for copy in head_weights(duo + 1):
                    copy.start()
        base = 3 * lax.rem(duo, 2)

        @pl.loop(jnp.where(turn == 0, 0, turn + 1), turn + 2)
        def _(n):
            c = part(n, NB)
            tot = jnp.where(duo == 0, 0.0, acc[:, c])
            for m in range(3):
                tot = tot + nt(qkv[:, pl.ds(pl.multiple_of(m * D + duo * NB, NB), NB)], wring[base + m, c])
            acc[:, c] = tot

    def sum_step(g, src, slot):
        c, m = part(lax.rem(g, DB), NB), g // DB

        for r in rows_of(512):
            acc[r, c] = jnp.where(m == 0, 0.0, acc[r, c]) + nt(src[r, part(m, D)], wring[slot])

    def mlp_step(g):
        @pl.when(g == 0)
        def _():
            wait("d", "pre")

        @pl.when(g < up_from)
        def _():
            slot, c = w_take(g), part(g, NB)

            for r in rows_of(256):
                d = nt(gb[r, :], wring[slot]).astype(BF16).astype(F32)
                big[r, c] = gelu_grad(big[r, c].astype(F32), d).astype(BF16)

        @pl.when(g == up_from)
        def _():
            start("dpre")

        @pl.when(jnp.logical_and(g >= up_from, g < norm_at))
        def _():
            sum_step(g - up_from, big, w_take(g))

        @pl.when(g == norm_at)
        def _():
            wait("h")
            rms_back_rows(xb, acc, gb, tb)
            start("dh")

        @pl.when(jnp.logical_and(g > norm_at, g < end))
        def _():
            slot, c = w_take(g - 1), part(g - norm_at - 1, NB)

            for r in rows_of(512):
                xb[r, c] = nt(tb[r, :], wring[slot]).astype(BF16)

        @pl.when(g == end - 1)
        def _():
            start("dmix")

    def tick(t, carry):
        for stage in (3, 2, 1, 0) if spread else ():
            j = t - OFFSETS[3] - 2 * (stage + 1)
            for color in range(3):
                @pl.when(live(j, color))
                def _():
                    copy = hand_on(color, stage, j)
                    copy.wait_send()
                    copy.wait_recv()
                    if stage == 0:
                        store(color, j).wait()
                    if stage < 3:
                        hand_on(color, stage + 1, j).start()
        for color in () if spread else range(3):
            j = t - LAST

            @pl.when(live(j, color))
            def _():
                store(color, j).wait()
        for stage in (3, 2, 1, 0):
            j = t - OFFSETS[stage]
            for color in range(3):
                @pl.when(live(j, color))
                def _():
                    slot, so = lax.rem(j, n_in), lax.rem(j, n_own)
                    copy = send(color, stage, j)
                    copy.wait_send()
                    copy.wait_recv()
                    keep = (color, so) + pick(color, stage, False)
                    if stage == 0:
                        tile, row, col = piece(3 * j + color)
                        mine = tiles[tile, :, :, :, bit["c"], pl.ds(row, ROWS), pl.ds(col, LANES)]
                    else:
                        mine = own[keep]
                    own[keep] = mine + bufs[stage][color, slot]
                    if stage < 3:
                        send(color, stage + 1, j).start()
                    else:
                        store(color, j).start()
                        if spread:
                            hand_on(color, 0, j).start()
        for color in range(3):
            @pl.when(live(t, color))
            def _():
                send(color, 0, t).start()
        if heads:
            for duo in range(DB):
                @pl.when(t == 1 + 4 * duo)
                def _():
                    for copy in head_loads(duo):
                        copy.wait()

            @pl.when(jnp.logical_and(t > 0, t <= 4 * DB))
            def _():
                for u in range(2):
                    attention_bwd(2 * lax.rem(t - 1, 4) + u, (t - 1) // 4, qkv, pt, xb)
        m = (3 * t + 5) // 4

        @pl.when(jnp.logical_and(m != (3 * t + 2) // 4, m < n_tiles))
        def _():
            produce(m)
        if heads:
            first_tick, last_attend = DB, 4 * DB
            since = t - first_tick
            quarter = jnp.where(t > last_attend, since - last_attend // 2 + 2, since // 2)
            norm_tick = first_tick + last_attend + last_attend // 2 - 2

            @pl.when(jnp.logical_and(jnp.logical_and(since >= 0, t < norm_tick), jnp.logical_or(t > last_attend, lax.rem(since, 2) == 0)))
            def _():
                input_step(quarter // 4, lax.rem(quarter, 4))

            @pl.when(t == last_attend + 1)
            def _():
                start("x")

            @pl.when(t == norm_tick)
            def _():
                wait("x", "d")
                rms_back_rows(xb, acc, tb, gb)
                start("first")
        if mlp:
            @pl.when(2 * t < end)
            def _():
                @pl.loop(0, 2)
                def _(u):
                    mlp_step(2 * t + u)
        return carry

    for layer in range(depth):
        a_load(0, layer).start()
    b_start(jnp.int32(0))
    if heads:
        for duo in range(DB):
            for copy in head_loads(duo):
                copy.start()
        for copy in head_weights(jnp.int32(0)):
            copy.start()
        start("d")
    if mlp:
        start("d", "pre", "h")
        for n in range(2):
            w_begin(jnp.int32(n))
    barrier = pltpu.get_barrier_semaphore()
    for d in "cxyz":
        pl.semaphore_signal(barrier, inc=1, device_id=(peer[d],), device_id_type=MESH)
    pl.semaphore_wait(barrier, 4)
    produce(jnp.int32(0))
    ticks = pl.cdiv(n_chunks, 3) + LAST + 8 * spread
    lax.fori_loop(0, ticks, tick, 0)
    if heads:
        wait("first")
    if mlp:
        wait("dpre", "dh", "dmix")


def scatter_sum(srcs, groups, n_tiles, collective_id, after=(), chain=0, layer=0, spread=False):
    depth = len(groups[0][1])
    n_own, n_in, blk = LAST + 1 + spread, 4, (ROWS, LANES)
    size = D * NB * n_tiles * 4
    outs = [(), (TD,), (TF, TD, TD)][chain]
    sums = (CUBE + (2,)) * spread + (2 * ROWS, NB * n_tiles)
    args = (*srcs, *after)
    dma = pltpu.SemaphoreType.DMA
    scratch = [
        pltpu.VMEM((2, depth, TOK, D), BF16), pltpu.VMEM((2, depth, TOK, NB), BF16), pltpu.VMEM((n_in, 2) + CUBE + (2 * ROWS, NB), F32),
        pltpu.VMEM((3, n_own) + CUBE + blk, F32)] + [pltpu.VMEM((3, n_in) + CUBE[n:] + blk, F32) for n in range(4)] + [
        dma((2, depth)), dma((2, depth)), dma((3, n_own)), dma((3, 4, n_in)), dma((3, 4, n_in))]
    if spread:
        scratch += [dma((3, 4, n_in))] * 2
    if chain:
        scratch += [pltpu.VMEM(TD, BF16)] * 3 + [
            pltpu.VMEM(TD, F32), pltpu.VMEM((6, D, NB) if chain == HEADS else (3, NB, D), BF16), dma((6,)), dma((6,))]
        scratch += [pltpu.VMEM(TP, BF16), pltpu.VMEM(T3, BF16), dma((DB, DB))] if chain == HEADS else [pltpu.VMEM(TF, BF16)]
    return pl.pallas_call(
        functools.partial(scatter_kernel, groups, n_tiles, len(srcs), len(after), chain, layer, spread),
        out_shape=[jax.ShapeDtypeStruct(sums, F32)] + [jax.ShapeDtypeStruct(o, BF16) for o in outs],
        in_specs=[ANY] * len(args),
        out_specs=[ANY] * (1 + len(outs)),
        scratch_shapes=scratch,
        compiler_params=pltpu.CompilerParams(collective_id=collective_id, has_side_effects=True, vmem_limit_bytes=VMEM_MOST),
        cost_estimate=pl.CostEstimate(flops=size * 4000, bytes_accessed=2 * size, transcendentals=0),
        name=f"scatter_sum_{collective_id}",
    )(*args)


def gather(shard):
    return lax.all_gather(shard, "data", axis=0, tiled=True)


def place_attention(full, layer, dst, carry, after):
    rows, part = 160, TOK * 160 // D

    def kernel(src, *refs):
        outs = refs[-4 - len(carry):]
        for n, out in zip((1, 2, 3, 0), outs):
            out[0] = src[:, n * D:(n + 1) * D]
        for ref, out in zip(refs, outs[4:]):
            out[...] = ref[...]

    strip = pl.BlockSpec((part, D), lambda i: (i, 0))
    return pl.pallas_call(
        kernel,
        grid=(D // rows,),
        out_shape=[jax.ShapeDtypeStruct((2, D, D), F32)] * 4 + [jax.ShapeDtypeStruct((TOK, D), BF16)] * len(carry),
        in_specs=[pl.BlockSpec((rows, 4 * D), lambda i: (i, 0))] + [strip] * len(carry) + [ANY] * (len(dst) + len(after)),
        out_specs=[pl.BlockSpec((1, rows, D), lambda i: (layer, i, 0))] * 4 + [strip] * len(carry),
        input_output_aliases={n + 1 + len(carry): n for n in range(len(dst))},
        compiler_params=pltpu.CompilerParams(vmem_limit_bytes=60 << 20),
        cost_estimate=pl.CostEstimate(flops=D * D, bytes_accessed=32 * D * D, transcendentals=0),
        name=f"place_attention_{layer}",
    )(full, *carry, *dst, *after)


def place_blocks(full, shape, where, dst, after, name):
    rows = D // 4
    blocks = full.shape[1] // D
    strips = [(n, i) for n in range(blocks) for i in range(D // rows)]

    def kernel(src, *refs):
        out, buf, load_sem, store_sem = refs[len(dst) + len(after):]
        loads, stores = [], []
        for k, (n, i) in enumerate(strips):
            row, col = where(n)
            loads.append(pltpu.make_async_copy(src.at[pl.ds(i * rows, rows), pl.ds(n * D, D)], buf.at[k], load_sem.at[k]))
            stores.append(pltpu.make_async_copy(buf.at[k], out.at[pl.ds(row * D + i * rows, rows), pl.ds(col * D, D)], store_sem.at[k]))
        for load in loads:
            load.start()
        for load, store in zip(loads, stores):
            load.wait()
            store.start()
        for store in stores:
            store.wait()

    return pl.pallas_call(
        kernel,
        out_shape=jax.ShapeDtypeStruct(shape, F32),
        in_specs=[ANY] * (1 + len(dst) + len(after)),
        out_specs=ANY,
        scratch_shapes=[pltpu.VMEM((len(strips), rows, D), F32)] + [pltpu.SemaphoreType.DMA((len(strips),))] * 2,
        input_output_aliases={1: 0} if dst else {},
        compiler_params=pltpu.CompilerParams(vmem_limit_bytes=VMEM_MOST),
        cost_estimate=pl.CostEstimate(flops=D * D, bytes_accessed=8 * blocks * D * D, transcendentals=0),
        name=name,
    )(full, *dst, *after)


def solution(mesh):
    def local_step(x_init, cot_out, w_query, w_key, w_value, w_proj, w_up, w_down):
        cot, x0 = cot_out.reshape(TD), x_init.reshape(TD)
        (nrm, qkv, pt, mx, nn2, act, h0, pre0, xmid, dmix1, dpre1, dh1) = front(x0, cot, w_query, w_key, w_value, w_proj, w_up, w_down)
        w_in = (w_query, w_key, w_value)
        both, ends = ((0, 0), (0, 1)), ((1, None), (2, None))

        def attention(layer, d_hidden, d_mixed, x_in, number, after):
            groups = ((0, ((0, layer),), 0, ((1, None),), 0), (DB, ((2, layer),), 0, None, 0))
            srcs = (mx, d_hidden, nrm, d_mixed, qkv, pt, x_in, d_hidden, *w_in)
            return scatter_sum(srcs, groups, 4 * DB, number, after, chain=HEADS, layer=layer)

        down = [tuple((DB * n, both, q * D, ends, 0) for n, q in enumerate(qs)) for qs in ((0, 1, 2), (3,))]
        shard1, dmid = attention(1, dh1, dmix1, xmid, 1, ())
        full1 = gather(shard1)
        shard_a, dpre0, dh0, dmix0 = scatter_sum(
            (act, dmid, cot, h0, pre0, dmid, w_proj, w_up, w_down), down[0], 3 * DB, 2, (shard1,), chain=MLP)
        full_a = gather(shard_a)
        shard0, dx = attention(0, dh0, dmix0, x0, 3, (shard_a,))
        full0 = gather(shard0)
        shard_up, = scatter_sum((nn2, dpre0, dpre1), ((0, both, 0, ends, 0),), FB, 4, (shard0,))
        full_up = gather(shard_up)
        shard_b, = scatter_sum((act, dmid, cot), down[1], DB, 5, (shard_up,), spread=True)
        half = place_attention(full1, 1, (), (), (shard_b,))
        g_down = place_blocks(full_a, (FF, D), lambda n: (n, 0), (), (half[0],), "place_down_0")
        g_down = place_blocks(shard_b.reshape(D, D), (FF, D), lambda n: (3, 0), (g_down,), (), "place_down_3")
        *attn, dx = place_attention(full0, 0, half, (dx,), (g_down,))
        g_up = place_blocks(full_up, (D, FF), lambda n: (0, n), (), (attn[0],), "place_up")
        return (*attn, g_up, g_down, dx.reshape(x_init.shape))

    data_spec = P("data")
    full_spec = P()
    in_specs = (data_spec, data_spec) + (full_spec,) * 6
    out_specs = (full_spec,) * 6 + (data_spec,)
    return jax.shard_map(local_step, mesh=mesh, in_specs=in_specs, out_specs=out_specs, check_vma=False)
```

```python
import functools

import jax
import jax.numpy as jnp
from jax import lax
from jax.experimental import pallas as pl
from jax.experimental.pallas import tpu as pltpu
from jax.sharding import PartitionSpec as P

EPS = 1e-6
F32, BF16 = jnp.float32, jnp.bfloat16
TOK, D, FF, SEQ = 1024, 1280, 5120, 128
NB = 256
DB, FB = D // NB, FF // NB
PAIRS = 10
GROUP = 4
VMEM_MOST = 67043328
SUBS = [pl.ds(j * NB, NB) for j in range(DB)]
ANY = pl.BlockSpec(memory_space=pl.ANY)
C0 = 0.7978845608028654
C1 = C0 * 0.044715


def nn(a, b):
    return lax.dot_general(a, b, (((1,), (0,)), ((), ())), preferred_element_type=F32)


def nt(a, b):
    return lax.dot_general(a, b, (((1,), (1,)), ((), ())), preferred_element_type=F32)


def tn(a, b):
    return lax.dot_general(a, b, (((0,), (0,)), ((), ())), preferred_element_type=F32)


def part(i, width):
    return pl.ds(pl.multiple_of(i * width, 128), width)


def rows_of(size):
    return [pl.ds(k * size, size) for k in range(TOK // size)]


class Stage:
    def __init__(self, count, source, step):
        self.count, self.source, self.step = count, source, step


def begin(sources, ring, sem, slot):
    for cond, src in sources:
        copy = pltpu.make_async_copy(src, ring.at[slot], sem.at[slot])
        if cond is None:
            copy.start()
        else:
            pl.when(cond)(copy.start)


def run_stages(items, ring, sem, follow=()):
    stages = [it for it in items if isinstance(it, Stage)]
    base = 0
    for it in items:
        if not isinstance(it, Stage):
            it()
            continue
        after = stages[stages.index(it) + 1].source(0) if it is not stages[-1] else follow

        def one(i, it=it, base=base, after=after):
            slot = lax.rem(base + i, 2)
            pltpu.make_async_copy(it.source(0)[0][1], ring.at[slot], sem.at[slot]).wait()
            other = lax.rem(base + i + 1, 2)

            @pl.when(i + 1 < it.count)
            def _():
                begin(it.source(i + 1), ring, sem, other)

            @pl.when(i + 1 >= it.count)
            def _():
                begin(after, ring, sem, other)
            it.step(i, slot)

        pl.loop(0, it.count)(one)
        base += it.count


def gelu(x):
    half = 0.5 * x
    return half * jnp.tanh(x * (C0 + C1 * (x * x))) + half


def gelu_grad(x, d):
    x2 = x * x
    t = jnp.tanh(x * (C0 + C1 * x2))
    return d * ((0.5 + 0.5 * t) + ((1.0 - t * t) * x) * (0.5 * C0 + 1.5 * C1 * x2))


def by_rows(fn, rows=256):
    @pl.loop(0, TOK // rows)
    def _(i):
        fn(part(i, rows))


def inverse_rms(x):
    return lax.rsqrt(jnp.mean(x * x, axis=-1, keepdims=True) + EPS)


def rms_rows(src, dst):
    def one(r):
        x = src[r, :].astype(F32)
        dst[r, :] = (x * inverse_rms(x)).astype(BF16)
    by_rows(one)


def add_rms_rows(res, acc, out, dst):
    def one(r):
        y = (res[r, :].astype(F32) + acc[r, :].astype(BF16).astype(F32)).astype(BF16)
        out[r, :] = y
        x = y.astype(F32)
        dst[r, :] = (x * inverse_rms(x)).astype(BF16)
    by_rows(one)


def rms_back_rows(x_ref, dy_acc, dres_ref, dst):
    def one(r):
        x = x_ref[r, :].astype(F32)
        dy = dy_acc[r, :].astype(BF16).astype(F32)
        inv = inverse_rms(x)
        dot = jnp.mean(dy * x, axis=-1, keepdims=True)
        dst[r, :] = (dres_ref[r, :].astype(F32) + (dy * inv - x * (inv * inv * inv * dot))).astype(BF16)
    by_rows(one)


def lane_mask():
    return lax.broadcasted_iota(jnp.int32, (SEQ, 2 * 64), 1) < 64


def split_heads(x, mask):
    zero = jnp.zeros_like(x)
    return jnp.concatenate([jnp.where(mask, x, zero), jnp.where(mask, zero, x)], axis=0)


def split_heads_t(x):
    y = x.T
    top = lax.broadcasted_iota(jnp.int32, y.shape, 0) < 64
    zero = jnp.zeros_like(y)
    return jnp.concatenate([jnp.where(top, y, zero), jnp.where(top, zero, y)], axis=1)


def attention_fwd(qkv, pt, mixed):
    mask = lane_mask()

    def one(block):
        for u in range(GROUP * PAIRS):
            h = u // GROUP
            rows = pl.ds(pl.multiple_of(block.start + (u % GROUP) * SEQ, SEQ), SEQ)
            q, k, v = (qkv[rows, pl.ds(n * D + h * SEQ, SEQ)] for n in range(3))
            st = nn(k, split_heads_t(q)) * 0.125
            e = jnp.exp(st - jnp.max(st, axis=0, keepdims=True))
            p = (e / jnp.sum(e, axis=0, keepdims=True)).astype(BF16)
            pt[rows, pl.ds(h * NB, NB)] = p
            o = tn(p, v)
            mixed[rows, pl.ds(h * SEQ, SEQ)] = jnp.where(mask, o[:SEQ], o[SEQ:]).astype(BF16)
    by_rows(one, GROUP * SEQ)


def attention_bwd(s, duo, qkv, pt, dmixed):
    mask = lane_mask()
    rows = part(s, SEQ)
    for h in range(2):
        lanes = [pl.ds(pl.multiple_of(n * D + duo * NB + h * SEQ, SEQ), SEQ) for n in range(3)]
        q, k, v = (qkv[rows, c] for c in lanes)
        do = split_heads(dmixed[rows, lanes[0]], mask)
        p = pt[rows, part(2 * duo + h, NB)]
        dp = nt(v, do).astype(BF16).astype(F32)
        pf = p.astype(F32)
        dot = jnp.sum(dp * pf, axis=0, keepdims=True)
        ds = (pf * (dp - dot) * 0.125).astype(BF16)
        dq = tn(ds, k)
        qkv[rows, lanes[0]] = jnp.where(mask, dq[:SEQ], dq[SEQ:]).astype(BF16)
        qkv[rows, lanes[1]] = nn(ds, split_heads(q, mask)).astype(BF16)
        qkv[rows, lanes[2]] = nn(p, do).astype(BF16)


def front_kernel(x0, cot, wq, wk, wv, wo, w1, w2,
                 n_out, qkv_out, pt_out, mx_out, nn_out, act_out, h0, pre0, xmid, dmix1, dpre1, dh1,
                 x, nrm, qkv, pt, mx, h, n2, big, g, acc, stg, ring, wsem, sems, stg_sem):
    def copy(n, src, dst):
        return pltpu.make_async_copy(src, dst, sems.at[n])

    cx, cg = copy(0, x0, x), copy(1, cot, g)
    cx.start()
    cg.start()
    begin([(None, wq.at[0])], ring, wsem, 0)
    cx.wait()
    rms_rows(x, nrm)

    def stage_copy(i, dst):
        slot = lax.rem(i, 2)
        return pltpu.make_async_copy(stg.at[slot], dst.at[:, part(i, D)], stg_sem.at[slot])

    def sums(stage_count, source, src, times, weight):
        def step(i, slot):
            for c in SUBS:
                for r in rows_of(512):
                    acc[r, c] = jnp.where(i == 0, 0.0, acc[r, c]) + times(src[r, part(i, D)], weight(slot, c))
        return Stage(stage_count, source, step)

    @pl.loop(0, 2)
    def _(l):
        first = l == 0
        outs = dict(n=copy(2, nrm, n_out.at[l]), qkv=copy(3, qkv, qkv_out.at[l]), pt=copy(4, pt, pt_out.at[l]),
                    mx=copy(5, mx, mx_out.at[l]), nn=copy(6, n2, nn_out.at[l]))
        only = dict(h=copy(7, h, h0), act=copy(8, big, act_out.at[0]))

        def qkv_step(i, slot):
            for j, c in enumerate(SUBS):
                for r in rows_of(256):
                    qkv[r, pl.ds(pl.multiple_of(i * D + j * NB, NB), NB)] = nn(nrm[r, :], ring[slot, :, c]).astype(BF16)

        def attend():
            outs["qkv"].start()
            attention_fwd(qkv, pt, mx)
            outs["pt"].start()
            outs["mx"].start()

        def proj_step(i, slot):
            for c in SUBS:
                y = nn(mx[...], ring[slot, :, c]).astype(BF16).astype(F32)
                h[:, c] = (x[:, c].astype(F32) + y).astype(BF16)

        def middle():
            rms_rows(h, n2)
            outs["nn"].start()
            pl.when(first)(only["h"].start)

        def up_step(i, slot):
            half = lax.rem(i, 2)
            pl.when(i >= 2)(stage_copy(i, pre0).wait)
            for j, c in enumerate(SUBS):
                for r in rows_of(128):
                    pre = nn(n2[r, :], ring[slot, :, c]).astype(BF16)
                    act = gelu(pre.astype(F32)).astype(BF16)
                    big[r, pl.ds(pl.multiple_of(i * D + j * NB, NB), NB)] = jnp.where(first, act, pre)
                    stg[half, r, c] = jnp.where(first, pre, act)
            pl.when(first)(stage_copy(i, pre0).start)
            pl.when(l == 1)(stage_copy(i, act_out.at[1]).start)

        outs["n"].start()
        run_stages([Stage(3, lambda i: [(i == m, w.at[l]) for m, w in enumerate((wq, wk, wv))], qkv_step), attend,
                    Stage(1, lambda i: [(None, wo.at[l])], proj_step), middle,
                    Stage(4, lambda i: [(None, w1.at[:, part(i, D)])], up_step)], ring, wsem, [(None, w2.at[pl.ds(0, D)])])
        for i in range(2):
            stage_copy(i, pre0).wait()

        @pl.when(first)
        def _():
            only["act"].start()
            run_stages([sums(4, lambda i: [(None, w2.at[part(i, D)])], big, nn, lambda slot, c: ring[slot, :, c])],
                       ring, wsem, [(None, wq.at[1])])
            for cp in (*outs.values(), *only.values()):
                cp.wait()
            add_rms_rows(h, acc, x, nrm)
            copy(9, x, xmid).start()

    def dact_step(i, slot):
        for j, c in enumerate(SUBS):
            to = pl.ds(pl.multiple_of(i * D + j * NB, NB), NB)
            for r in rows_of(256):
                d = nt(g[r, :], ring[slot, c]).astype(BF16).astype(F32)
                big[r, to] = gelu_grad(big[r, to].astype(F32), d).astype(BF16)

    def after_dact():
        copy(8, big, dpre1).start()

    def after_dn2():
        copy(9, x, xmid).wait()
        rms_back_rows(h, acc, g, x)
        copy(9, x, dh1).start()
        copy(2, nrm, n_out.at[1]).wait()

    def dmix_step(i, slot):
        for c in SUBS:
            nrm[:, c] = nt(x[...], ring[slot, c]).astype(BF16)

    cg.wait()
    run_stages([Stage(4, lambda i: [(None, w2.at[part(i, D)])], dact_step), after_dact,
                sums(4, lambda i: [(None, w1.at[:, part(i, D)])], big, nt, lambda slot, c: ring[slot, c]), after_dn2,
                Stage(1, lambda i: [(None, wo.at[1])], dmix_step)], ring, wsem)
    copy(2, nrm, dmix1).start()
    for n, src, dst in ((2, nrm, dmix1), (3, qkv, qkv_out.at[1]), (4, pt, pt_out.at[1]), (5, mx, mx_out.at[1]),
                        (6, n2, nn_out.at[1]), (8, big, dpre1), (9, x, dh1)):
        copy(n, src, dst).wait()


TD, T3, TF, TP = (TOK, D), (TOK, 3 * D), (TOK, FF), (TOK, PAIRS * NB)


def front(x0, cot, *weights):
    both = [(2,) + s for s in (TD, T3, TP, TD, TD, TF)]
    outs = both + [TD, TF, TD, TD, TF, TD]
    vmem = [pltpu.VMEM(s, BF16) for s in (TD, TD, T3, TP, TD, TD, TD, TF, TD)]
    return pl.pallas_call(
        front_kernel,
        out_shape=[jax.ShapeDtypeStruct(s, BF16) for s in outs],
        in_specs=[ANY] * (2 + len(weights)),
        out_specs=[ANY] * len(outs),
        scratch_shapes=vmem + [pltpu.VMEM(TD, F32), pltpu.VMEM((2, TOK, D), BF16), pltpu.VMEM((2, D, D), BF16),
                               pltpu.SemaphoreType.DMA((2,)), pltpu.SemaphoreType.DMA((10,)), pltpu.SemaphoreType.DMA((2,))],
        compiler_params=pltpu.CompilerParams(vmem_limit_bytes=VMEM_MOST),
        name="front",
    )(x0, cot, *weights)


MESH = pl.DeviceIdType.MESH
ROWS, LANES = 40, 128
OFFSETS = (1, 3, 5, 7)
LAST = OFFSETS[3] + 1
ORDERS = ("xyz", "yzx", "zxy")
CUBE = (2, 2, 2)
HEADS, MLP = 1, 2
N_OUT = (1, 2, 4)


def scatter_kernel(groups, n_tiles, n_src, n_after, chain, layer_in, spread, *refs):
    srcs, refs = refs[:n_src], refs[n_src + n_after:]
    out_ref, more, refs = refs[0], refs[1:N_OUT[chain]], refs[N_OUT[chain]:]
    a_buf, b_buf, tiles, own, rc, r1, r2, r3, a_sem, b_sem, out_sem, send_sem, recv_sem, *refs = refs
    heads, mlp, depth = chain == HEADS, chain == MLP, len(groups[0][1])
    if spread:
        all_send, all_recv = refs
    if chain:
        xb, gb, tb, acc, wring, w_sem, at_sem, big, *refs = refs
    if heads:
        (qkv, head_sem), pt = refs, big
        _, _, _, dmixed_in, qkv_in, pt_in, x_in, d_in, wq, wk, wv = srcs
        qkv_in, pt_in = qkv_in.at[layer_in], pt_in.at[layer_in]
    if mlp:
        _, _, _, h_in, pre_in, d_in, wo, w1, w2 = srcs
    me = lax.axis_index("data")
    bit, peer = {}, {}
    for n, d in enumerate("cxyz"):
        bit[d] = lax.rem(me // 2 ** n, 2)
        peer[d] = me + 2 ** n * (1 - 2 * bit[d])
    n_own, n_in, ring = own.shape[1], rc.shape[1], tiles.shape[0]
    n_chunks = 4 * n_tiles
    bufs = (rc, r1, r2, r3)

    def group_of(m):
        a = 0
        for first in groups[1:]:
            a = a + (m >= first[0]).astype(jnp.int32)
        return a

    def source(spec):
        n, layer = spec
        return srcs[n] if layer is None else srcs[n].at[layer]

    def a_load(a, layer):
        _, ins, col, _, _ = groups[a]
        return pltpu.make_async_copy(source(ins[layer]).at[:, pl.ds(col, D)], a_buf.at[a % 2, layer], a_sem.at[a % 2, layer])

    def b_load(a, m, layer, ahead=True):
        first, _, _, ins, col = groups[a]
        if ahead:
            col = pl.multiple_of(col + (m - first) * NB, NB)
        slot = lax.rem(m, 2)
        return pltpu.make_async_copy(source(ins[layer]).at[:, pl.ds(col, NB)], b_buf.at[slot, layer], b_sem.at[slot, layer])

    def in_group(a, m, fn):
        last = groups[a + 1][0] if a + 1 < len(groups) else n_tiles

        @pl.when(jnp.logical_and(m >= groups[a][0], m < last))
        def _():
            fn()

    def b_start(m):
        for a in range(len(groups)):
            if groups[a][3] is None:
                continue

            def go(a=a):
                for layer in range(depth):
                    b_load(a, m, layer).start()
            in_group(a, m, go)

    def produce(m):
        half, slot, to = lax.rem(group_of(m), 2), lax.rem(m, 2), lax.rem(m, ring)

        @pl.when(m < (DB if heads else n_tiles))
        def _():
            for layer in range(depth):
                b_load(0, m, layer, False).wait()
        if heads:
            @pl.when(m >= DB)
            def _():
                b_buf[slot, 0] = qkv[:, pl.ds(pl.multiple_of(lax.rem(m - DB, 3) * D + ((m - DB) // 3) * NB, NB), NB)]
        for a in range(len(groups)):
            @pl.when(m == groups[a][0])
            def _():
                for layer in range(depth):
                    a_load(a, layer).wait()
                if a + 1 < len(groups):
                    for layer in range(depth):
                        a_load(a + 1, layer).start()
        b_start(m + 1)

        for z in range(2):
            tot = None
            for layer in range(depth):
                y = tn(a_buf[half, layer, :, part(z, D // 2)], b_buf[slot, layer])
                tot = y if tot is None else tot + y
            tiles[to, z] = tot.reshape(CUBE + (2 * ROWS, NB))

    def pick(color, stage, other):
        idx = {d: slice(None) for d in "zyx"}
        for s in range(stage):
            d = ORDERS[color][s]
            idx[d] = 1 - bit[d] if (other and s == stage - 1) else bit[d]
        return tuple(idx[d] for d in "zyx")

    def piece(k):
        sub = lax.rem(k, 4)
        return (lax.rem(k // 4, ring), pl.multiple_of(lax.rem(sub, 2) * ROWS, 8), pl.multiple_of((sub // 2) * LANES, LANES))

    def send(color, stage, j):
        slot, so = lax.rem(j, n_in), lax.rem(j, n_own)
        if stage == 0:
            tile, row, col = piece(3 * j + color)
            src, to = tiles.at[tile, :, :, :, 1 - bit["c"], pl.ds(row, ROWS), pl.ds(col, LANES)], peer["c"]
        else:
            src, to = own.at[(color, so) + pick(color, stage, True)], peer[ORDERS[color][stage - 1]]
        return pltpu.make_async_remote_copy(src, bufs[stage].at[color, slot], send_sem.at[color, stage, slot],
                                            recv_sem.at[color, stage, slot], device_id=(to,), device_id_type=MESH)

    def place(color, j):
        k = 3 * j + color
        _, row, col = piece(k)
        tile = k // 4
        if heads:
            tile = jnp.where(tile < DB, tile, DB + DB * lax.rem(tile - DB, 3) + (tile - DB) // 3)
        return pl.ds(row, ROWS), pl.ds(pl.multiple_of(tile * NB + col, LANES), LANES)

    def store(color, j):
        so = lax.rem(j, n_own)
        where = place(color, j)
        if spread:
            where = (bit["z"], bit["y"], bit["x"], bit["c"]) + where
        return pltpu.make_async_copy(own.at[(color, so) + pick(color, 3, False)], out_ref.at[where], out_sem.at[color, so])

    def hand_on(color, stage, j):
        slot, so = lax.rem(j, n_in), lax.rem(j, n_own)
        idx = {d: bit[d] for d in "zyxc"}
        for d in ORDERS[color][3 - stage:]:
            idx[d] = slice(None)
        dst = out_ref.at[(idx["z"], idx["y"], idx["x"], idx["c"]) + place(color, j)]
        src = dst if stage else own.at[(color, so) + pick(color, 3, False)]
        to = peer[ORDERS[color][2 - stage] if stage < 3 else "c"]
        return pltpu.make_async_remote_copy(src, dst, all_send.at[color, stage, slot], all_recv.at[color, stage, slot],
                                            device_id=(to,), device_id_type=MESH)

    def live(j, color):
        return jnp.logical_and(j >= 0, 3 * j + color < n_chunks)

    up_from, norm_at, end = FB, 2 * FB, 2 * FB + 1 + DB

    def w_begin(w):
        slot = lax.rem(w, 3)
        begin([(w < up_from, w2.at[part(w, NB)]),
               (jnp.logical_and(w >= up_from, w < norm_at), w1.at[part(lax.rem(w, DB), NB), part((w - up_from) // DB, D)]),
               (jnp.logical_and(w >= norm_at, w < end - 1), wo.at[layer_in, part(lax.rem(w, DB), NB)])], wring, w_sem, slot)

    def w_take(w):
        slot = lax.rem(w, 3)
        pltpu.make_async_copy(wo.at[0, pl.ds(0, NB)], wring.at[slot], w_sem.at[slot]).wait()
        w_begin(w + 2)
        return slot

    def head_weights(duo):
        col = pl.multiple_of(duo * NB, NB)
        base = 3 * lax.rem(duo, 2)
        return [pltpu.make_async_copy(ref.at[layer_in, :, pl.ds(col, NB)], wring.at[base + m], w_sem.at[base + m])
                for m, ref in enumerate((wq, wk, wv))]

    def start(*names):
        for name in names:
            copies[name].start()

    def wait(*names):
        for name in names:
            copies[name].wait()

    if chain:
        if heads:
            table = dict(x=(x_in, xb), d=(d_in, tb), first=(gb, *more))
        else:
            table = dict(d=(d_in, gb), h=(h_in, xb), pre=(pre_in, big), dpre=(big, more[0]), dh=(tb, more[1]), dmix=(xb, more[2]))
        copies = {name: pltpu.make_async_copy(src, dst, at_sem.at[n]) for n, (name, (src, dst)) in enumerate(table.items())}

    def head_loads(duo):
        cols = [pl.ds(n * D + duo * NB, NB) for n in range(3)]
        pairs = [(dmixed_in, xb, cols[0]), (pt_in, pt, pl.ds(duo * 2 * NB, 2 * NB))] + [(qkv_in, qkv, c) for c in cols]
        return [pltpu.make_async_copy(src.at[:, c], dst.at[:, c], head_sem.at[duo, n]) for n, (src, dst, c) in enumerate(pairs)]

    def input_step(duo, turn):
        @pl.when(turn == 0)
        def _():
            for copy in head_weights(duo):
                copy.wait()

            @pl.when(duo < DB - 1)
            def _():
                for copy in head_weights(duo + 1):
                    copy.start()
        base = 3 * lax.rem(duo, 2)

        @pl.loop(jnp.where(turn == 0, 0, turn + 1), turn + 2)
        def _(n):
            c = part(n, NB)
            tot = jnp.where(duo == 0, 0.0, acc[:, c])
            for m in range(3):
                tot = tot + nt(qkv[:, pl.ds(pl.multiple_of(m * D + duo * NB, NB), NB)], wring[base + m, c])
            acc[:, c] = tot

    def sum_step(g, src, slot):
        c, m = part(lax.rem(g, DB), NB), g // DB

        for r in rows_of(512):
            acc[r, c] = jnp.where(m == 0, 0.0, acc[r, c]) + nt(src[r, part(m, D)], wring[slot])

    def mlp_step(g):
        @pl.when(g == 0)
        def _():
            wait("d", "pre")

        @pl.when(g < up_from)
        def _():
            slot, c = w_take(g), part(g, NB)

            for r in rows_of(256):
                d = nt(gb[r, :], wring[slot]).astype(BF16).astype(F32)
                big[r, c] = gelu_grad(big[r, c].astype(F32), d).astype(BF16)

        @pl.when(g == up_from)
        def _():
            start("dpre")

        @pl.when(jnp.logical_and(g >= up_from, g < norm_at))
        def _():
            sum_step(g - up_from, big, w_take(g))

        @pl.when(g == norm_at)
        def _():
            wait("h")
            rms_back_rows(xb, acc, gb, tb)
            start("dh")

        @pl.when(jnp.logical_and(g > norm_at, g < end))
        def _():
            slot, c = w_take(g - 1), part(g - norm_at - 1, NB)

            for r in rows_of(512):
                xb[r, c] = nt(tb[r, :], wring[slot]).astype(BF16)

        @pl.when(g == end - 1)
        def _():
            start("dmix")

    def tick(t, carry):
        for stage in (3, 2, 1, 0) if spread else ():
            j = t - OFFSETS[3] - 2 * (stage + 1)
            for color in range(3):
                @pl.when(live(j, color))
                def _():
                    copy = hand_on(color, stage, j)
                    copy.wait_send()
                    copy.wait_recv()
                    if stage == 0:
                        store(color, j).wait()
                    if stage < 3:
                        hand_on(color, stage + 1, j).start()
        for color in () if spread else range(3):
            j = t - LAST

            @pl.when(live(j, color))
            def _():
                store(color, j).wait()
        for stage in (3, 2, 1, 0):
            j = t - OFFSETS[stage]
            for color in range(3):
                @pl.when(live(j, color))
                def _():
                    slot, so = lax.rem(j, n_in), lax.rem(j, n_own)
                    copy = send(color, stage, j)
                    copy.wait_send()
                    copy.wait_recv()
                    keep = (color, so) + pick(color, stage, False)
                    if stage == 0:
                        tile, row, col = piece(3 * j + color)
                        mine = tiles[tile, :, :, :, bit["c"], pl.ds(row, ROWS), pl.ds(col, LANES)]
                    else:
                        mine = own[keep]
                    own[keep] = mine + bufs[stage][color, slot]
                    if stage < 3:
                        send(color, stage + 1, j).start()
                    else:
                        store(color, j).start()
                        if spread:
                            hand_on(color, 0, j).start()
        for color in range(3):
            @pl.when(live(t, color))
            def _():
                send(color, 0, t).start()
        if heads:
            for duo in range(DB):
                @pl.when(t == 1 + 4 * duo)
                def _():
                    for copy in head_loads(duo):
                        copy.wait()

            @pl.when(jnp.logical_and(t > 0, t <= 4 * DB))
            def _():
                for u in range(2):
                    attention_bwd(2 * lax.rem(t - 1, 4) + u, (t - 1) // 4, qkv, pt, xb)
        m = (3 * t + 5) // 4

        @pl.when(jnp.logical_and(m != (3 * t + 2) // 4, m < n_tiles))
        def _():
            produce(m)
        if heads:
            first_tick, last_attend = DB, 4 * DB
            since = t - first_tick
            quarter = jnp.where(t > last_attend, since - last_attend // 2 + 2, since // 2)
            norm_tick = first_tick + last_attend + last_attend // 2 - 2

            @pl.when(jnp.logical_and(jnp.logical_and(since >= 0, t < norm_tick), jnp.logical_or(t > last_attend, lax.rem(since, 2) == 0)))
            def _():
                input_step(quarter // 4, lax.rem(quarter, 4))

            @pl.when(t == last_attend + 1)
            def _():
                start("x")

            @pl.when(t == norm_tick)
            def _():
                wait("x", "d")
                rms_back_rows(xb, acc, tb, gb)
                start("first")
        if mlp:
            @pl.when(2 * t < end)
            def _():
                @pl.loop(0, 2)
                def _(u):
                    mlp_step(2 * t + u)
        return carry

    for layer in range(depth):
        a_load(0, layer).start()
    b_start(jnp.int32(0))
    if heads:
        for duo in range(DB):
            for copy in head_loads(duo):
                copy.start()
        for copy in head_weights(jnp.int32(0)):
            copy.start()
        start("d")
    if mlp:
        start("d", "pre", "h")
        for n in range(2):
            w_begin(jnp.int32(n))
    barrier = pltpu.get_barrier_semaphore()
    for d in "cxyz":
        pl.semaphore_signal(barrier, inc=1, device_id=(peer[d],), device_id_type=MESH)
    pl.semaphore_wait(barrier, 4)
    produce(jnp.int32(0))
    ticks = pl.cdiv(n_chunks, 3) + LAST + 8 * spread
    lax.fori_loop(0, ticks, tick, 0)
    if heads:
        wait("first")
    if mlp:
        wait("dpre", "dh", "dmix")


def scatter_sum(srcs, groups, n_tiles, collective_id, after=(), chain=0, layer=0, spread=False):
    depth = len(groups[0][1])
    n_own, n_in, blk = LAST + 1 + spread, 4, (ROWS, LANES)
    size = D * NB * n_tiles * 4
    outs = [(), (TD,), (TF, TD, TD)][chain]
    sums = (CUBE + (2,)) * spread + (2 * ROWS, NB * n_tiles)
    args = (*srcs, *after)
    dma = pltpu.SemaphoreType.DMA
    scratch = [
        pltpu.VMEM((2, depth, TOK, D), BF16), pltpu.VMEM((2, depth, TOK, NB), BF16), pltpu.VMEM((n_in, 2) + CUBE + (2 * ROWS, NB), F32),
        pltpu.VMEM((3, n_own) + CUBE + blk, F32)] + [pltpu.VMEM((3, n_in) + CUBE[n:] + blk, F32) for n in range(4)] + [
        dma((2, depth)), dma((2, depth)), dma((3, n_own)), dma((3, 4, n_in)), dma((3, 4, n_in))]
    if spread:
        scratch += [dma((3, 4, n_in))] * 2
    if chain:
        scratch += [pltpu.VMEM(TD, BF16)] * 3 + [
            pltpu.VMEM(TD, F32), pltpu.VMEM((6, D, NB) if chain == HEADS else (3, NB, D), BF16), dma((6,)), dma((6,))]
        scratch += [pltpu.VMEM(TP, BF16), pltpu.VMEM(T3, BF16), dma((DB, DB))] if chain == HEADS else [pltpu.VMEM(TF, BF16)]
    return pl.pallas_call(
        functools.partial(scatter_kernel, groups, n_tiles, len(srcs), len(after), chain, layer, spread),
        out_shape=[jax.ShapeDtypeStruct(sums, F32)] + [jax.ShapeDtypeStruct(o, BF16) for o in outs],
        in_specs=[ANY] * len(args),
        out_specs=[ANY] * (1 + len(outs)),
        scratch_shapes=scratch,
        compiler_params=pltpu.CompilerParams(collective_id=collective_id, has_side_effects=True, vmem_limit_bytes=VMEM_MOST),
        cost_estimate=pl.CostEstimate(flops=size * 4000, bytes_accessed=2 * size, transcendentals=0),
        name=f"scatter_sum_{collective_id}",
    )(*args)


def gather(shard):
    return lax.all_gather(shard, "data", axis=0, tiled=True)


def place_attention(full, layer, dst, carry, after):
    rows, part = 160, TOK * 160 // D

    def kernel(src, *refs):
        outs = refs[-4 - len(carry):]
        for n, out in zip((1, 2, 3, 0), outs):
            out[0] = src[:, n * D:(n + 1) * D]
        for ref, out in zip(refs, outs[4:]):
            out[...] = ref[...]

    strip = pl.BlockSpec((part, D), lambda i: (i, 0))
    return pl.pallas_call(
        kernel,
        grid=(D // rows,),
        out_shape=[jax.ShapeDtypeStruct((2, D, D), F32)] * 4 + [jax.ShapeDtypeStruct((TOK, D), BF16)] * len(carry),
        in_specs=[pl.BlockSpec((rows, 4 * D), lambda i: (i, 0))] + [strip] * len(carry) + [ANY] * (len(dst) + len(after)),
        out_specs=[pl.BlockSpec((1, rows, D), lambda i: (layer, i, 0))] * 4 + [strip] * len(carry),
        input_output_aliases={n + 1 + len(carry): n for n in range(len(dst))},
        compiler_params=pltpu.CompilerParams(vmem_limit_bytes=60 << 20),
        cost_estimate=pl.CostEstimate(flops=D * D, bytes_accessed=32 * D * D, transcendentals=0),
        name=f"place_attention_{layer}",
    )(full, *carry, *dst, *after)


def place_blocks(full, shape, where, dst, after, name):
    rows = D // 4
    blocks = full.shape[1] // D
    strips = [(n, i) for n in range(blocks) for i in range(D // rows)]

    def kernel(src, *refs):
        out, buf, load_sem, store_sem = refs[len(dst) + len(after):]
        loads, stores = [], []
        for k, (n, i) in enumerate(strips):
            row, col = where(n)
            loads.append(pltpu.make_async_copy(src.at[pl.ds(i * rows, rows), pl.ds(n * D, D)], buf.at[k], load_sem.at[k]))
            stores.append(pltpu.make_async_copy(buf.at[k], out.at[pl.ds(row * D + i * rows, rows), pl.ds(col * D, D)], store_sem.at[k]))
        for load in loads:
            load.start()
        for load, store in zip(loads, stores):
            load.wait()
            store.start()
        for store in stores:
            store.wait()

    return pl.pallas_call(
        kernel,
        out_shape=jax.ShapeDtypeStruct(shape, F32),
        in_specs=[ANY] * (1 + len(dst) + len(after)),
        out_specs=ANY,
        scratch_shapes=[pltpu.VMEM((len(strips), rows, D), F32)] + [pltpu.SemaphoreType.DMA((len(strips),))] * 2,
        input_output_aliases={1: 0} if dst else {},
        compiler_params=pltpu.CompilerParams(vmem_limit_bytes=VMEM_MOST),
        cost_estimate=pl.CostEstimate(flops=D * D, bytes_accessed=8 * blocks * D * D, transcendentals=0),
        name=name,
    )(full, *dst, *after)


def solution(mesh):
    def local_step(x_init, cot_out, w_query, w_key, w_value, w_proj, w_up, w_down):
        cot, x0 = cot_out.reshape(TD), x_init.reshape(TD)
        (nrm, qkv, pt, mx, nn2, act, h0, pre0, xmid, dmix1, dpre1, dh1) = front(x0, cot, w_query, w_key, w_value, w_proj, w_up, w_down)
        w_in = (w_query, w_key, w_value)
        both, ends = ((0, 0), (0, 1)), ((1, None), (2, None))

        def attention(layer, d_hidden, d_mixed, x_in, number, after):
            groups = ((0, ((0, layer),), 0, ((1, None),), 0), (DB, ((2, layer),), 0, None, 0))
            srcs = (mx, d_hidden, nrm, d_mixed, qkv, pt, x_in, d_hidden, *w_in)
            return scatter_sum(srcs, groups, 4 * DB, number, after, chain=HEADS, layer=layer)

        down = [tuple((DB * n, both, q * D, ends, 0) for n, q in enumerate(qs)) for qs in ((0, 1, 2), (3,))]
        shard1, dmid = attention(1, dh1, dmix1, xmid, 1, ())
        full1 = gather(shard1)
        shard_a, dpre0, dh0, dmix0 = scatter_sum(
            (act, dmid, cot, h0, pre0, dmid, w_proj, w_up, w_down), down[0], 3 * DB, 2, (shard1,), chain=MLP)
        full_a = gather(shard_a)
        shard0, dx = attention(0, dh0, dmix0, x0, 3, (shard_a,))
        full0 = gather(shard0)
        shard_up, = scatter_sum((nn2, dpre0, dpre1), ((0, both, 0, ends, 0),), FB, 4, (shard0,))
        full_up = gather(shard_up)
        shard_b, = scatter_sum((act, dmid, cot), down[1], DB, 5, (shard_up,), spread=True)
        half = place_attention(full1, 1, (), (), (shard_b,))
        g_down = place_blocks(full_a, (FF, D), lambda n: (n, 0), (), (half[0],), "place_down_0")
        g_down = place_blocks(shard_b.reshape(D, D), (FF, D), lambda n: (3, 0), (g_down,), (), "place_down_3")
        *attn, dx = place_attention(full0, 0, half, (dx,), (g_down,))
        g_up = place_blocks(full_up, (D, FF), lambda n: (0, n), (), (attn[0],), "place_up")
        return (*attn, g_up, g_down, dx.reshape(x_init.shape))

    data_spec = P("data")
    full_spec = P()
    in_specs = (data_spec, data_spec) + (full_spec,) * 6
    out_specs = (full_spec,) * 6 + (data_spec,)
    return jax.shard_map(local_step, mesh=mesh, in_specs=in_specs, out_specs=out_specs, check_vma=False)
```

```python
import functools

import jax
import jax.numpy as jnp
from jax import lax
from jax.experimental import pallas as pl
from jax.experimental.pallas import tpu as pltpu
from jax.sharding import PartitionSpec as P

EPS = 1e-6
F32, BF16 = jnp.float32, jnp.bfloat16
TOK, D, FF, SEQ = 1024, 1280, 5120, 128
NB = 256
DB, FB = D // NB, FF // NB
PAIRS = 10
GROUP = 8
VMEM_MOST = 67043328
SUBS = [pl.ds(j * NB, NB) for j in range(DB)]
ANY = pl.BlockSpec(memory_space=pl.ANY)
C0 = 0.7978845608028654
C1 = C0 * 0.044715


def nn(a, b):
    return lax.dot_general(a, b, (((1,), (0,)), ((), ())), preferred_element_type=F32)


def nt(a, b):
    return lax.dot_general(a, b, (((1,), (1,)), ((), ())), preferred_element_type=F32)


def tn(a, b):
    return lax.dot_general(a, b, (((0,), (0,)), ((), ())), preferred_element_type=F32)


def part(i, width):
    return pl.ds(pl.multiple_of(i * width, 128), width)


def rows_of(size):
    return [pl.ds(k * size, size) for k in range(TOK // size)]


class Stage:
    def __init__(self, count, source, step):
        self.count, self.source, self.step = count, source, step


def begin(sources, ring, sem, slot):
    for cond, src in sources:
        copy = pltpu.make_async_copy(src, ring.at[slot], sem.at[slot])
        if cond is None:
            copy.start()
        else:
            pl.when(cond)(copy.start)


def run_stages(items, ring, sem, follow=()):
    stages = [it for it in items if isinstance(it, Stage)]
    base = 0
    for it in items:
        if not isinstance(it, Stage):
            it()
            continue
        after = stages[stages.index(it) + 1].source(0) if it is not stages[-1] else follow

        def one(i, it=it, base=base, after=after):
            slot = lax.rem(base + i, 2)
            pltpu.make_async_copy(it.source(0)[0][1], ring.at[slot], sem.at[slot]).wait()
            other = lax.rem(base + i + 1, 2)

            @pl.when(i + 1 < it.count)
            def _():
                begin(it.source(i + 1), ring, sem, other)

            @pl.when(i + 1 >= it.count)
            def _():
                begin(after, ring, sem, other)
            it.step(i, slot)

        pl.loop(0, it.count)(one)
        base += it.count


def gelu(x):
    half = 0.5 * x
    return half * jnp.tanh(x * (C0 + C1 * (x * x))) + half


def gelu_grad(x, d):
    x2 = x * x
    t = jnp.tanh(x * (C0 + C1 * x2))
    return d * ((0.5 + 0.5 * t) + ((1.0 - t * t) * x) * (0.5 * C0 + 1.5 * C1 * x2))


def by_rows(fn, rows=256):
    @pl.loop(0, TOK // rows)
    def _(i):
        fn(part(i, rows))


def inverse_rms(x):
    return lax.rsqrt(jnp.mean(x * x, axis=-1, keepdims=True) + EPS)


def rms_rows(src, dst):
    def one(r):
        x = src[r, :].astype(F32)
        dst[r, :] = (x * inverse_rms(x)).astype(BF16)
    by_rows(one)


def add_rms_rows(res, acc, out, dst):
    def one(r):
        y = (res[r, :].astype(F32) + acc[r, :].astype(BF16).astype(F32)).astype(BF16)
        out[r, :] = y
        x = y.astype(F32)
        dst[r, :] = (x * inverse_rms(x)).astype(BF16)
    by_rows(one)


def rms_back_rows(x_ref, dy_acc, dres_ref, dst):
    def one(r):
        x = x_ref[r, :].astype(F32)
        dy = dy_acc[r, :].astype(BF16).astype(F32)
        inv = inverse_rms(x)
        dot = jnp.mean(dy * x, axis=-1, keepdims=True)
        dst[r, :] = (dres_ref[r, :].astype(F32) + (dy * inv - x * (inv * inv * inv * dot))).astype(BF16)
    by_rows(one)


def lane_mask():
    return lax.broadcasted_iota(jnp.int32, (SEQ, 2 * 64), 1) < 64


def split_heads(x, mask):
    zero = jnp.zeros_like(x)
    return jnp.concatenate([jnp.where(mask, x, zero), jnp.where(mask, zero, x)], axis=0)


def split_heads_t(x):
    y = x.T
    top = lax.broadcasted_iota(jnp.int32, y.shape, 0) < 64
    zero = jnp.zeros_like(y)
    return jnp.concatenate([jnp.where(top, y, zero), jnp.where(top, zero, y)], axis=1)


def attention_fwd(qkv, pt, mixed):
    mask = lane_mask()

    def one(block):
        for u in range(GROUP * PAIRS):
            h = u // GROUP
            rows = pl.ds(pl.multiple_of(block.start + (u % GROUP) * SEQ, SEQ), SEQ)
            q, k, v = (qkv[rows, pl.ds(n * D + h * SEQ, SEQ)] for n in range(3))
            st = nn(k, split_heads_t(q)) * 0.125
            e = jnp.exp(st - jnp.max(st, axis=0, keepdims=True))
            p = (e / jnp.sum(e, axis=0, keepdims=True)).astype(BF16)
            pt[rows, pl.ds(h * NB, NB)] = p
            o = tn(p, v)
            mixed[rows, pl.ds(h * SEQ, SEQ)] = jnp.where(mask, o[:SEQ], o[SEQ:]).astype(BF16)
    by_rows(one, GROUP * SEQ)


def attention_bwd(s, duo, qkv, pt, dmixed):
    mask = lane_mask()
    rows = part(s, SEQ)
    for h in range(2):
        lanes = [pl.ds(pl.multiple_of(n * D + duo * NB + h * SEQ, SEQ), SEQ) for n in range(3)]
        q, k, v = (qkv[rows, c] for c in lanes)
        do = split_heads(dmixed[rows, lanes[0]], mask)
        p = pt[rows, part(2 * duo + h, NB)]
        dp = nt(v, do).astype(BF16).astype(F32)
        pf = p.astype(F32)
        dot = jnp.sum(dp * pf, axis=0, keepdims=True)
        ds = (pf * (dp - dot) * 0.125).astype(BF16)
        dq = tn(ds, k)
        qkv[rows, lanes[0]] = jnp.where(mask, dq[:SEQ], dq[SEQ:]).astype(BF16)
        qkv[rows, lanes[1]] = nn(ds, split_heads(q, mask)).astype(BF16)
        qkv[rows, lanes[2]] = nn(p, do).astype(BF16)


def front_kernel(x0, cot, wq, wk, wv, wo, w1, w2,
                 n_out, qkv_out, pt_out, mx_out, nn_out, act_out, h0, pre0, xmid, dmix1, dpre1, dh1,
                 x, nrm, qkv, pt, mx, h, n2, big, g, acc, stg, ring, wsem, sems, stg_sem):
    def copy(n, src, dst):
        return pltpu.make_async_copy(src, dst, sems.at[n])

    cx, cg = copy(0, x0, x), copy(1, cot, g)
    cx.start()
    cg.start()
    begin([(None, wq.at[0])], ring, wsem, 0)
    cx.wait()
    rms_rows(x, nrm)

    def stage_copy(i, dst):
        slot = lax.rem(i, 2)
        return pltpu.make_async_copy(stg.at[slot], dst.at[:, part(i, D)], stg_sem.at[slot])

    def sums(stage_count, source, src, times, weight):
        def step(i, slot):
            for c in SUBS:
                for r in rows_of(512):
                    acc[r, c] = jnp.where(i == 0, 0.0, acc[r, c]) + times(src[r, part(i, D)], weight(slot, c))
        return Stage(stage_count, source, step)

    @pl.loop(0, 2)
    def _(l):
        first = l == 0
        outs = dict(n=copy(2, nrm, n_out.at[l]), qkv=copy(3, qkv, qkv_out.at[l]), pt=copy(4, pt, pt_out.at[l]),
                    mx=copy(5, mx, mx_out.at[l]), nn=copy(6, n2, nn_out.at[l]))
        only = dict(h=copy(7, h, h0), act=copy(8, big, act_out.at[0]))

        def qkv_step(i, slot):
            for j, c in enumerate(SUBS):
                for r in rows_of(256):
                    qkv[r, pl.ds(pl.multiple_of(i * D + j * NB, NB), NB)] = nn(nrm[r, :], ring[slot, :, c]).astype(BF16)

        def attend():
            outs["qkv"].start()
            attention_fwd(qkv, pt, mx)
            outs["pt"].start()
            outs["mx"].start()

        def proj_step(i, slot):
            for c in SUBS:
                y = nn(mx[...], ring[slot, :, c]).astype(BF16).astype(F32)
                h[:, c] = (x[:, c].astype(F32) + y).astype(BF16)

        def middle():
            rms_rows(h, n2)
            outs["nn"].start()
            pl.when(first)(only["h"].start)

        def up_step(i, slot):
            half = lax.rem(i, 2)
            pl.when(i >= 2)(stage_copy(i, pre0).wait)
            for j, c in enumerate(SUBS):
                for r in rows_of(128):
                    pre = nn(n2[r, :], ring[slot, :, c]).astype(BF16)
                    act = gelu(pre.astype(F32)).astype(BF16)
                    big[r, pl.ds(pl.multiple_of(i * D + j * NB, NB), NB)] = jnp.where(first, act, pre)
                    stg[half, r, c] = jnp.where(first, pre, act)
            pl.when(first)(stage_copy(i, pre0).start)
            pl.when(l == 1)(stage_copy(i, act_out.at[1]).start)

        outs["n"].start()
        run_stages([Stage(3, lambda i: [(i == m, w.at[l]) for m, w in enumerate((wq, wk, wv))], qkv_step), attend,
                    Stage(1, lambda i: [(None, wo.at[l])], proj_step), middle,
                    Stage(4, lambda i: [(None, w1.at[:, part(i, D)])], up_step)], ring, wsem, [(None, w2.at[pl.ds(0, D)])])
        for i in range(2):
            stage_copy(i, pre0).wait()

        @pl.when(first)
        def _():
            only["act"].start()
            run_stages([sums(4, lambda i: [(None, w2.at[part(i, D)])], big, nn, lambda slot, c: ring[slot, :, c])],
                       ring, wsem, [(None, wq.at[1])])
            for cp in (*outs.values(), *only.values()):
                cp.wait()
            add_rms_rows(h, acc, x, nrm)
            copy(9, x, xmid).start()

    def dact_step(i, slot):
        for j, c in enumerate(SUBS):
            to = pl.ds(pl.multiple_of(i * D + j * NB, NB), NB)
            for r in rows_of(256):
                d = nt(g[r, :], ring[slot, c]).astype(BF16).astype(F32)
                big[r, to] = gelu_grad(big[r, to].astype(F32), d).astype(BF16)

    def after_dact():
        copy(8, big, dpre1).start()

    def after_dn2():
        copy(9, x, xmid).wait()
        rms_back_rows(h, acc, g, x)
        copy(9, x, dh1).start()
        copy(2, nrm, n_out.at[1]).wait()

    def dmix_step(i, slot):
        for c in SUBS:
            nrm[:, c] = nt(x[...], ring[slot, c]).astype(BF16)

    cg.wait()
    run_stages([Stage(4, lambda i: [(None, w2.at[part(i, D)])], dact_step), after_dact,
                sums(4, lambda i: [(None, w1.at[:, part(i, D)])], big, nt, lambda slot, c: ring[slot, c]), after_dn2,
                Stage(1, lambda i: [(None, wo.at[1])], dmix_step)], ring, wsem)
    copy(2, nrm, dmix1).start()
    for n, src, dst in ((2, nrm, dmix1), (3, qkv, qkv_out.at[1]), (4, pt, pt_out.at[1]), (5, mx, mx_out.at[1]),
                        (6, n2, nn_out.at[1]), (8, big, dpre1), (9, x, dh1)):
        copy(n, src, dst).wait()


TD, T3, TF, TP = (TOK, D), (TOK, 3 * D), (TOK, FF), (TOK, PAIRS * NB)


def front(x0, cot, *weights):
    both = [(2,) + s for s in (TD, T3, TP, TD, TD, TF)]
    outs = both + [TD, TF, TD, TD, TF, TD]
    vmem = [pltpu.VMEM(s, BF16) for s in (TD, TD, T3, TP, TD, TD, TD, TF, TD)]
    return pl.pallas_call(
        front_kernel,
        out_shape=[jax.ShapeDtypeStruct(s, BF16) for s in outs],
        in_specs=[ANY] * (2 + len(weights)),
        out_specs=[ANY] * len(outs),
        scratch_shapes=vmem + [pltpu.VMEM(TD, F32), pltpu.VMEM((2, TOK, D), BF16), pltpu.VMEM((2, D, D), BF16),
                               pltpu.SemaphoreType.DMA((2,)), pltpu.SemaphoreType.DMA((10,)), pltpu.SemaphoreType.DMA((2,))],
        compiler_params=pltpu.CompilerParams(vmem_limit_bytes=VMEM_MOST),
        name="front",
    )(x0, cot, *weights)


MESH = pl.DeviceIdType.MESH
ROWS, LANES = 40, 128
OFFSETS = (1, 3, 5, 7)
LAST = OFFSETS[3] + 1
ORDERS = ("xyz", "yzx", "zxy")
CUBE = (2, 2, 2)
HEADS, MLP = 1, 2
N_OUT = (1, 2, 4)


def scatter_kernel(groups, n_tiles, n_src, n_after, chain, layer_in, spread, *refs):
    srcs, refs = refs[:n_src], refs[n_src + n_after:]
    out_ref, more, refs = refs[0], refs[1:N_OUT[chain]], refs[N_OUT[chain]:]
    a_buf, b_buf, tiles, own, rc, r1, r2, r3, a_sem, b_sem, out_sem, send_sem, recv_sem, *refs = refs
    heads, mlp, depth = chain == HEADS, chain == MLP, len(groups[0][1])
    if spread:
        all_send, all_recv = refs
    if chain:
        xb, gb, tb, acc, wring, w_sem, at_sem, big, *refs = refs
    if heads:
        (qkv, head_sem), pt = refs, big
        _, _, _, dmixed_in, qkv_in, pt_in, x_in, d_in, wq, wk, wv = srcs
        qkv_in, pt_in = qkv_in.at[layer_in], pt_in.at[layer_in]
    if mlp:
        _, _, _, h_in, pre_in, d_in, wo, w1, w2 = srcs
    me = lax.axis_index("data")
    bit, peer = {}, {}
    for n, d in enumerate("cxyz"):
        bit[d] = lax.rem(me // 2 ** n, 2)
        peer[d] = me + 2 ** n * (1 - 2 * bit[d])
    n_own, n_in, ring = own.shape[1], rc.shape[1], tiles.shape[0]
    n_chunks = 4 * n_tiles
    bufs = (rc, r1, r2, r3)

    def group_of(m):
        a = 0
        for first in groups[1:]:
            a = a + (m >= first[0]).astype(jnp.int32)
        return a

    def source(spec):
        n, layer = spec
        return srcs[n] if layer is None else srcs[n].at[layer]

    def a_load(a, layer):
        _, ins, col, _, _ = groups[a]
        return pltpu.make_async_copy(source(ins[layer]).at[:, pl.ds(col, D)], a_buf.at[a % 2, layer], a_sem.at[a % 2, layer])

    def b_load(a, m, layer, ahead=True):
        first, _, _, ins, col = groups[a]
        if ahead:
            col = pl.multiple_of(col + (m - first) * NB, NB)
        slot = lax.rem(m, 2)
        return pltpu.make_async_copy(source(ins[layer]).at[:, pl.ds(col, NB)], b_buf.at[slot, layer], b_sem.at[slot, layer])

    def in_group(a, m, fn):
        last = groups[a + 1][0] if a + 1 < len(groups) else n_tiles

        @pl.when(jnp.logical_and(m >= groups[a][0], m < last))
        def _():
            fn()

    def b_start(m):
        for a in range(len(groups)):
            if groups[a][3] is None:
                continue

            def go(a=a):
                for layer in range(depth):
                    b_load(a, m, layer).start()
            in_group(a, m, go)

    def produce(m):
        half, slot, to = lax.rem(group_of(m), 2), lax.rem(m, 2), lax.rem(m, ring)

        @pl.when(m < (DB if heads else n_tiles))
        def _():
            for layer in range(depth):
                b_load(0, m, layer, False).wait()
        if heads:
            @pl.when(m >= DB)
            def _():
                b_buf[slot, 0] = qkv[:, pl.ds(pl.multiple_of(lax.rem(m - DB, 3) * D + ((m - DB) // 3) * NB, NB), NB)]
        for a in range(len(groups)):
            @pl.when(m == groups[a][0])
            def _():
                for layer in range(depth):
                    a_load(a, layer).wait()
                if a + 1 < len(groups):
                    for layer in range(depth):
                        a_load(a + 1, layer).start()
        b_start(m + 1)

        for z in range(2):
            tot = None
            for layer in range(depth):
                y = tn(a_buf[half, layer, :, part(z, D // 2)], b_buf[slot, layer])
                tot = y if tot is None else tot + y
            tiles[to, z] = tot.reshape(CUBE + (2 * ROWS, NB))

    def pick(color, stage, other):
        idx = {d: slice(None) for d in "zyx"}
        for s in range(stage):
            d = ORDERS[color][s]
            idx[d] = 1 - bit[d] if (other and s == stage - 1) else bit[d]
        return tuple(idx[d] for d in "zyx")

    def piece(k):
        sub = lax.rem(k, 4)
        return (lax.rem(k // 4, ring), pl.multiple_of(lax.rem(sub, 2) * ROWS, 8), pl.multiple_of((sub // 2) * LANES, LANES))

    def send(color, stage, j):
        slot, so = lax.rem(j, n_in), lax.rem(j, n_own)
        if stage == 0:
            tile, row, col = piece(3 * j + color)
            src, to = tiles.at[tile, :, :, :, 1 - bit["c"], pl.ds(row, ROWS), pl.ds(col, LANES)], peer["c"]
        else:
            src, to = own.at[(color, so) + pick(color, stage, True)], peer[ORDERS[color][stage - 1]]
        return pltpu.make_async_remote_copy(src, bufs[stage].at[color, slot], send_sem.at[color, stage, slot],
                                            recv_sem.at[color, stage, slot], device_id=(to,), device_id_type=MESH)

    def place(color, j):
        k = 3 * j + color
        _, row, col = piece(k)
        tile = k // 4
        if heads:
            tile = jnp.where(tile < DB, tile, DB + DB * lax.rem(tile - DB, 3) + (tile - DB) // 3)
        return pl.ds(row, ROWS), pl.ds(pl.multiple_of(tile * NB + col, LANES), LANES)

    def store(color, j):
        so = lax.rem(j, n_own)
        where = place(color, j)
        if spread:
            where = (bit["z"], bit["y"], bit["x"], bit["c"]) + where
        return pltpu.make_async_copy(own.at[(color, so) + pick(color, 3, False)], out_ref.at[where], out_sem.at[color, so])

    def hand_on(color, stage, j):
        slot, so = lax.rem(j, n_in), lax.rem(j, n_own)
        idx = {d: bit[d] for d in "zyxc"}
        for d in ORDERS[color][3 - stage:]:
            idx[d] = slice(None)
        dst = out_ref.at[(idx["z"], idx["y"], idx["x"], idx["c"]) + place(color, j)]
        src = dst if stage else own.at[(color, so) + pick(color, 3, False)]
        to = peer[ORDERS[color][2 - stage] if stage < 3 else "c"]
        return pltpu.make_async_remote_copy(src, dst, all_send.at[color, stage, slot], all_recv.at[color, stage, slot],
                                            device_id=(to,), device_id_type=MESH)

    def live(j, color):
        return jnp.logical_and(j >= 0, 3 * j + color < n_chunks)

    up_from, norm_at, end = FB, 2 * FB, 2 * FB + 1 + DB

    def w_begin(w):
        slot = lax.rem(w, 3)
        begin([(w < up_from, w2.at[part(w, NB)]),
               (jnp.logical_and(w >= up_from, w < norm_at), w1.at[part(lax.rem(w, DB), NB), part((w - up_from) // DB, D)]),
               (jnp.logical_and(w >= norm_at, w < end - 1), wo.at[layer_in, part(lax.rem(w, DB), NB)])], wring, w_sem, slot)

    def w_take(w):
        slot = lax.rem(w, 3)
        pltpu.make_async_copy(wo.at[0, pl.ds(0, NB)], wring.at[slot], w_sem.at[slot]).wait()
        w_begin(w + 2)
        return slot

    def head_weights(duo):
        col = pl.multiple_of(duo * NB, NB)
        base = 3 * lax.rem(duo, 2)
        return [pltpu.make_async_copy(ref.at[layer_in, :, pl.ds(col, NB)], wring.at[base + m], w_sem.at[base + m])
                for m, ref in enumerate((wq, wk, wv))]

    def start(*names):
        for name in names:
            copies[name].start()

    def wait(*names):
        for name in names:
            copies[name].wait()

    if chain:
        if heads:
            table = dict(x=(x_in, xb), d=(d_in, tb), first=(gb, *more))
        else:
            table = dict(d=(d_in, gb), h=(h_in, xb), pre=(pre_in, big), dpre=(big, more[0]), dh=(tb, more[1]), dmix=(xb, more[2]))
        copies = {name: pltpu.make_async_copy(src, dst, at_sem.at[n]) for n, (name, (src, dst)) in enumerate(table.items())}

    def head_loads(duo):
        cols = [pl.ds(n * D + duo * NB, NB) for n in range(3)]
        pairs = [(dmixed_in, xb, cols[0]), (pt_in, pt, pl.ds(duo * 2 * NB, 2 * NB))] + [(qkv_in, qkv, c) for c in cols]
        return [pltpu.make_async_copy(src.at[:, c], dst.at[:, c], head_sem.at[duo, n]) for n, (src, dst, c) in enumerate(pairs)]

    def input_step(duo, turn):
        @pl.when(turn == 0)
        def _():
            for copy in head_weights(duo):
                copy.wait()

            @pl.when(duo < DB - 1)
            def _():
                for copy in head_weights(duo + 1):
                    copy.start()
        base = 3 * lax.rem(duo, 2)

        @pl.loop(jnp.where(turn == 0, 0, turn + 1), turn + 2)
        def _(n):
            c = part(n, NB)
            tot = jnp.where(duo == 0, 0.0, acc[:, c])
            for m in range(3):
                tot = tot + nt(qkv[:, pl.ds(pl.multiple_of(m * D + duo * NB, NB), NB)], wring[base + m, c])
            acc[:, c] = tot

    def sum_step(g, src, slot):
        c, m = part(lax.rem(g, DB), NB), g // DB

        for r in rows_of(512):
            acc[r, c] = jnp.where(m == 0, 0.0, acc[r, c]) + nt(src[r, part(m, D)], wring[slot])

    def mlp_step(g):
        @pl.when(g == 0)
        def _():
            wait("d", "pre")

        @pl.when(g < up_from)
        def _():
            slot, c = w_take(g), part(g, NB)

            for r in rows_of(256):
                d = nt(gb[r, :], wring[slot]).astype(BF16).astype(F32)
                big[r, c] = gelu_grad(big[r, c].astype(F32), d).astype(BF16)

        @pl.when(g == up_from)
        def _():
            start("dpre")

        @pl.when(jnp.logical_and(g >= up_from, g < norm_at))
        def _():
            sum_step(g - up_from, big, w_take(g))

        @pl.when(g == norm_at)
        def _():
            wait("h")
            rms_back_rows(xb, acc, gb, tb)
            start("dh")

        @pl.when(jnp.logical_and(g > norm_at, g < end))
        def _():
            slot, c = w_take(g - 1), part(g - norm_at - 1, NB)

            for r in rows_of(512):
                xb[r, c] = nt(tb[r, :], wring[slot]).astype(BF16)

        @pl.when(g == end - 1)
        def _():
            start("dmix")

    def tick(t, carry):
        for stage in (3, 2, 1, 0) if spread else ():
            j = t - OFFSETS[3] - 2 * (stage + 1)
            for color in range(3):
                @pl.when(live(j, color))
                def _():
                    copy = hand_on(color, stage, j)
                    copy.wait_send()
                    copy.wait_recv()
                    if stage == 0:
                        store(color, j).wait()
                    if stage < 3:
                        hand_on(color, stage + 1, j).start()
        for color in () if spread else range(3):
            j = t - LAST

            @pl.when(live(j, color))
            def _():
                store(color, j).wait()
        for stage in (3, 2, 1, 0):
            j = t - OFFSETS[stage]
            for color in range(3):
                @pl.when(live(j, color))
                def _():
                    slot, so = lax.rem(j, n_in), lax.rem(j, n_own)
                    copy = send(color, stage, j)
                    copy.wait_send()
                    copy.wait_recv()
                    keep = (color, so) + pick(color, stage, False)
                    if stage == 0:
                        tile, row, col = piece(3 * j + color)
                        mine = tiles[tile, :, :, :, bit["c"], pl.ds(row, ROWS), pl.ds(col, LANES)]
                    else:
                        mine = own[keep]
                    own[keep] = mine + bufs[stage][color, slot]
                    if stage < 3:
                        send(color, stage + 1, j).start()
                    else:
                        store(color, j).start()
                        if spread:
                            hand_on(color, 0, j).start()
        for color in range(3):
            @pl.when(live(t, color))
            def _():
                send(color, 0, t).start()
        if heads:
            for duo in range(DB):
                @pl.when(t == 1 + 4 * duo)
                def _():
                    for copy in head_loads(duo):
                        copy.wait()

            @pl.when(jnp.logical_and(t > 0, t <= 4 * DB))
            def _():
                for u in range(2):
                    attention_bwd(2 * lax.rem(t - 1, 4) + u, (t - 1) // 4, qkv, pt, xb)
        m = (3 * t + 5) // 4

        @pl.when(jnp.logical_and(m != (3 * t + 2) // 4, m < n_tiles))
        def _():
            produce(m)
        if heads:
            first_tick, last_attend = DB, 4 * DB
            since = t - first_tick
            quarter = jnp.where(t > last_attend, since - last_attend // 2 + 2, since // 2)
            norm_tick = first_tick + last_attend + last_attend // 2 - 2

            @pl.when(jnp.logical_and(jnp.logical_and(since >= 0, t < norm_tick), jnp.logical_or(t > last_attend, lax.rem(since, 2) == 0)))
            def _():
                input_step(quarter // 4, lax.rem(quarter, 4))

            @pl.when(t == last_attend + 1)
            def _():
                start("x")

            @pl.when(t == norm_tick)
            def _():
                wait("x", "d")
                rms_back_rows(xb, acc, tb, gb)
                start("first")
        if mlp:
            @pl.when(2 * t < end)
            def _():
                @pl.loop(0, 2)
                def _(u):
                    mlp_step(2 * t + u)
        return carry

    for layer in range(depth):
        a_load(0, layer).start()
    b_start(jnp.int32(0))
    if heads:
        for duo in range(DB):
            for copy in head_loads(duo):
                copy.start()
        for copy in head_weights(jnp.int32(0)):
            copy.start()
        start("d")
    if mlp:
        start("d", "pre", "h")
        for n in range(2):
            w_begin(jnp.int32(n))
    barrier = pltpu.get_barrier_semaphore()
    for d in "cxyz":
        pl.semaphore_signal(barrier, inc=1, device_id=(peer[d],), device_id_type=MESH)
    pl.semaphore_wait(barrier, 4)
    produce(jnp.int32(0))
    ticks = pl.cdiv(n_chunks, 3) + LAST + 8 * spread
    lax.fori_loop(0, ticks, tick, 0)
    if heads:
        wait("first")
    if mlp:
        wait("dpre", "dh", "dmix")


def scatter_sum(srcs, groups, n_tiles, collective_id, after=(), chain=0, layer=0, spread=False):
    depth = len(groups[0][1])
    n_own, n_in, blk = LAST + 1 + spread, 4, (ROWS, LANES)
    size = D * NB * n_tiles * 4
    outs = [(), (TD,), (TF, TD, TD)][chain]
    sums = (CUBE + (2,)) * spread + (2 * ROWS, NB * n_tiles)
    args = (*srcs, *after)
    dma = pltpu.SemaphoreType.DMA
    scratch = [
        pltpu.VMEM((2, depth, TOK, D), BF16), pltpu.VMEM((2, depth, TOK, NB), BF16), pltpu.VMEM((n_in, 2) + CUBE + (2 * ROWS, NB), F32),
        pltpu.VMEM((3, n_own) + CUBE + blk, F32)] + [pltpu.VMEM((3, n_in) + CUBE[n:] + blk, F32) for n in range(4)] + [
        dma((2, depth)), dma((2, depth)), dma((3, n_own)), dma((3, 4, n_in)), dma((3, 4, n_in))]
    if spread:
        scratch += [dma((3, 4, n_in))] * 2
    if chain:
        scratch += [pltpu.VMEM(TD, BF16)] * 3 + [
            pltpu.VMEM(TD, F32), pltpu.VMEM((6, D, NB) if chain == HEADS else (3, NB, D), BF16), dma((6,)), dma((6,))]
        scratch += [pltpu.VMEM(TP, BF16), pltpu.VMEM(T3, BF16), dma((DB, DB))] if chain == HEADS else [pltpu.VMEM(TF, BF16)]
    return pl.pallas_call(
        functools.partial(scatter_kernel, groups, n_tiles, len(srcs), len(after), chain, layer, spread),
        out_shape=[jax.ShapeDtypeStruct(sums, F32)] + [jax.ShapeDtypeStruct(o, BF16) for o in outs],
        in_specs=[ANY] * len(args),
        out_specs=[ANY] * (1 + len(outs)),
        scratch_shapes=scratch,
        compiler_params=pltpu.CompilerParams(collective_id=collective_id, has_side_effects=True, vmem_limit_bytes=VMEM_MOST),
        cost_estimate=pl.CostEstimate(flops=size * 4000, bytes_accessed=2 * size, transcendentals=0),
        name=f"scatter_sum_{collective_id}",
    )(*args)


def gather(shard):
    return lax.all_gather(shard, "data", axis=0, tiled=True)


def place_attention(full, layer, dst, carry, after):
    rows, part = 160, TOK * 160 // D

    def kernel(src, *refs):
        outs = refs[-4 - len(carry):]
        for n, out in zip((1, 2, 3, 0), outs):
            out[0] = src[:, n * D:(n + 1) * D]
        for ref, out in zip(refs, outs[4:]):
            out[...] = ref[...]

    strip = pl.BlockSpec((part, D), lambda i: (i, 0))
    return pl.pallas_call(
        kernel,
        grid=(D // rows,),
        out_shape=[jax.ShapeDtypeStruct((2, D, D), F32)] * 4 + [jax.ShapeDtypeStruct((TOK, D), BF16)] * len(carry),
        in_specs=[pl.BlockSpec((rows, 4 * D), lambda i: (i, 0))] + [strip] * len(carry) + [ANY] * (len(dst) + len(after)),
        out_specs=[pl.BlockSpec((1, rows, D), lambda i: (layer, i, 0))] * 4 + [strip] * len(carry),
        input_output_aliases={n + 1 + len(carry): n for n in range(len(dst))},
        compiler_params=pltpu.CompilerParams(vmem_limit_bytes=60 << 20),
        cost_estimate=pl.CostEstimate(flops=D * D, bytes_accessed=32 * D * D, transcendentals=0),
        name=f"place_attention_{layer}",
    )(full, *carry, *dst, *after)


def place_blocks(full, shape, where, dst, after, name):
    rows = D // 4
    blocks = full.shape[1] // D
    strips = [(n, i) for n in range(blocks) for i in range(D // rows)]

    def kernel(src, *refs):
        out, buf, load_sem, store_sem = refs[len(dst) + len(after):]
        loads, stores = [], []
        for k, (n, i) in enumerate(strips):
            row, col = where(n)
            loads.append(pltpu.make_async_copy(src.at[pl.ds(i * rows, rows), pl.ds(n * D, D)], buf.at[k], load_sem.at[k]))
            stores.append(pltpu.make_async_copy(buf.at[k], out.at[pl.ds(row * D + i * rows, rows), pl.ds(col * D, D)], store_sem.at[k]))
        for load in loads:
            load.start()
        for load, store in zip(loads, stores):
            load.wait()
            store.start()
        for store in stores:
            store.wait()

    return pl.pallas_call(
        kernel,
        out_shape=jax.ShapeDtypeStruct(shape, F32),
        in_specs=[ANY] * (1 + len(dst) + len(after)),
        out_specs=ANY,
        scratch_shapes=[pltpu.VMEM((len(strips), rows, D), F32)] + [pltpu.SemaphoreType.DMA((len(strips),))] * 2,
        input_output_aliases={1: 0} if dst else {},
        compiler_params=pltpu.CompilerParams(vmem_limit_bytes=VMEM_MOST),
        cost_estimate=pl.CostEstimate(flops=D * D, bytes_accessed=8 * blocks * D * D, transcendentals=0),
        name=name,
    )(full, *dst, *after)


def solution(mesh):
    def local_step(x_init, cot_out, w_query, w_key, w_value, w_proj, w_up, w_down):
        cot, x0 = cot_out.reshape(TD), x_init.reshape(TD)
        (nrm, qkv, pt, mx, nn2, act, h0, pre0, xmid, dmix1, dpre1, dh1) = front(x0, cot, w_query, w_key, w_value, w_proj, w_up, w_down)
        w_in = (w_query, w_key, w_value)
        both, ends = ((0, 0), (0, 1)), ((1, None), (2, None))

        def attention(layer, d_hidden, d_mixed, x_in, number, after):
            groups = ((0, ((0, layer),), 0, ((1, None),), 0), (DB, ((2, layer),), 0, None, 0))
            srcs = (mx, d_hidden, nrm, d_mixed, qkv, pt, x_in, d_hidden, *w_in)
            return scatter_sum(srcs, groups, 4 * DB, number, after, chain=HEADS, layer=layer)

        down = [tuple((DB * n, both, q * D, ends, 0) for n, q in enumerate(qs)) for qs in ((0, 1, 2), (3,))]
        shard1, dmid = attention(1, dh1, dmix1, xmid, 1, ())
        full1 = gather(shard1)
        shard_a, dpre0, dh0, dmix0 = scatter_sum(
            (act, dmid, cot, h0, pre0, dmid, w_proj, w_up, w_down), down[0], 3 * DB, 2, (shard1,), chain=MLP)
        full_a = gather(shard_a)
        shard0, dx = attention(0, dh0, dmix0, x0, 3, (shard_a,))
        full0 = gather(shard0)
        shard_up, = scatter_sum((nn2, dpre0, dpre1), ((0, both, 0, ends, 0),), FB, 4, (shard0,))
        full_up = gather(shard_up)
        shard_b, = scatter_sum((act, dmid, cot), down[1], DB, 5, (shard_up,), spread=True)
        half = place_attention(full1, 1, (), (), (shard_b,))
        g_down = place_blocks(full_a, (FF, D), lambda n: (n, 0), (), (half[0],), "place_down_0")
        g_down = place_blocks(shard_b.reshape(D, D), (FF, D), lambda n: (3, 0), (g_down,), (), "place_down_3")
        *attn, dx = place_attention(full0, 0, half, (dx,), (g_down,))
        g_up = place_blocks(full_up, (D, FF), lambda n: (0, n), (), (attn[0],), "place_up")
        return (*attn, g_up, g_down, dx.reshape(x_init.shape))

    data_spec = P("data")
    full_spec = P()
    in_specs = (data_spec, data_spec) + (full_spec,) * 6
    out_specs = (full_spec,) * 6 + (data_spec,)
    return jax.shard_map(local_step, mesh=mesh, in_specs=in_specs, out_specs=out_specs, check_vma=False)
```
